8 devices in a mesh: dp: 1 (over z), sp: 8 (over x, y, core).
Axes of the slice: x: 2, y: 2, z: 1, core: 2. Of those that a mesh axis runs over, the one named last changes fastest.
Arguments:
- q: bfloat16 [32, 16, 256], P('dp')
- k: bfloat16 [32, 8192, 1, 256], P('dp', 'sp')
- v: bfloat16 [32, 8192, 1, 256], P('dp', 'sp')
Outputs:
- q: bfloat16 [32, 16, 256], P('dp')
All inputs are finite; a program needn't handle non-finite values.
Results may differ from the reference program's by a relative error of at most 0.012.
Values are sent between devices in bfloat16 or wider.
A program may use at most 2 GiB of HBM per device.

```python
import jax
import jax.numpy as jnp

BATCH = 32
CACHE = 8192
HEADS = 16
KV_HEADS = 1
HEAD = 256


def setup_inputs(seed: int = 0, part: int = 0) -> dict:
    kq, kk, kv = (jax.random.fold_in(k, part) for k in jax.random.split(jax.random.key(seed), 3))
    return {
        "q": (3 * jax.random.normal(kq, (BATCH, HEADS, HEAD), jnp.float32)).astype(jnp.bfloat16),
        "k": jax.random.normal(kk, (BATCH, CACHE, KV_HEADS, HEAD), jnp.float32).astype(jnp.bfloat16),
        "v": jax.random.normal(kv, (BATCH, CACHE, KV_HEADS, HEAD), jnp.float32).astype(jnp.bfloat16),
    }


def einsum(form, a, b):
    return jnp.einsum(form, a.astype(jnp.float32), b.astype(jnp.float32))


def reference(q, k, v):
    grouped = q.reshape(BATCH, KV_HEADS, -1, HEAD)
    scores = einsum("bgsd,bugd->bgsu", grouped, k) * HEAD**-0.5
    weights = jax.nn.softmax(scores, -1).astype(jnp.bfloat16)
    return einsum("bgsu,bugd->bgsd", weights, v).astype(jnp.bfloat16).reshape(BATCH, HEADS, HEAD)
```

```python
import functools

import jax
import jax.numpy as jnp
from jax import lax
from jax.experimental import pallas as pl
from jax.experimental.pallas import tpu as pltpu
from jax.sharding import PartitionSpec as P

MESH = pl.DeviceIdType.MESH
F32 = jnp.float32
BF16 = jnp.bfloat16
AHEAD = 4


def kernel(n, scale, q_hbm, k_hbm, v_hbm, o_ref, q_buf, k_buf, v_buf, part, sent, stat, got, got_stat, out,
           q_sem, k_sem, v_sem, send_sem, send_stat_sem, got_sem, got_stat_sem, out_sem):
    me = lax.axis_index("sp")
    batch, heads, head = q_buf.shape
    groups = batch // n

    def peer(r):
        return lax.rem(me + r, n)

    def k_copy(s):
        return pltpu.make_async_copy(k_hbm.at[s], k_buf.at[s], k_sem.at[s])

    def v_copy(s):
        return pltpu.make_async_copy(v_hbm.at[s], v_buf.at[s], v_sem.at[s])

    q_copy = pltpu.make_async_copy(q_hbm, q_buf, q_sem)
    k_copy(0).start()
    q_copy.start()
    for s in range(AHEAD):
        if s > 0:
            k_copy(s).start()
        v_copy(s).start()

    barrier = pltpu.get_barrier_semaphore()
    for r in range(1, n):
        pl.semaphore_signal(barrier, inc=1, device_id={"sp": peer(r)}, device_id_type=MESH)

    def scores_of(s):
        return lax.dot_general(q_buf[s], k_buf[s], (((1,), (1,)), ((), ())), preferred_element_type=F32)

    def finish(s, scores):
        high = jnp.max(scores, -1, keepdims=True)
        weights = jnp.exp((scores - high) * scale)
        total = jnp.sum(weights, -1, keepdims=True)
        seen = jnp.dot(weights.astype(BF16), v_buf[s], preferred_element_type=F32)
        part[s] = seen
        sent[s] = seen.astype(BF16)
        lane = lax.broadcasted_iota(jnp.int32, (heads, 128), 1)
        both = jnp.where(lane == 0, high * scale, total)
        stat[s, :, :heads] = jnp.transpose(both)[:2]

    def send(s):
        owner = lax.rem(s, n)
        group = s // n
        slot = lax.rem(me - owner + n, n) - 1

        @pl.when(owner != me)
        def _():
            pltpu.make_async_remote_copy(
                src_ref=sent.at[s], dst_ref=got.at[group, slot], send_sem=send_sem, recv_sem=got_sem.at[group],
                device_id={"sp": owner}, device_id_type=MESH).start()
            pltpu.make_async_remote_copy(
                src_ref=stat.at[s], dst_ref=got_stat.at[group, slot], send_sem=send_stat_sem,
                recv_sem=got_stat_sem.at[group], device_id={"sp": owner}, device_id_type=MESH).start()

    def combine(group):
        s = group * n + me
        pltpu.make_async_copy(got.at[group], got.at[group], got_sem.at[group]).wait()
        pltpu.make_async_copy(got_stat.at[group], got_stat.at[group], got_stat_sem.at[group]).wait()
        stats = [stat[s]] + [got_stat[group, r] for r in range(n - 1)]
        high = functools.reduce(jnp.maximum, [x[:1] for x in stats])
        scales = [jnp.exp(x[:1] - high) for x in stats]
        total = functools.reduce(jnp.add, [w * x[1:] for w, x in zip(scales, stats)])
        rows = jnp.concatenate([w / total for w in scales], 0)
        columns = jnp.transpose(rows)[:heads]
        result = part[s] * columns[:, :1]
        for r in range(n - 1):
            result += got[group, r].astype(F32) * columns[:, r + 1:r + 2]
        out[s] = result.astype(BF16)
        for r in range(1, n):
            pltpu.make_async_remote_copy(
                src_ref=out.at[s], dst_ref=out.at[s], send_sem=send_sem, recv_sem=out_sem,
                device_id={"sp": peer(r)}, device_id_type=MESH).start()

    q_copy.wait()
    k_copy(0).wait()
    pl.semaphore_wait(barrier, n - 1)

    def step(s, scores):
        k_copy(s).wait()
        v_copy(s - 1).wait()
        later = s + AHEAD - 1

        @pl.when(later < batch)
        def _():
            k_copy(later).start()
            v_copy(later).start()

        @pl.when(s >= 2)
        def _():
            send(s - 2)

        @pl.when((lax.rem(s, n) == n - 1) & (s >= 2 * n - 1))
        def _():
            combine(s // n - 1)

        new = scores_of(s)
        finish(s - 1, scores)
        return new

    scores = lax.fori_loop(1, batch, step, scores_of(0))
    v_copy(batch - 1).wait()
    finish(batch - 1, scores)
    send(batch - 2)
    send(batch - 1)
    combine(groups - 1)
    others = batch - groups
    pltpu.make_async_copy(out.at[pl.ds(0, others)], out.at[pl.ds(0, others)], out_sem).wait()
    o_ref[...] = out[...]
    pltpu.make_async_copy(out.at[pl.ds(0, others)], out.at[pl.ds(0, others)], send_sem).wait()
    pltpu.make_async_copy(out.at[pl.ds(0, others)], out.at[pl.ds(0, others)], send_sem).wait()
    pltpu.make_async_copy(stat.at[pl.ds(0, others)], stat.at[pl.ds(0, others)], send_stat_sem).wait()


def solution(mesh):
    n = mesh.shape["sp"]

    def step(q, k, v):
        batch, heads, head = q.shape
        tokens = k.shape[1]
        k = k.reshape(batch, tokens, head)
        v = v.reshape(batch, tokens, head)
        groups = batch // n
        return pl.pallas_call(
            functools.partial(kernel, n, head ** -0.5),
            out_shape=jax.ShapeDtypeStruct(q.shape, BF16),
            in_specs=[pl.BlockSpec(memory_space=pltpu.HBM)] * 3,
            out_specs=pl.BlockSpec(memory_space=pltpu.VMEM),
            scratch_shapes=[
                pltpu.VMEM((batch, heads, head), BF16),
                pltpu.VMEM((batch, tokens, head), BF16),
                pltpu.VMEM((batch, tokens, head), BF16),
                pltpu.VMEM((batch, heads, head), F32),
                pltpu.VMEM((batch, heads, head), BF16),
                pltpu.VMEM((batch, 2, 128), F32),
                pltpu.VMEM((groups, n - 1, heads, head), BF16),
                pltpu.VMEM((groups, n - 1, 2, 128), F32),
                pltpu.VMEM((batch, heads, head), BF16),
                pltpu.SemaphoreType.DMA,
                pltpu.SemaphoreType.DMA((batch,)),
                pltpu.SemaphoreType.DMA((batch,)),
                pltpu.SemaphoreType.DMA,
                pltpu.SemaphoreType.DMA,
                pltpu.SemaphoreType.DMA((groups,)),
                pltpu.SemaphoreType.DMA((groups,)),
                pltpu.SemaphoreType.DMA,
            ],
            compiler_params=pltpu.CompilerParams(
                collective_id=0, has_side_effects=True, vmem_limit_bytes=48 * 1024 * 1024),
            name="decode",
        )(q, k, v)

    return jax.shard_map(
        step,
        mesh=mesh,
        in_specs=(P("dp", None, None), P("dp", "sp", None, None), P("dp", "sp", None, None)),
        out_specs=P("dp", None, None),
        check_vma=False,
    )
```

```python
import functools

import jax
import jax.numpy as jnp
from jax import lax
from jax.experimental import pallas as pl
from jax.experimental.pallas import tpu as pltpu
from jax.sharding import PartitionSpec as P

MESH = pl.DeviceIdType.MESH
F32 = jnp.float32
BF16 = jnp.bfloat16
BLOCK = 2
AHEAD = 2


def kernel(n, scale, q_hbm, k_hbm, v_hbm, o_ref, q_buf, k_buf, v_buf, raw, part, sent, stat, got, got_stat, out,
           q_sem, k_sem, v_sem, send_sem, send_stat_sem, got_sem, got_stat_sem, out_sem):
    me = lax.axis_index("sp")
    batch, heads, head = q_buf.shape
    groups = batch // n
    blocks = batch // BLOCK

    def peer(r):
        return lax.rem(me + r, n)

    def k_copy(b):
        run = pl.ds(b * BLOCK, BLOCK)
        return pltpu.make_async_copy(k_hbm.at[run], k_buf.at[run], k_sem.at[lax.rem(b, 2 * AHEAD)])

    def v_copy(b):
        run = pl.ds(b * BLOCK, BLOCK)
        return pltpu.make_async_copy(v_hbm.at[run], v_buf.at[run], v_sem.at[lax.rem(b, 2 * AHEAD)])

    q_copy = pltpu.make_async_copy(q_hbm, q_buf, q_sem)
    k_copy(0).start()
    q_copy.start()
    for b in range(AHEAD):
        if b > 0:
            k_copy(b).start()
        v_copy(b).start()

    barrier = pltpu.get_barrier_semaphore()
    for r in range(1, n):
        pl.semaphore_signal(barrier, inc=1, device_id={"sp": peer(r)}, device_id_type=MESH)

    def scores_of(s, parity, j):
        raw[parity][j] = lax.dot_general(q_buf[s], k_buf[s], (((1,), (1,)), ((), ())), preferred_element_type=F32)

    def finish(s, parity, j):
        scores = raw[parity][j]
        high = jnp.max(scores, -1, keepdims=True)
        weights = jnp.exp((scores - high) * scale)
        total = jnp.sum(weights, -1, keepdims=True)
        seen = jnp.dot(weights.astype(BF16), v_buf[s], preferred_element_type=F32)
        part[s] = seen
        sent[s] = seen.astype(BF16)
        lane = lax.broadcasted_iota(jnp.int32, (heads, 128), 1)
        both = jnp.where(lane == 0, high * scale, total)
        stat[s, :, :heads] = jnp.transpose(both)[:2]

    def send(s):
        owner = lax.rem(s, n)
        group = s // n
        slot = lax.rem(me - owner + n, n) - 1

        @pl.when(owner != me)
        def _():
            pltpu.make_async_remote_copy(
                src_ref=sent.at[s], dst_ref=got.at[group, slot], send_sem=send_sem, recv_sem=got_sem.at[group],
                device_id={"sp": owner}, device_id_type=MESH).start()
            pltpu.make_async_remote_copy(
                src_ref=stat.at[s], dst_ref=got_stat.at[group, slot], send_sem=send_stat_sem,
                recv_sem=got_stat_sem.at[group], device_id={"sp": owner}, device_id_type=MESH).start()

    def combine(group):
        s = group * n + me
        pltpu.make_async_copy(got.at[group], got.at[group], got_sem.at[group]).wait()
        pltpu.make_async_copy(got_stat.at[group], got_stat.at[group], got_stat_sem.at[group]).wait()
        stats = [stat[s]] + [got_stat[group, r] for r in range(n - 1)]
        high = functools.reduce(jnp.maximum, [x[:1] for x in stats])
        scales = [jnp.exp(x[:1] - high) for x in stats]
        total = functools.reduce(jnp.add, [w * x[1:] for w, x in zip(scales, stats)])
        rows = jnp.concatenate([w / total for w in scales], 0)
        columns = jnp.transpose(rows)[:heads]
        result = part[s] * columns[:, :1]
        for r in range(n - 1):
            result += got[group, r].astype(F32) * columns[:, r + 1:r + 2]
        out[s] = result.astype(BF16)
        for r in range(1, n):
            pltpu.make_async_remote_copy(
                src_ref=out.at[s], dst_ref=out.at[s], send_sem=send_sem, recv_sem=out_sem,
                device_id={"sp": peer(r)}, device_id_type=MESH).start()

    q_copy.wait()
    k_copy(0).wait()
    pl.semaphore_wait(barrier, n - 1)
    for j in range(BLOCK):
        scores_of(j, 0, j)

    def block(b, parity):
        k_copy(b).wait()
        v_copy(b - 1).wait()
        later = b + AHEAD - 1

        @pl.when(later < blocks)
        def _():
            k_copy(later).start()
            v_copy(later).start()

        @pl.when(b >= 2)
        def _():
            for j in range(BLOCK):
                send((b - 2) * BLOCK + j)

        for j in range(BLOCK):
            scores_of(b * BLOCK + j, parity, j)
        for j in range(BLOCK):
            finish((b - 1) * BLOCK + j, 1 - parity, j)

    per = n // BLOCK

    def pair(i, _):
        block(2 * i - 1, 1)
        block(2 * i, 0)

        @pl.when((lax.rem(2 * i, per) == 0) & (2 * i >= 2 * per))
        def _():
            combine(2 * i // per - 2)
        return 0

    lax.fori_loop(1, blocks // 2, pair, 0)
    block(blocks - 1, 1)
    v_copy(blocks - 1).wait()
    for j in range(BLOCK):
        finish((blocks - 1) * BLOCK + j, 1, j)
    for j in range(2 * BLOCK):
        send((blocks - 2) * BLOCK + j)
    for group in range(groups - 2, groups):
        combine(group)
    others = batch - groups
    pltpu.make_async_copy(out.at[pl.ds(0, others)], out.at[pl.ds(0, others)], out_sem).wait()
    o_ref[...] = out[...]
    pltpu.make_async_copy(out.at[pl.ds(0, others)], out.at[pl.ds(0, others)], send_sem).wait()
    pltpu.make_async_copy(out.at[pl.ds(0, others)], out.at[pl.ds(0, others)], send_sem).wait()
    pltpu.make_async_copy(stat.at[pl.ds(0, others)], stat.at[pl.ds(0, others)], send_stat_sem).wait()


def solution(mesh):
    n = mesh.shape["sp"]

    def step(q, k, v):
        batch, heads, head = q.shape
        tokens = k.shape[1]
        k = k.reshape(batch, tokens, head)
        v = v.reshape(batch, tokens, head)
        groups = batch // n
        return pl.pallas_call(
            functools.partial(kernel, n, head ** -0.5),
            out_shape=jax.ShapeDtypeStruct(q.shape, BF16),
            in_specs=[pl.BlockSpec(memory_space=pltpu.HBM)] * 3,
            out_specs=pl.BlockSpec(memory_space=pltpu.VMEM),
            scratch_shapes=[
                pltpu.VMEM((batch, heads, head), BF16),
                pltpu.VMEM((batch, tokens, head), BF16),
                pltpu.VMEM((batch, tokens, head), BF16),
                [pltpu.VMEM((BLOCK, heads, tokens), F32)] * 2,
                pltpu.VMEM((batch, heads, head), F32),
                pltpu.VMEM((batch, heads, head), BF16),
                pltpu.VMEM((batch, 2, 128), F32),
                pltpu.VMEM((groups, n - 1, heads, head), BF16),
                pltpu.VMEM((groups, n - 1, 2, 128), F32),
                pltpu.VMEM((batch, heads, head), BF16),
                pltpu.SemaphoreType.DMA,
                pltpu.SemaphoreType.DMA((2 * AHEAD,)),
                pltpu.SemaphoreType.DMA((2 * AHEAD,)),
                pltpu.SemaphoreType.DMA,
                pltpu.SemaphoreType.DMA,
                pltpu.SemaphoreType.DMA((groups,)),
                pltpu.SemaphoreType.DMA((groups,)),
                pltpu.SemaphoreType.DMA,
            ],
            compiler_params=pltpu.CompilerParams(
                collective_id=0, has_side_effects=True, vmem_limit_bytes=67043328 - 320 * 1024),
            name="decode",
        )(q, k, v)

    return jax.shard_map(
        step,
        mesh=mesh,
        in_specs=(P("dp", None, None), P("dp", "sp", None, None), P("dp", "sp", None, None)),
        out_specs=P("dp", None, None),
        check_vma=False,
    )
```

```python
import functools

import jax
import jax.numpy as jnp
from jax import lax
from jax.experimental import pallas as pl
from jax.experimental.pallas import tpu as pltpu
from jax.sharding import PartitionSpec as P

MESH = pl.DeviceIdType.MESH
F32 = jnp.float32
BF16 = jnp.bfloat16
BLOCK = 2
PIECES = 2
AHEAD = 3


def kernel(n, scale, q_hbm, k_hbm, v_hbm, o_ref, q_buf, k_buf, v_buf, raw, part, sent, stat, got, got_stat, out,
           q_sem, k_sem, v_sem, send_sem, send_stat_sem, got_sem, got_stat_sem, out_sem):
    me = lax.axis_index("sp")
    batch, heads, head = q_buf.shape
    groups = batch // n
    blocks = batch // BLOCK

    def peer(r):
        return lax.rem(me + r, n)

    class Run:
        def __init__(self, hbm, buf, sem, b):
            self.hbm, self.buf, self.first, self.sem = hbm, buf, b * BLOCK, sem.at[lax.rem(b, 2 * AHEAD)]

        def start(self):
            rows = k_buf.shape[1] // PIECES
            for j in range(BLOCK):
                for p in range(PIECES):
                    at = (self.first + j, pl.ds(p * rows, rows))
                    pltpu.make_async_copy(self.hbm.at[at], self.buf.at[at], self.sem).start()

        def wait(self):
            run = self.buf.at[pl.ds(self.first, BLOCK)]
            pltpu.make_async_copy(run, run, self.sem).wait()

    k_copy = functools.partial(Run, k_hbm, k_buf, k_sem)
    v_copy = functools.partial(Run, v_hbm, v_buf, v_sem)

    q_copy = pltpu.make_async_copy(q_hbm, q_buf, q_sem)
    k_copy(0).start()
    q_copy.start()
    for b in range(AHEAD):
        if b > 0:
            k_copy(b).start()
        v_copy(b).start()

    barrier = pltpu.get_barrier_semaphore()
    for r in range(1, n):
        pl.semaphore_signal(barrier, inc=1, device_id={"sp": peer(r)}, device_id_type=MESH)

    def scores_of(s, parity, j):
        raw[parity][j] = lax.dot_general(q_buf[s], k_buf[s], (((1,), (1,)), ((), ())), preferred_element_type=F32)

    def finish(s, parity, j):
        scores = raw[parity][j]
        high = jnp.max(scores, -1, keepdims=True)
        weights = jnp.exp((scores - high) * scale)
        total = jnp.sum(weights, -1, keepdims=True)
        seen = jnp.dot(weights.astype(BF16), v_buf[s], preferred_element_type=F32)
        part[s] = seen
        sent[s] = seen.astype(BF16)
        lane = lax.broadcasted_iota(jnp.int32, (heads, 128), 1)
        both = jnp.where(lane == 0, high * scale, total)
        stat[s, :, :heads] = jnp.transpose(both)[:2]

    def send(s):
        owner = lax.rem(s, n)
        group = s // n
        slot = lax.rem(me - owner + n, n) - 1

        @pl.when(owner != me)
        def _():
            pltpu.make_async_remote_copy(
                src_ref=sent.at[s], dst_ref=got.at[group, slot], send_sem=send_sem, recv_sem=got_sem.at[group],
                device_id={"sp": owner}, device_id_type=MESH).start()
            pltpu.make_async_remote_copy(
                src_ref=stat.at[s], dst_ref=got_stat.at[group, slot], send_sem=send_stat_sem,
                recv_sem=got_stat_sem.at[group], device_id={"sp": owner}, device_id_type=MESH).start()

    def combine(group):
        s = group * n + me
        pltpu.make_async_copy(got.at[group], got.at[group], got_sem.at[group]).wait()
        pltpu.make_async_copy(got_stat.at[group], got_stat.at[group], got_stat_sem.at[group]).wait()
        stats = [stat[s]] + [got_stat[group, r] for r in range(n - 1)]
        high = functools.reduce(jnp.maximum, [x[:1] for x in stats])
        scales = [jnp.exp(x[:1] - high) for x in stats]
        total = functools.reduce(jnp.add, [w * x[1:] for w, x in zip(scales, stats)])
        rows = jnp.concatenate([w / total for w in scales], 0)
        columns = jnp.transpose(rows)[:heads]
        result = part[s] * columns[:, :1]
        for r in range(n - 1):
            result += got[group, r].astype(F32) * columns[:, r + 1:r + 2]
        out[s] = result.astype(BF16)
        for r in range(1, n):
            pltpu.make_async_remote_copy(
                src_ref=out.at[s], dst_ref=out.at[s], send_sem=send_sem, recv_sem=out_sem,
                device_id={"sp": peer(r)}, device_id_type=MESH).start()

    q_copy.wait()
    k_copy(0).wait()
    pl.semaphore_wait(barrier, n - 1)
    for j in range(BLOCK):
        scores_of(j, 0, j)

    def block(b, parity):
        k_copy(b).wait()
        v_copy(b - 1).wait()
        later = b + AHEAD - 1

        @pl.when(later < blocks)
        def _():
            k_copy(later).start()
            v_copy(later).start()

        @pl.when(b >= 2)
        def _():
            for j in range(BLOCK):
                send((b - 2) * BLOCK + j)

        for j in range(BLOCK):
            scores_of(b * BLOCK + j, parity, j)
        for j in range(BLOCK):
            finish((b - 1) * BLOCK + j, 1 - parity, j)

    per = n // BLOCK

    def pair(i, _):
        block(2 * i - 1, 1)
        block(2 * i, 0)

        @pl.when((lax.rem(2 * i, per) == 0) & (2 * i >= 2 * per))
        def _():
            combine(2 * i // per - 2)
        return 0

    lax.fori_loop(1, blocks // 2, pair, 0)
    block(blocks - 1, 1)
    v_copy(blocks - 1).wait()
    for j in range(BLOCK):
        finish((blocks - 1) * BLOCK + j, 1, j)
    for j in range(2 * BLOCK):
        send((blocks - 2) * BLOCK + j)
    for group in range(groups - 2, groups):
        combine(group)
    others = batch - groups
    pltpu.make_async_copy(out.at[pl.ds(0, others)], out.at[pl.ds(0, others)], out_sem).wait()
    o_ref[...] = out[...]
    pltpu.make_async_copy(out.at[pl.ds(0, others)], out.at[pl.ds(0, others)], send_sem).wait()
    pltpu.make_async_copy(out.at[pl.ds(0, others)], out.at[pl.ds(0, others)], send_sem).wait()
    pltpu.make_async_copy(stat.at[pl.ds(0, others)], stat.at[pl.ds(0, others)], send_stat_sem).wait()


def solution(mesh):
    n = mesh.shape["sp"]

    def step(q, k, v):
        batch, heads, head = q.shape
        tokens = k.shape[1]
        k = k.reshape(batch, tokens, head)
        v = v.reshape(batch, tokens, head)
        groups = batch // n
        return pl.pallas_call(
            functools.partial(kernel, n, head ** -0.5),
            out_shape=jax.ShapeDtypeStruct(q.shape, BF16),
            in_specs=[pl.BlockSpec(memory_space=pltpu.HBM)] * 3,
            out_specs=pl.BlockSpec(memory_space=pltpu.VMEM),
            scratch_shapes=[
                pltpu.VMEM((batch, heads, head), BF16),
                pltpu.VMEM((batch, tokens, head), BF16),
                pltpu.VMEM((batch, tokens, head), BF16),
                [pltpu.VMEM((BLOCK, heads, tokens), F32)] * 2,
                pltpu.VMEM((batch, heads, head), F32),
                pltpu.VMEM((batch, heads, head), BF16),
                pltpu.VMEM((batch, 2, 128), F32),
                pltpu.VMEM((groups, n - 1, heads, head), BF16),
                pltpu.VMEM((groups, n - 1, 2, 128), F32),
                pltpu.VMEM((batch, heads, head), BF16),
                pltpu.SemaphoreType.DMA,
                pltpu.SemaphoreType.DMA((2 * AHEAD,)),
                pltpu.SemaphoreType.DMA((2 * AHEAD,)),
                pltpu.SemaphoreType.DMA,
                pltpu.SemaphoreType.DMA,
                pltpu.SemaphoreType.DMA((groups,)),
                pltpu.SemaphoreType.DMA((groups,)),
                pltpu.SemaphoreType.DMA,
            ],
            compiler_params=pltpu.CompilerParams(
                collective_id=0, has_side_effects=True, vmem_limit_bytes=48 * 1024 * 1024),
            name="decode",
        )(pltpu.with_memory_space_constraint(q, pltpu.HBM), k, v)

    return jax.shard_map(
        step,
        mesh=mesh,
        in_specs=(P("dp", None, None), P("dp", "sp", None, None), P("dp", "sp", None, None)),
        out_specs=P("dp", None, None),
        check_vma=False,
    )
```

```python
import functools

import jax
import jax.numpy as jnp
from jax import lax
from jax.experimental import pallas as pl
from jax.experimental.pallas import tpu as pltpu
from jax.sharding import PartitionSpec as P

MESH = pl.DeviceIdType.MESH
F32 = jnp.float32
BF16 = jnp.bfloat16
BLOCK = 2
PIECES = 2
AHEAD = 5


def kernel(n, scale, q_hbm, k_hbm, v_hbm, o_ref, q_buf, k_buf, v_buf, raw, part, sent, stat, got, got_stat, out,
           q_sem, k_sem, v_sem, send_sem, send_stat_sem, got_sem, got_stat_sem, out_sem):
    me = lax.axis_index("sp")
    batch, heads, head = q_buf.shape
    groups = batch // n
    blocks = batch // BLOCK

    def peer(r):
        return lax.rem(me + r, n)

    class Run:
        def __init__(self, hbm, buf, sem, b):
            self.hbm, self.buf, self.first, self.sem = hbm, buf, b * BLOCK, sem.at[lax.rem(b, 2 * AHEAD)]

        def start(self):
            rows = k_buf.shape[1] // PIECES
            for j in range(BLOCK):
                for p in range(PIECES):
                    at = (self.first + j, pl.ds(p * rows, rows))
                    pltpu.make_async_copy(self.hbm.at[at], self.buf.at[at], self.sem).start()

        def wait(self):
            run = self.buf.at[pl.ds(self.first, BLOCK)]
            pltpu.make_async_copy(run, run, self.sem).wait()

    k_copy = functools.partial(Run, k_hbm, k_buf, k_sem)
    v_copy = functools.partial(Run, v_hbm, v_buf, v_sem)

    q_copy = pltpu.make_async_copy(q_hbm, q_buf, q_sem)
    k_copy(0).start()
    q_copy.start()
    for b in range(AHEAD):
        if b > 0:
            k_copy(b).start()
        v_copy(b).start()

    barrier = pltpu.get_barrier_semaphore()
    for r in range(1, n):
        pl.semaphore_signal(barrier, inc=1, device_id={"sp": peer(r)}, device_id_type=MESH)

    def scores_of(s, parity, j):
        raw[parity][j] = lax.dot_general(q_buf[s], k_buf[s], (((1,), (1,)), ((), ())), preferred_element_type=F32)

    def finish(s, parity, j):
        scores = raw[parity][j]
        high = jnp.max(scores, -1, keepdims=True)
        weights = jnp.exp((scores - high) * scale)
        total = jnp.sum(weights, -1, keepdims=True)
        seen = jnp.dot(weights.astype(BF16), v_buf[s], preferred_element_type=F32)
        part[s] = seen
        sent[s] = seen.astype(BF16)
        lane = lax.broadcasted_iota(jnp.int32, (heads, 128), 1)
        both = jnp.where(lane == 0, high * scale, total)
        stat[s, :, :heads] = jnp.transpose(both)[:2]

    def send(s):
        owner = lax.rem(s, n)
        group = s // n
        slot = lax.rem(me - owner + n, n) - 1

        @pl.when(owner != me)
        def _():
            pltpu.make_async_remote_copy(
                src_ref=sent.at[s], dst_ref=got.at[group, slot], send_sem=send_sem, recv_sem=got_sem.at[group],
                device_id={"sp": owner}, device_id_type=MESH).start()
            pltpu.make_async_remote_copy(
                src_ref=stat.at[s], dst_ref=got_stat.at[group, slot], send_sem=send_stat_sem,
                recv_sem=got_stat_sem.at[group], device_id={"sp": owner}, device_id_type=MESH).start()

    def combine(group):
        s = group * n + me
        pltpu.make_async_copy(got.at[group], got.at[group], got_sem.at[group]).wait()
        pltpu.make_async_copy(got_stat.at[group], got_stat.at[group], got_stat_sem.at[group]).wait()
        stats = [stat[s]] + [got_stat[group, r] for r in range(n - 1)]
        high = functools.reduce(jnp.maximum, [x[:1] for x in stats])
        scales = [jnp.exp(x[:1] - high) for x in stats]
        total = functools.reduce(jnp.add, [w * x[1:] for w, x in zip(scales, stats)])
        rows = jnp.concatenate([w / total for w in scales], 0)
        columns = jnp.transpose(rows)[:heads]
        result = part[s] * columns[:, :1]
        for r in range(n - 1):
            result += got[group, r].astype(F32) * columns[:, r + 1:r + 2]
        out[s] = result.astype(BF16)
        for r in range(1, n):
            pltpu.make_async_remote_copy(
                src_ref=out.at[s], dst_ref=out.at[s], send_sem=send_sem, recv_sem=out_sem,
                device_id={"sp": peer(r)}, device_id_type=MESH).start()

    q_copy.wait()
    k_copy(0).wait()
    pl.semaphore_wait(barrier, n - 1)
    for j in range(BLOCK):
        scores_of(j, 0, j)

    def block(b, parity):
        k_copy(b).wait()
        v_copy(b - 1).wait()
        later = b + AHEAD - 1

        @pl.when(later < blocks)
        def _():
            k_copy(later).start()
            v_copy(later).start()

        @pl.when(b >= 2)
        def _():
            for j in range(BLOCK):
                send((b - 2) * BLOCK + j)

        for j in range(BLOCK):
            scores_of(b * BLOCK + j, parity, j)
        for j in range(BLOCK):
            finish((b - 1) * BLOCK + j, 1 - parity, j)

    per = n // BLOCK

    def pair(i, _):
        block(2 * i - 1, 1)
        block(2 * i, 0)

        @pl.when((lax.rem(2 * i, per) == 0) & (2 * i >= 2 * per))
        def _():
            combine(2 * i // per - 2)
        return 0

    lax.fori_loop(1, blocks // 2, pair, 0)
    block(blocks - 1, 1)
    v_copy(blocks - 1).wait()
    for j in range(BLOCK):
        finish((blocks - 1) * BLOCK + j, 1, j)
    for j in range(2 * BLOCK):
        send((blocks - 2) * BLOCK + j)
    for group in range(groups - 2, groups):
        combine(group)
    others = batch - groups
    pltpu.make_async_copy(out.at[pl.ds(0, others)], out.at[pl.ds(0, others)], out_sem).wait()
    o_ref[...] = out[...]
    pltpu.make_async_copy(out.at[pl.ds(0, others)], out.at[pl.ds(0, others)], send_sem).wait()
    pltpu.make_async_copy(out.at[pl.ds(0, others)], out.at[pl.ds(0, others)], send_sem).wait()
    pltpu.make_async_copy(stat.at[pl.ds(0, others)], stat.at[pl.ds(0, others)], send_stat_sem).wait()


def solution(mesh):
    n = mesh.shape["sp"]

    def step(q, k, v):
        batch, heads, head = q.shape
        tokens = k.shape[1]
        k = k.reshape(batch, tokens, head)
        v = v.reshape(batch, tokens, head)
        groups = batch // n
        return pl.pallas_call(
            functools.partial(kernel, n, head ** -0.5),
            out_shape=jax.ShapeDtypeStruct(q.shape, BF16),
            in_specs=[pl.BlockSpec(memory_space=pltpu.HBM)] * 3,
            out_specs=pl.BlockSpec(memory_space=pltpu.VMEM),
            scratch_shapes=[
                pltpu.VMEM((batch, heads, head), BF16),
                pltpu.VMEM((batch, tokens, head), BF16),
                pltpu.VMEM((batch, tokens, head), BF16),
                [pltpu.VMEM((BLOCK, heads, tokens), F32)] * 2,
                pltpu.VMEM((batch, heads, head), F32),
                pltpu.VMEM((batch, heads, head), BF16),
                pltpu.VMEM((batch, 2, 128), F32),
                pltpu.VMEM((groups, n - 1, heads, head), BF16),
                pltpu.VMEM((groups, n - 1, 2, 128), F32),
                pltpu.VMEM((batch, heads, head), BF16),
                pltpu.SemaphoreType.DMA,
                pltpu.SemaphoreType.DMA((2 * AHEAD,)),
                pltpu.SemaphoreType.DMA((2 * AHEAD,)),
                pltpu.SemaphoreType.DMA,
                pltpu.SemaphoreType.DMA,
                pltpu.SemaphoreType.DMA((groups,)),
                pltpu.SemaphoreType.DMA((groups,)),
                pltpu.SemaphoreType.DMA,
            ],
            compiler_params=pltpu.CompilerParams(
                collective_id=0, has_side_effects=True, vmem_limit_bytes=48 * 1024 * 1024),
            name="decode",
        )(pltpu.with_memory_space_constraint(q, pltpu.HBM), k, v)

    return jax.shard_map(
        step,
        mesh=mesh,
        in_specs=(P("dp", None, None), P("dp", "sp", None, None), P("dp", "sp", None, None)),
        out_specs=P("dp", None, None),
        check_vma=False,
    )
```

```python
import functools

import jax
import jax.numpy as jnp
from jax import lax
from jax.experimental import pallas as pl
from jax.experimental.pallas import tpu as pltpu
from jax.sharding import PartitionSpec as P

MESH = pl.DeviceIdType.MESH
F32 = jnp.float32
BF16 = jnp.bfloat16
BLOCK = 2
PIECES = 2
AHEAD = 5
DIRECT = 3
CUTS = (0, 6, 10)
LANES = 128


def kernel(n, scale, q_hbm, k_hbm, v_hbm, o_ref, q_buf, k_buf, v_buf, raw0, raw1, part, other, mine, mine_stat, theirs,
           theirs_stat, out, q_sem, k_sem, v_sem, pair_send, pair_recv, acc_send, stat_send, acc_recv, stat_recv,
           direct_acc_recv, direct_stat_recv, direct_acc_recv2, direct_stat_recv2, out_send, out_recv):
    me = lax.axis_index("sp")
    chip, core = me // 2, lax.rem(me, 2)
    chips = n // 2
    batch, heads, head = q_buf.shape
    tokens = k_buf.shape[1]
    blocks = batch // BLOCK
    staged = blocks - DIRECT
    groups = list(zip(CUTS, CUTS[1:] + (staged,)))
    raw = (raw0, raw1)

    def device(r, same):
        return lax.rem(chip + r, chips) * 2 + (core if same else 1 - core)

    class Run:
        def __init__(self, hbm, buf, sem, b):
            self.hbm, self.buf, self.first, self.sem = hbm, buf, b * BLOCK, sem.at[lax.rem(b, 2 * AHEAD)]

        def start(self):
            rows = tokens // PIECES
            for j in range(BLOCK):
                for p in range(PIECES):
                    at = (self.first + j, pl.ds(p * rows, rows))
                    pltpu.make_async_copy(self.hbm.at[at], self.buf.at[at], self.sem).start()

        def wait(self):
            run = self.buf.at[pl.ds(self.first, BLOCK)]
            pltpu.make_async_copy(run, run, self.sem).wait()

    k_copy = functools.partial(Run, k_hbm, k_buf, k_sem)
    v_copy = functools.partial(Run, v_hbm, v_buf, v_sem)

    def wait(ref, sem):
        pltpu.make_async_copy(ref, ref, sem).wait()

    def remote(src, dst, send_sem, recv_sem, to):
        pltpu.make_async_remote_copy(src_ref=src, dst_ref=dst, send_sem=send_sem, recv_sem=recv_sem,
                                     device_id={"sp": to}, device_id_type=MESH).start()

    q_copy = pltpu.make_async_copy(q_hbm, q_buf, q_sem)
    k_copy(0).start()
    q_copy.start()
    for b in range(AHEAD):
        if b > 0:
            k_copy(b).start()
        v_copy(b).start()

    barrier = pltpu.get_barrier_semaphore()
    for r in range(1, n):
        pl.semaphore_signal(barrier, inc=1, device_id={"sp": lax.rem(me + r, n)}, device_id_type=MESH)

    lane = lax.broadcasted_iota(jnp.int32, (heads, LANES), 1)

    def scores_of(s, to):
        to[...] = lax.dot_general(q_buf[s], k_buf[s], (((1,), (1,)), ((), ())), preferred_element_type=F32)

    def finish(s, raw):
        scores = raw[...]
        high = jnp.max(scores, -1, keepdims=True)
        weights = jnp.exp((scores - high) * scale)
        total = jnp.sum(weights, -1, keepdims=True)
        part[s, :, :head] = jnp.dot(weights.astype(BF16), v_buf[s], preferred_element_type=F32)
        part[s, :, head:] = jnp.where(lane == 0, high * scale, total)

    def to_pair(t):
        remote(part.at[BLOCK * t + 1 - core], other.at[t], pair_send, pair_recv.at[lax.rem(t, 8)], device(0, False))

    def add_pair(t):
        a, b = part[BLOCK * t + core], other[t]
        high_a, high_b = a[:, head:head + 1], b[:, head:head + 1]
        high = jnp.maximum(high_a, high_b)
        scale_a, scale_b = jnp.exp(high_a - high), jnp.exp(high_b - high)
        total = scale_a * a[:, head + 1:head + 2] + scale_b * b[:, head + 1:head + 2]
        mine[t, chip] = (scale_a * a[:, :head] + scale_b * b[:, :head]).astype(BF16)
        mine_stat[t, chip, :, :heads] = jnp.transpose(jnp.where(lane == 0, high, total))[:2]

    def group_of(t):
        return sum((t >= cut).astype(jnp.int32) if not isinstance(t, int) else int(t >= cut) for cut in CUTS[1:])

    def to_chips(t):
        group = group_of(t)
        for r in range(1, chips):
            remote(mine.at[t, chip], mine.at[t, chip], acc_send, acc_recv.at[group], device(r, True))
            remote(mine_stat.at[t, chip], mine_stat.at[t, chip], stat_send, stat_recv.at[group], device(r, True))

    def to_all(t):
        d = t - staged
        for r in range(chips):
            if r > 0:
                remote(mine.at[t, chip], mine.at[t, chip], acc_send, direct_acc_recv.at[d], device(r, True))
                remote(mine_stat.at[t, chip], mine_stat.at[t, chip], stat_send, direct_stat_recv.at[d], device(r, True))
            remote(mine.at[t, chip], theirs.at[d, chip], acc_send, direct_acc_recv2.at[d], device(r, False))
            remote(mine_stat.at[t, chip], theirs_stat.at[d, chip], stat_send, direct_stat_recv2.at[d], device(r, False))

    def add_chips(work):
        rows = []
        for _, stat, _, _ in work:
            highs = [stat[c, 0:1] for c in range(chips)]
            totals = [stat[c, 1:2] for c in range(chips)]
            high = functools.reduce(jnp.maximum, highs)
            scales = [jnp.exp(x - high) for x in highs]
            total = functools.reduce(jnp.add, [w * x for w, x in zip(scales, totals)])
            rows += [w / total for w in scales]
        while len(rows) % 8:
            rows.append(rows[-1])
        columns = jnp.transpose(jnp.concatenate(rows, 0))[:heads]
        for i, (acc, _, t, j) in enumerate(work):
            terms = [acc[c].astype(F32) * columns[:, i * chips + c:i * chips + c + 1] for c in range(chips)]
            out[t, j] = functools.reduce(jnp.add, terms).astype(BF16)

    def add_group(g):
        first, last = groups[g]
        count = (last - first) * (chips - 1)
        flat = mine.at[pl.ds(0, count // (chips - 1)), pl.ds(0, chips - 1)]
        flat_stat = mine_stat.at[pl.ds(0, count // (chips - 1)), pl.ds(0, chips - 1)]
        wait(flat, acc_recv.at[g])
        wait(flat_stat, stat_recv.at[g])
        add_chips([(mine.at[t], mine_stat.at[t], t, core) for t in range(first, last)])
        run = pl.ds(first, last - first)
        remote(out.at[run, core], out.at[run, core], out_send, out_recv, device(0, False))

    def block(b):
        b, parity, first, last = b if isinstance(b, tuple) else (b, b % 2, b, b)
        if first < blocks:
            k_copy(b).wait()
        v_copy(b - 1).wait()
        if first >= 4:
            wait(other.at[0], pair_recv.at[lax.rem(b - 4, 8)])
        if first < blocks:
            later = b + AHEAD - 1
            if last + AHEAD - 1 < blocks:
                k_copy(later).start()
                v_copy(later).start()
            elif first + AHEAD - 1 < blocks:
                @pl.when(later < blocks)
                def _():
                    k_copy(later).start()
                    v_copy(later).start()
        if first == 2:
            pl.semaphore_wait(barrier, n - 1)
        if first >= 2:
            to_pair(b - 2)
        if first >= 5:
            to_chips(b - 5)
        if first < blocks:
            for j in range(BLOCK):
                scores_of(b * BLOCK + j, raw[parity].at[j])
        for j in range(BLOCK):
            finish((b - 1) * BLOCK + j, raw[1 - parity].at[j])
        if first >= 4:
            add_pair(b - 4)

    q_copy.wait()
    k_copy(0).wait()
    for j in range(BLOCK):
        scores_of(j, raw[0].at[j])
    for b in range(1, 5):
        block(b)

    def two(i, _):
        block((2 * i + 5, 1, 5, blocks - 2))
        block((2 * i + 6, 0, 5, blocks - 2))
        return 0

    lax.fori_loop(0, (blocks - 6) // 2, two, 0)
    block(blocks - 1)
    block(blocks)
    to_pair(blocks - 1)
    to_chips(blocks - 4)
    for t in range(blocks - 3, blocks):
        if t == blocks - 1:
            add_group(0)
        wait(other.at[0], pair_recv.at[t % 8])
        add_pair(t)
        to_all(t)
    for g in range(1, len(groups)):
        add_group(g)
    for d in range(DIRECT):
        wait(mine.at[0, pl.ds(0, chips - 1)], direct_acc_recv.at[d])
        wait(mine_stat.at[0, pl.ds(0, chips - 1)], direct_stat_recv.at[d])
        wait(mine.at[0], direct_acc_recv2.at[d])
        wait(mine_stat.at[0], direct_stat_recv2.at[d])
        t = staged + d
        add_chips([(mine.at[t], mine_stat.at[t], t, core), (theirs.at[d], theirs_stat.at[d], t, 1 - core)])
    wait(out.at[pl.ds(0, staged), 0], out_recv)
    for t in range(blocks):
        for j in range(BLOCK):
            o_ref[t * BLOCK + j] = out[t, j]
    wait(out.at[pl.ds(0, staged), 0], out_send)
    wait(part.at[pl.ds(0, blocks)], pair_send)
    sends = (staged * (chips - 1) + DIRECT * (n - 1)) // chips
    wait(mine.at[pl.ds(0, sends)], acc_send)
    wait(mine_stat.at[pl.ds(0, sends)], stat_send)


def solution(mesh):
    n = mesh.shape["sp"]

    def step(q, k, v):
        batch, heads, head = q.shape
        tokens = k.shape[1]
        k = k.reshape(batch, tokens, head)
        v = v.reshape(batch, tokens, head)
        blocks, chips = batch // BLOCK, n // 2
        dma = pltpu.SemaphoreType.DMA
        return pl.pallas_call(
            functools.partial(kernel, n, head ** -0.5),
            out_shape=jax.ShapeDtypeStruct(q.shape, BF16),
            in_specs=[pl.BlockSpec(memory_space=pltpu.HBM)] * 3,
            out_specs=pl.BlockSpec(memory_space=pltpu.VMEM),
            scratch_shapes=[
                pltpu.VMEM((batch, heads, head), BF16),
                pltpu.VMEM((batch, tokens, head), BF16),
                pltpu.VMEM((batch, tokens, head), BF16),
                pltpu.VMEM((BLOCK, heads, tokens), F32),
                pltpu.VMEM((BLOCK, heads, tokens), F32),
                pltpu.VMEM((batch, heads, head + LANES), F32),
                pltpu.VMEM((blocks, heads, head + LANES), F32),
                pltpu.VMEM((blocks, chips, heads, head), BF16),
                pltpu.VMEM((blocks, chips, 2, LANES), F32),
                pltpu.VMEM((DIRECT, chips, heads, head), BF16),
                pltpu.VMEM((DIRECT, chips, 2, LANES), F32),
                pltpu.VMEM((blocks, BLOCK, heads, head), BF16),
                dma, dma((2 * AHEAD,)), dma((2 * AHEAD,)),
                dma, dma((8,)),
                dma, dma, dma((len(CUTS),)), dma((len(CUTS),)),
                dma((DIRECT,)), dma((DIRECT,)), dma((DIRECT,)), dma((DIRECT,)),
                dma, dma,
            ],
            compiler_params=pltpu.CompilerParams(
                collective_id=0, has_side_effects=True, vmem_limit_bytes=48 * 1024 * 1024),
            name="decode",
        )(pltpu.with_memory_space_constraint(q, pltpu.HBM), k, v)

    return jax.shard_map(
        step,
        mesh=mesh,
        in_specs=(P("dp", None, None), P("dp", "sp", None, None), P("dp", "sp", None, None)),
        out_specs=P("dp", None, None),
        check_vma=False,
    )
```

```python
import functools

import jax
import jax.numpy as jnp
from jax import lax
from jax.experimental import pallas as pl
from jax.experimental.pallas import tpu as pltpu
from jax.sharding import PartitionSpec as P

MESH = pl.DeviceIdType.MESH
F32 = jnp.float32
BF16 = jnp.bfloat16
BLOCK = 2
PIECES = 2
AHEAD = 5
DIRECT = 1
CUTS = (0, 6, 10)
LANES = 128


def kernel(n, scale, q_hbm, k_hbm, v_hbm, o_ref, q_buf, k_buf, v_buf, raw0, raw1, part, other, mine, mine_stat, theirs,
           theirs_stat, out, q_sem, k_sem, v_sem, pair_send, pair_recv, acc_send, stat_send, acc_recv, stat_recv,
           direct_acc_recv, direct_stat_recv, direct_acc_recv2, direct_stat_recv2, out_send, out_recv):
    me = lax.axis_index("sp")
    chip, core = me // 2, lax.rem(me, 2)
    chips = n // 2
    batch, heads, head = q_buf.shape
    tokens = k_buf.shape[1]
    blocks = batch // BLOCK
    staged = blocks - DIRECT
    groups = list(zip(CUTS, CUTS[1:] + (staged,)))
    raw = (raw0, raw1)

    def device(r, same):
        return lax.rem(chip + r, chips) * 2 + (core if same else 1 - core)

    class Run:
        def __init__(self, hbm, buf, sem, b):
            self.hbm, self.buf, self.first, self.sem = hbm, buf, b * BLOCK, sem.at[lax.rem(b, 2 * AHEAD)]

        def start(self):
            rows = tokens // PIECES
            for j in range(BLOCK):
                for p in range(PIECES):
                    at = (self.first + j, pl.ds(p * rows, rows))
                    pltpu.make_async_copy(self.hbm.at[at], self.buf.at[at], self.sem).start()

        def wait(self):
            run = self.buf.at[pl.ds(self.first, BLOCK)]
            pltpu.make_async_copy(run, run, self.sem).wait()

    k_copy = functools.partial(Run, k_hbm, k_buf, k_sem)
    v_copy = functools.partial(Run, v_hbm, v_buf, v_sem)

    def wait(ref, sem):
        pltpu.make_async_copy(ref, ref, sem).wait()

    def remote(src, dst, send_sem, recv_sem, to):
        pltpu.make_async_remote_copy(src_ref=src, dst_ref=dst, send_sem=send_sem, recv_sem=recv_sem,
                                     device_id={"sp": to}, device_id_type=MESH).start()

    q_copy = pltpu.make_async_copy(q_hbm, q_buf, q_sem)
    k_copy(0).start()
    q_copy.start()
    for b in range(AHEAD):
        if b > 0:
            k_copy(b).start()
        v_copy(b).start()

    barrier = pltpu.get_barrier_semaphore()
    for r in range(1, n):
        pl.semaphore_signal(barrier, inc=1, device_id={"sp": lax.rem(me + r, n)}, device_id_type=MESH)

    lane = lax.broadcasted_iota(jnp.int32, (heads, LANES), 1)

    def scores_of(s, to):
        to[...] = lax.dot_general(q_buf[s], k_buf[s], (((1,), (1,)), ((), ())), preferred_element_type=F32)

    def finish(s, raw):
        scores = raw[...]
        high = jnp.max(scores, -1, keepdims=True)
        weights = jnp.exp((scores - high) * scale)
        total = jnp.sum(weights, -1, keepdims=True)
        part[s, :, :head] = jnp.dot(weights.astype(BF16), v_buf[s], preferred_element_type=F32)
        part[s, :, head:] = jnp.where(lane == 0, high * scale, total)

    def to_pair(t):
        remote(part.at[BLOCK * t + 1 - core], other.at[t], pair_send, pair_recv.at[lax.rem(t, 8)], device(0, False))

    def add_pair(t):
        a, b = part[BLOCK * t + core], other[t]
        high_a, high_b = a[:, head:head + 1], b[:, head:head + 1]
        high = jnp.maximum(high_a, high_b)
        scale_a, scale_b = jnp.exp(high_a - high), jnp.exp(high_b - high)
        total = scale_a * a[:, head + 1:head + 2] + scale_b * b[:, head + 1:head + 2]
        mine[t, chip] = (scale_a * a[:, :head] + scale_b * b[:, :head]).astype(BF16)
        mine_stat[t, chip, :, :heads] = jnp.transpose(jnp.where(lane == 0, high, total))[:2]

    def group_of(t):
        return sum((t >= cut).astype(jnp.int32) if not isinstance(t, int) else int(t >= cut) for cut in CUTS[1:])

    def to_chips(t):
        group = group_of(t)
        for r in range(1, chips):
            remote(mine.at[t, chip], mine.at[t, chip], acc_send, acc_recv.at[group], device(r, True))
            remote(mine_stat.at[t, chip], mine_stat.at[t, chip], stat_send, stat_recv.at[group], device(r, True))

    def to_all(t):
        d = t - staged
        for r in range(chips):
            if r > 0:
                remote(mine.at[t, chip], mine.at[t, chip], acc_send, direct_acc_recv.at[d], device(r, True))
                remote(mine_stat.at[t, chip], mine_stat.at[t, chip], stat_send, direct_stat_recv.at[d], device(r, True))
            remote(mine.at[t, chip], theirs.at[d, chip], acc_send, direct_acc_recv2.at[d], device(r, False))
            remote(mine_stat.at[t, chip], theirs_stat.at[d, chip], stat_send, direct_stat_recv2.at[d], device(r, False))

    def add_chips(work):
        rows = []
        for _, stat, _, _ in work:
            highs = [stat[c, 0:1] for c in range(chips)]
            totals = [stat[c, 1:2] for c in range(chips)]
            high = functools.reduce(jnp.maximum, highs)
            scales = [jnp.exp(x - high) for x in highs]
            total = functools.reduce(jnp.add, [w * x for w, x in zip(scales, totals)])
            rows += [w / total for w in scales]
        while len(rows) % 8:
            rows.append(rows[-1])
        columns = jnp.transpose(jnp.concatenate(rows, 0))[:heads]
        for i, (acc, _, t, j) in enumerate(work):
            terms = [acc[c].astype(F32) * columns[:, i * chips + c:i * chips + c + 1] for c in range(chips)]
            out[t, j] = functools.reduce(jnp.add, terms).astype(BF16)

    def add_group(g):
        first, last = groups[g]
        count = (last - first) * (chips - 1)
        flat = mine.at[pl.ds(0, count // (chips - 1)), pl.ds(0, chips - 1)]
        flat_stat = mine_stat.at[pl.ds(0, count // (chips - 1)), pl.ds(0, chips - 1)]
        wait(flat, acc_recv.at[g])
        wait(flat_stat, stat_recv.at[g])
        add_chips([(mine.at[t], mine_stat.at[t], t, core) for t in range(first, last)])
        run = pl.ds(first, last - first)
        remote(out.at[run, core], out.at[run, core], out_send, out_recv, device(0, False))

    def block(b):
        b, parity, first, last = b if isinstance(b, tuple) else (b, b % 2, b, b)
        if first < blocks:
            k_copy(b).wait()
        v_copy(b - 1).wait()
        if first >= 4:
            wait(other.at[0], pair_recv.at[lax.rem(b - 4, 8)])
        if first < blocks:
            later = b + AHEAD - 1
            if last + AHEAD - 1 < blocks:
                k_copy(later).start()
                v_copy(later).start()
            elif first + AHEAD - 1 < blocks:
                @pl.when(later < blocks)
                def _():
                    k_copy(later).start()
                    v_copy(later).start()
        if first == 2:
            pl.semaphore_wait(barrier, n - 1)
        if first >= 2:
            to_pair(b - 2)
        if first >= 5:
            to_chips(b - 5)
        if first < blocks:
            for j in range(BLOCK):
                scores_of(b * BLOCK + j, raw[parity].at[j])
        for j in range(BLOCK):
            finish((b - 1) * BLOCK + j, raw[1 - parity].at[j])
        if first >= 4:
            add_pair(b - 4)

    q_copy.wait()
    k_copy(0).wait()
    for j in range(BLOCK):
        scores_of(j, raw[0].at[j])
    for b in range(1, 5):
        block(b)

    def two(i, _):
        block((2 * i + 5, 1, 5, blocks - 2))
        block((2 * i + 6, 0, 5, blocks - 2))
        return 0

    lax.fori_loop(0, (blocks - 6) // 2, two, 0)
    block(blocks - 1)
    block(blocks)
    to_pair(blocks - 1)
    to_chips(blocks - 4)
    for t in range(blocks - 3, blocks):
        if t == blocks - 1:
            add_group(0)
        wait(other.at[0], pair_recv.at[t % 8])
        add_pair(t)
        (to_all if t >= staged else to_chips)(t)
    for g in range(1, len(groups)):
        add_group(g)
    for d in range(DIRECT):
        wait(mine.at[0, pl.ds(0, chips - 1)], direct_acc_recv.at[d])
        wait(mine_stat.at[0, pl.ds(0, chips - 1)], direct_stat_recv.at[d])
        wait(mine.at[0], direct_acc_recv2.at[d])
        wait(mine_stat.at[0], direct_stat_recv2.at[d])
        t = staged + d
        add_chips([(mine.at[t], mine_stat.at[t], t, core), (theirs.at[d], theirs_stat.at[d], t, 1 - core)])
    wait(out.at[pl.ds(0, staged), 0], out_recv)
    for t in range(blocks):
        for j in range(BLOCK):
            o_ref[t * BLOCK + j] = out[t, j]
    wait(out.at[pl.ds(0, staged), 0], out_send)
    wait(part.at[pl.ds(0, blocks)], pair_send)
    sends = (staged * (chips - 1) + DIRECT * (n - 1)) // chips
    wait(mine.at[pl.ds(0, sends)], acc_send)
    wait(mine_stat.at[pl.ds(0, sends)], stat_send)


def solution(mesh):
    n = mesh.shape["sp"]

    def step(q, k, v):
        batch, heads, head = q.shape
        tokens = k.shape[1]
        k = k.reshape(batch, tokens, head)
        v = v.reshape(batch, tokens, head)
        blocks, chips = batch // BLOCK, n // 2
        dma = pltpu.SemaphoreType.DMA
        return pl.pallas_call(
            functools.partial(kernel, n, head ** -0.5),
            out_shape=jax.ShapeDtypeStruct(q.shape, BF16),
            in_specs=[pl.BlockSpec(memory_space=pltpu.HBM)] * 3,
            out_specs=pl.BlockSpec(memory_space=pltpu.VMEM),
            scratch_shapes=[
                pltpu.VMEM((batch, heads, head), BF16),
                pltpu.VMEM((batch, tokens, head), BF16),
                pltpu.VMEM((batch, tokens, head), BF16),
                pltpu.VMEM((BLOCK, heads, tokens), F32),
                pltpu.VMEM((BLOCK, heads, tokens), F32),
                pltpu.VMEM((batch, heads, head + LANES), F32),
                pltpu.VMEM((blocks, heads, head + LANES), F32),
                pltpu.VMEM((blocks, chips, heads, head), BF16),
                pltpu.VMEM((blocks, chips, 2, LANES), F32),
                pltpu.VMEM((DIRECT, chips, heads, head), BF16),
                pltpu.VMEM((DIRECT, chips, 2, LANES), F32),
                pltpu.VMEM((blocks, BLOCK, heads, head), BF16),
                dma, dma((2 * AHEAD,)), dma((2 * AHEAD,)),
                dma, dma((8,)),
                dma, dma, dma((len(CUTS),)), dma((len(CUTS),)),
                dma((DIRECT,)), dma((DIRECT,)), dma((DIRECT,)), dma((DIRECT,)),
                dma, dma,
            ],
            compiler_params=pltpu.CompilerParams(
                collective_id=0, has_side_effects=True, vmem_limit_bytes=48 * 1024 * 1024),
            name="decode",
        )(pltpu.with_memory_space_constraint(q, pltpu.HBM), k, v)

    return jax.shard_map(
        step,
        mesh=mesh,
        in_specs=(P("dp", None, None), P("dp", "sp", None, None), P("dp", "sp", None, None)),
        out_specs=P("dp", None, None),
        check_vma=False,
    )
```

```python
import functools

import jax
import jax.numpy as jnp
from jax import lax
from jax.experimental import pallas as pl
from jax.experimental.pallas import tpu as pltpu
from jax.sharding import PartitionSpec as P

MESH = pl.DeviceIdType.MESH
F32 = jnp.float32
BF16 = jnp.bfloat16
BLOCK = 2
PIECES = 2
AHEAD = 5
DIRECT = 1
CUTS = (0, 6, 10)
LANES = 128


def kernel(n, scale, q_hbm, k_hbm, v_hbm, o_ref, q_buf, k_buf, v_buf, raw0, raw1, part, other, mine, mine_stat, theirs,
           theirs_stat, out, q_sem, k_sem, v_sem, pair_send, pair_recv, acc_send, stat_send, acc_recv, stat_recv,
           direct_acc_recv, direct_stat_recv, direct_acc_recv2, direct_stat_recv2, out_send, out_recv):
    me = lax.axis_index("sp")
    chip, core = me // 2, lax.rem(me, 2)
    chips = n // 2
    batch, heads, head = q_buf.shape
    tokens = k_buf.shape[1]
    blocks = batch // BLOCK
    staged = blocks - DIRECT
    groups = list(zip(CUTS, CUTS[1:] + (staged,)))
    raw = (raw0, raw1)

    def device(r, same):
        return lax.rem(chip + r, chips) * 2 + (core if same else 1 - core)

    class Run:
        def __init__(self, hbm, buf, sem, b):
            self.hbm, self.buf, self.first, self.sem = hbm, buf, b * BLOCK, sem.at[lax.rem(b, 2 * AHEAD)]

        def start(self):
            rows = tokens // PIECES
            for j in range(BLOCK):
                for p in range(PIECES):
                    at = (self.first + j, pl.ds(p * rows, rows))
                    pltpu.make_async_copy(self.hbm.at[at], self.buf.at[at], self.sem).start()

        def wait(self):
            run = self.buf.at[pl.ds(self.first, BLOCK)]
            pltpu.make_async_copy(run, run, self.sem).wait()

    k_copy = functools.partial(Run, k_hbm, k_buf, k_sem)
    v_copy = functools.partial(Run, v_hbm, v_buf, v_sem)

    def wait(ref, sem):
        pltpu.make_async_copy(ref, ref, sem).wait()

    def remote(src, dst, send_sem, recv_sem, to):
        pltpu.make_async_remote_copy(src_ref=src, dst_ref=dst, send_sem=send_sem, recv_sem=recv_sem,
                                     device_id={"sp": to}, device_id_type=MESH).start()

    q_copy = pltpu.make_async_copy(q_hbm, q_buf, q_sem)
    k_copy(0).start()
    q_copy.start()
    for b in range(AHEAD):
        if b > 0:
            k_copy(b).start()
        v_copy(b).start()

    barrier = pltpu.get_barrier_semaphore()
    for r in range(1, n):
        pl.semaphore_signal(barrier, inc=1, device_id={"sp": lax.rem(me + r, n)}, device_id_type=MESH)

    lane = lax.broadcasted_iota(jnp.int32, (heads, LANES), 1)

    def scores_of(s, to):
        to[...] = lax.dot_general(q_buf[s], k_buf[s], (((1,), (1,)), ((), ())), preferred_element_type=F32)

    def finish(s, raw):
        scores = raw[...]
        high = jnp.max(scores, -1, keepdims=True)
        weights = jnp.exp((scores - high) * scale)
        total = jnp.sum(weights, -1, keepdims=True)
        part[s, :, :head] = jnp.dot(weights.astype(BF16), v_buf[s], preferred_element_type=F32)
        part[s, :, head:head + LANES] = jnp.broadcast_to(high * scale, (heads, LANES))
        part[s, :, head + LANES:] = jnp.broadcast_to(total, (heads, LANES))

    def to_pair(t):
        remote(part.at[BLOCK * t + 1 - core], other.at[t], pair_send, pair_recv.at[lax.rem(t, 8)], device(0, False))

    def add_pair(t):
        a, b = part.at[BLOCK * t + core], other.at[t]
        high_a, high_b = a[:, head:head + LANES], b[:, head:head + LANES]
        high = jnp.maximum(high_a, high_b)
        scale_a, scale_b = jnp.exp(high_a - high), jnp.exp(high_b - high)
        total = scale_a * a[:, head + LANES:] + scale_b * b[:, head + LANES:]
        for at in range(0, head, LANES):
            run = slice(at, at + LANES)
            mine[t, chip, :, run] = (scale_a * a[:, run] + scale_b * b[:, run]).astype(BF16)
        both = jnp.where(lane == 0, high, total)
        mine_stat[t, chip, :, :chips * heads] = jnp.transpose(jnp.concatenate([both] * chips, 0))[:2]

    def group_of(t):
        return sum((t >= cut).astype(jnp.int32) if not isinstance(t, int) else int(t >= cut) for cut in CUTS[1:])

    def to_chips(t):
        group = group_of(t)
        for r in range(1, chips):
            remote(mine.at[t, chip], mine.at[t, chip], acc_send, acc_recv.at[group], device(r, True))
            remote(mine_stat.at[t, chip], mine_stat.at[t, chip], stat_send, stat_recv.at[group], device(r, True))

    def to_all(t):
        d = t - staged
        for r in range(chips):
            if r > 0:
                remote(mine.at[t, chip], mine.at[t, chip], acc_send, direct_acc_recv.at[d], device(r, True))
                remote(mine_stat.at[t, chip], mine_stat.at[t, chip], stat_send, direct_stat_recv.at[d], device(r, True))
            remote(mine.at[t, chip], theirs.at[d, chip], acc_send, direct_acc_recv2.at[d], device(r, False))
            remote(mine_stat.at[t, chip], theirs_stat.at[d, chip], stat_send, direct_stat_recv2.at[d], device(r, False))

    wide = chips * heads
    owner = lax.broadcasted_iota(jnp.int32, (1, wide), 1) // heads
    diagonal = lax.rem(lax.broadcasted_iota(jnp.int32, (heads, wide), 1), heads) == lax.broadcasted_iota(
        jnp.int32, (heads, wide), 0)

    def add_chips(work):
        for acc, stat, t, j in work:
            highs = [stat[c, 0:1, :wide] for c in range(chips)]
            totals = [stat[c, 1:2, :wide] for c in range(chips)]
            high = functools.reduce(jnp.maximum, highs)
            scales = [jnp.exp(x - high) for x in highs]
            total = functools.reduce(jnp.add, [w * x for w, x in zip(scales, totals)])
            row = scales[0]
            for c in range(1, chips):
                row = jnp.where(owner == c, scales[c], row)
            rest = jnp.where(diagonal, jnp.broadcast_to(row / total, (heads, wide)), 0.0)
            terms = []
            for _ in range(3):
                terms.append(rest.astype(BF16))
                rest = rest - terms[-1].astype(F32)
            sums = jnp.dot(jnp.concatenate(terms, 0), acc[...].reshape(wide, head), preferred_element_type=F32)
            out[t, j] = (sums[:heads] + (sums[heads:2 * heads] + sums[2 * heads:])).astype(BF16)

    def add_group(g):
        first, last = groups[g]
        count = (last - first) * (chips - 1)
        flat = mine.at[pl.ds(0, count // (chips - 1)), pl.ds(0, chips - 1)]
        flat_stat = mine_stat.at[pl.ds(0, count // (chips - 1)), pl.ds(0, chips - 1)]
        wait(flat, acc_recv.at[g])
        wait(flat_stat, stat_recv.at[g])
        add_chips([(mine.at[t], mine_stat.at[t], t, core) for t in range(first, last)])
        run = pl.ds(first, last - first)
        remote(out.at[run, core], out.at[run, core], out_send, out_recv, device(0, False))

    def block(b):
        b, parity, first, last = b if isinstance(b, tuple) else (b, b % 2, b, b)
        if first < blocks:
            k_copy(b).wait()
        v_copy(b - 1).wait()
        if first >= 4:
            wait(other.at[0], pair_recv.at[lax.rem(b - 4, 8)])
        if first < blocks:
            later = b + AHEAD - 1
            if last + AHEAD - 1 < blocks:
                k_copy(later).start()
                v_copy(later).start()
            elif first + AHEAD - 1 < blocks:
                @pl.when(later < blocks)
                def _():
                    k_copy(later).start()
                    v_copy(later).start()
        if first == 2:
            pl.semaphore_wait(barrier, n - 1)
        if first >= 2:
            to_pair(b - 2)
        if first >= 5:
            to_chips(b - 5)
        if first < blocks:
            for j in range(BLOCK):
                scores_of(b * BLOCK + j, raw[parity].at[j])
        for j in range(BLOCK):
            finish((b - 1) * BLOCK + j, raw[1 - parity].at[j])
        if first >= 4:
            add_pair(b - 4)

    q_copy.wait()
    k_copy(0).wait()
    for j in range(BLOCK):
        scores_of(j, raw[0].at[j])
    for b in range(1, 5):
        block(b)

    def two(i, _):
        block((2 * i + 5, 1, 5, blocks - 2))
        block((2 * i + 6, 0, 5, blocks - 2))
        return 0

    lax.fori_loop(0, (blocks - 6) // 2, two, 0)
    block(blocks - 1)
    block(blocks)
    to_pair(blocks - 1)
    to_chips(blocks - 4)
    for t in range(blocks - 3, blocks):
        if t == blocks - 1:
            add_group(0)
        wait(other.at[0], pair_recv.at[t % 8])
        add_pair(t)
        (to_all if t >= staged else to_chips)(t)
    for g in range(1, len(groups)):
        add_group(g)
    for d in range(DIRECT):
        wait(mine.at[0, pl.ds(0, chips - 1)], direct_acc_recv.at[d])
        wait(mine_stat.at[0, pl.ds(0, chips - 1)], direct_stat_recv.at[d])
        wait(mine.at[0], direct_acc_recv2.at[d])
        wait(mine_stat.at[0], direct_stat_recv2.at[d])
        t = staged + d
        add_chips([(mine.at[t], mine_stat.at[t], t, core), (theirs.at[d], theirs_stat.at[d], t, 1 - core)])
    wait(out.at[pl.ds(0, staged), 0], out_recv)
    for t in range(blocks):
        for j in range(BLOCK):
            o_ref[t * BLOCK + j] = out[t, j]
    wait(out.at[pl.ds(0, staged), 0], out_send)
    wait(part.at[pl.ds(0, blocks)], pair_send)
    sends = (staged * (chips - 1) + DIRECT * (n - 1)) // chips
    wait(mine.at[pl.ds(0, sends)], acc_send)
    wait(mine_stat.at[pl.ds(0, sends)], stat_send)


def solution(mesh):
    n = mesh.shape["sp"]

    def step(q, k, v):
        batch, heads, head = q.shape
        tokens = k.shape[1]
        k = k.reshape(batch, tokens, head)
        v = v.reshape(batch, tokens, head)
        blocks, chips = batch // BLOCK, n // 2
        dma = pltpu.SemaphoreType.DMA
        return pl.pallas_call(
            functools.partial(kernel, n, head ** -0.5),
            out_shape=jax.ShapeDtypeStruct(q.shape, BF16),
            in_specs=[pl.BlockSpec(memory_space=pltpu.HBM)] * 3,
            out_specs=pl.BlockSpec(memory_space=pltpu.VMEM),
            scratch_shapes=[
                pltpu.VMEM((batch, heads, head), BF16),
                pltpu.VMEM((batch, tokens, head), BF16),
                pltpu.VMEM((batch, tokens, head), BF16),
                pltpu.VMEM((BLOCK, heads, tokens), F32),
                pltpu.VMEM((BLOCK, heads, tokens), F32),
                pltpu.VMEM((batch, heads, head + 2 * LANES), F32),
                pltpu.VMEM((blocks, heads, head + 2 * LANES), F32),
                pltpu.VMEM((blocks, chips, heads, head), BF16),
                pltpu.VMEM((blocks, chips, 2, LANES), F32),
                pltpu.VMEM((DIRECT, chips, heads, head), BF16),
                pltpu.VMEM((DIRECT, chips, 2, LANES), F32),
                pltpu.VMEM((blocks, BLOCK, heads, head), BF16),
                dma, dma((2 * AHEAD,)), dma((2 * AHEAD,)),
                dma, dma((8,)),
                dma, dma, dma((len(CUTS),)), dma((len(CUTS),)),
                dma((DIRECT,)), dma((DIRECT,)), dma((DIRECT,)), dma((DIRECT,)),
                dma, dma,
            ],
            compiler_params=pltpu.CompilerParams(
                collective_id=0, has_side_effects=True, vmem_limit_bytes=48 * 1024 * 1024),
            name="decode",
        )(pltpu.with_memory_space_constraint(q, pltpu.HBM), k, v)

    return jax.shard_map(
        step,
        mesh=mesh,
        in_specs=(P("dp", None, None), P("dp", "sp", None, None), P("dp", "sp", None, None)),
        out_specs=P("dp", None, None),
        check_vma=False,
    )
```

```python
import functools

import jax
import jax.numpy as jnp
from jax import lax
from jax.experimental import pallas as pl
from jax.experimental.pallas import tpu as pltpu
from jax.sharding import PartitionSpec as P

MESH = pl.DeviceIdType.MESH
F32 = jnp.float32
BF16 = jnp.bfloat16
BLOCK = 2
PIECES = 2
AHEAD = 5
DIRECT = 1
LAG = 6
CUTS = (0, 6, 10)
LANES = 128


def kernel(n, scale, q_hbm, k_hbm, v_hbm, o_ref, q_buf, k_buf, v_buf, raw0, raw1, part, other, mine, mine_stat, theirs,
           theirs_stat, out, q_sem, k_sem, v_sem, pair_send, pair_recv, acc_send, stat_send, acc_recv, stat_recv,
           direct_acc_recv, direct_stat_recv, direct_acc_recv2, direct_stat_recv2, out_send, out_recv):
    me = lax.axis_index("sp")
    chip, core = me // 2, lax.rem(me, 2)
    chips = n // 2
    batch, heads, head = q_buf.shape
    tokens = k_buf.shape[1]
    blocks = batch // BLOCK
    staged = blocks - DIRECT
    groups = list(zip(CUTS, CUTS[1:] + (staged,)))
    raw = (raw0, raw1)

    def device(r, same):
        return lax.rem(chip + r, chips) * 2 + (core if same else 1 - core)

    class Run:
        def __init__(self, hbm, buf, sem, b):
            self.hbm, self.buf, self.first, self.sem = hbm, buf, b * BLOCK, sem.at[lax.rem(b, 2 * AHEAD)]

        def start(self):
            rows = tokens // PIECES
            for j in range(BLOCK):
                for p in range(PIECES):
                    at = (self.first + j, pl.ds(p * rows, rows))
                    pltpu.make_async_copy(self.hbm.at[at], self.buf.at[at], self.sem).start()

        def wait(self):
            run = self.buf.at[pl.ds(self.first, BLOCK)]
            pltpu.make_async_copy(run, run, self.sem).wait()

    k_copy = functools.partial(Run, k_hbm, k_buf, k_sem)
    v_copy = functools.partial(Run, v_hbm, v_buf, v_sem)

    def wait(ref, sem):
        pltpu.make_async_copy(ref, ref, sem).wait()

    def remote(src, dst, send_sem, recv_sem, to):
        pltpu.make_async_remote_copy(src_ref=src, dst_ref=dst, send_sem=send_sem, recv_sem=recv_sem,
                                     device_id={"sp": to}, device_id_type=MESH).start()

    q_copy = pltpu.make_async_copy(q_hbm, q_buf, q_sem)
    k_copy(0).start()
    q_copy.start()
    for b in range(AHEAD):
        if b > 0:
            k_copy(b).start()
        v_copy(b).start()

    barrier = pltpu.get_barrier_semaphore()
    for r in range(1, n):
        pl.semaphore_signal(barrier, inc=1, device_id={"sp": lax.rem(me + r, n)}, device_id_type=MESH)

    lane = lax.broadcasted_iota(jnp.int32, (heads, LANES), 1)

    def scores_of(s, to):
        to[...] = lax.dot_general(q_buf[s], k_buf[s], (((1,), (1,)), ((), ())), preferred_element_type=F32)

    def finish(s, raw):
        scores = raw[...]
        high = jnp.max(scores, -1, keepdims=True)
        weights = jnp.exp((scores - high) * scale)
        total = jnp.sum(weights, -1, keepdims=True)
        part[s, :, :head] = jnp.dot(weights.astype(BF16), v_buf[s], preferred_element_type=F32)
        part[s, :, head:head + LANES] = jnp.broadcast_to(high * scale, (heads, LANES))
        part[s, :, head + LANES:] = jnp.broadcast_to(total, (heads, LANES))

    def to_pair(t):
        remote(part.at[BLOCK * t + 1 - core], other.at[t], pair_send, pair_recv.at[t], device(0, False))

    def add_pair(t):
        a, b = part.at[BLOCK * t + core], other.at[t]
        high_a, high_b = a[:, head:head + LANES], b[:, head:head + LANES]
        high = jnp.maximum(high_a, high_b)
        scale_a, scale_b = jnp.exp(high_a - high), jnp.exp(high_b - high)
        total = scale_a * a[:, head + LANES:] + scale_b * b[:, head + LANES:]
        for at in range(0, head, LANES):
            run = slice(at, at + LANES)
            mine[t, chip, :, run] = (scale_a * a[:, run] + scale_b * b[:, run]).astype(BF16)
        both = jnp.where(lane == 0, high, total)
        mine_stat[t, chip, :, :chips * heads] = jnp.transpose(jnp.concatenate([both] * chips, 0))[:2]

    def group_of(t):
        return sum((t >= cut).astype(jnp.int32) if not isinstance(t, int) else int(t >= cut) for cut in CUTS[1:])

    def to_chips(t):
        group = group_of(t)
        for r in range(1, chips):
            remote(mine.at[t, chip], mine.at[t, chip], acc_send, acc_recv.at[group], device(r, True))
            remote(mine_stat.at[t, chip], mine_stat.at[t, chip], stat_send, stat_recv.at[group], device(r, True))

    def to_all(t):
        d = t - staged
        for r in range(chips):
            if r > 0:
                remote(mine.at[t, chip], mine.at[t, chip], acc_send, direct_acc_recv.at[d], device(r, True))
                remote(mine_stat.at[t, chip], mine_stat.at[t, chip], stat_send, direct_stat_recv.at[d], device(r, True))
            remote(mine.at[t, chip], theirs.at[d, chip], acc_send, direct_acc_recv2.at[d], device(r, False))
            remote(mine_stat.at[t, chip], theirs_stat.at[d, chip], stat_send, direct_stat_recv2.at[d], device(r, False))

    wide = chips * heads
    owner = lax.broadcasted_iota(jnp.int32, (1, wide), 1) // heads
    diagonal = lax.rem(lax.broadcasted_iota(jnp.int32, (heads, wide), 1), heads) == lax.broadcasted_iota(
        jnp.int32, (heads, wide), 0)

    def add_chips(work):
        for acc, stat, t, j in work:
            highs = [stat[c, 0:1, :wide] for c in range(chips)]
            totals = [stat[c, 1:2, :wide] for c in range(chips)]
            high = functools.reduce(jnp.maximum, highs)
            scales = [jnp.exp(x - high) for x in highs]
            total = functools.reduce(jnp.add, [w * x for w, x in zip(scales, totals)])
            row = scales[0]
            for c in range(1, chips):
                row = jnp.where(owner == c, scales[c], row)
            rest = jnp.where(diagonal, jnp.broadcast_to(row / total, (heads, wide)), 0.0)
            terms = []
            for _ in range(3):
                terms.append(rest.astype(BF16))
                rest = rest - terms[-1].astype(F32)
            sums = jnp.dot(jnp.concatenate(terms, 0), acc[...].reshape(wide, head), preferred_element_type=F32)
            out[t, j] = (sums[:heads] + (sums[heads:2 * heads] + sums[2 * heads:])).astype(BF16)

    def add_group(g):
        first, last = groups[g]
        count = (last - first) * (chips - 1)
        flat = mine.at[pl.ds(0, count // (chips - 1)), pl.ds(0, chips - 1)]
        flat_stat = mine_stat.at[pl.ds(0, count // (chips - 1)), pl.ds(0, chips - 1)]
        wait(flat, acc_recv.at[g])
        wait(flat_stat, stat_recv.at[g])
        add_chips([(mine.at[t], mine_stat.at[t], t, core) for t in range(first, last)])
        run = pl.ds(first, last - first)
        remote(out.at[run, core], out.at[run, core], out_send, out_recv, device(0, False))

    def block(b):
        b, parity, first, last = b if isinstance(b, tuple) else (b, b % 2, b, b)
        if first < blocks:
            k_copy(b).wait()
        v_copy(b - 1).wait()
        if first >= LAG:
            wait(other.at[0], pair_recv.at[b - LAG])
        if first < blocks:
            later = b + AHEAD - 1
            if last + AHEAD - 1 < blocks:
                k_copy(later).start()
                v_copy(later).start()
            elif first + AHEAD - 1 < blocks:
                @pl.when(later < blocks)
                def _():
                    k_copy(later).start()
                    v_copy(later).start()
        if first == 2:
            pl.semaphore_wait(barrier, n - 1)
        if first >= 2:
            to_pair(b - 2)
        if first > LAG:
            to_chips(b - LAG - 1)
        if first < blocks:
            for j in range(BLOCK):
                scores_of(b * BLOCK + j, raw[parity].at[j])
        for j in range(BLOCK):
            finish((b - 1) * BLOCK + j, raw[1 - parity].at[j])
        if first >= LAG:
            add_pair(b - LAG)

    q_copy.wait()
    k_copy(0).wait()
    for j in range(BLOCK):
        scores_of(j, raw[0].at[j])
    for b in range(1, LAG + 1):
        block(b)

    def two(i, _):
        block((2 * i + LAG + 1, 1, LAG + 1, blocks - 2))
        block((2 * i + LAG + 2, 0, LAG + 1, blocks - 2))
        return 0

    lax.fori_loop(0, (blocks - LAG - 2) // 2, two, 0)
    block(blocks - 1)
    block(blocks)
    to_pair(blocks - 1)
    to_chips(blocks - LAG)
    for t in range(blocks - LAG + 1, blocks):
        if t == blocks - 1:
            add_group(0)
        wait(other.at[0], pair_recv.at[t])
        add_pair(t)
        (to_all if t >= staged else to_chips)(t)
    for g in range(1, len(groups)):
        add_group(g)
    for d in range(DIRECT):
        wait(mine.at[0, pl.ds(0, chips - 1)], direct_acc_recv.at[d])
        wait(mine_stat.at[0, pl.ds(0, chips - 1)], direct_stat_recv.at[d])
        wait(mine.at[0], direct_acc_recv2.at[d])
        wait(mine_stat.at[0], direct_stat_recv2.at[d])
        t = staged + d
        add_chips([(mine.at[t], mine_stat.at[t], t, core), (theirs.at[d], theirs_stat.at[d], t, 1 - core)])
    wait(out.at[pl.ds(0, staged), 0], out_recv)
    for t in range(blocks):
        for j in range(BLOCK):
            o_ref[t * BLOCK + j] = out[t, j]
    wait(out.at[pl.ds(0, staged), 0], out_send)
    wait(part.at[pl.ds(0, blocks)], pair_send)
    sends = (staged * (chips - 1) + DIRECT * (n - 1)) // chips
    wait(mine.at[pl.ds(0, sends)], acc_send)
    wait(mine_stat.at[pl.ds(0, sends)], stat_send)


def solution(mesh):
    n = mesh.shape["sp"]

    def step(q, k, v):
        batch, heads, head = q.shape
        tokens = k.shape[1]
        k = k.reshape(batch, tokens, head)
        v = v.reshape(batch, tokens, head)
        blocks, chips = batch // BLOCK, n // 2
        dma = pltpu.SemaphoreType.DMA
        return pl.pallas_call(
            functools.partial(kernel, n, head ** -0.5),
            out_shape=jax.ShapeDtypeStruct(q.shape, BF16),
            in_specs=[pl.BlockSpec(memory_space=pltpu.HBM)] * 3,
            out_specs=pl.BlockSpec(memory_space=pltpu.VMEM),
            scratch_shapes=[
                pltpu.VMEM((batch, heads, head), BF16),
                pltpu.VMEM((batch, tokens, head), BF16),
                pltpu.VMEM((batch, tokens, head), BF16),
                pltpu.VMEM((BLOCK, heads, tokens), F32),
                pltpu.VMEM((BLOCK, heads, tokens), F32),
                pltpu.VMEM((batch, heads, head + 2 * LANES), F32),
                pltpu.VMEM((blocks, heads, head + 2 * LANES), F32),
                pltpu.VMEM((blocks, chips, heads, head), BF16),
                pltpu.VMEM((blocks, chips, 2, LANES), F32),
                pltpu.VMEM((DIRECT, chips, heads, head), BF16),
                pltpu.VMEM((DIRECT, chips, 2, LANES), F32),
                pltpu.VMEM((blocks, BLOCK, heads, head), BF16),
                dma, dma((2 * AHEAD,)), dma((2 * AHEAD,)),
                dma, dma((blocks,)),
                dma, dma, dma((len(CUTS),)), dma((len(CUTS),)),
                dma((DIRECT,)), dma((DIRECT,)), dma((DIRECT,)), dma((DIRECT,)),
                dma, dma,
            ],
            compiler_params=pltpu.CompilerParams(
                collective_id=0, has_side_effects=True, vmem_limit_bytes=48 * 1024 * 1024),
            name="decode",
        )(pltpu.with_memory_space_constraint(q, pltpu.HBM), k, v)

    return jax.shard_map(
        step,
        mesh=mesh,
        in_specs=(P("dp", None, None), P("dp", "sp", None, None), P("dp", "sp", None, None)),
        out_specs=P("dp", None, None),
        check_vma=False,
    )
```

```python
import functools

import jax
import jax.numpy as jnp
from jax import lax
from jax.experimental import pallas as pl
from jax.experimental.pallas import tpu as pltpu
from jax.sharding import PartitionSpec as P

MESH = pl.DeviceIdType.MESH
F32 = jnp.float32
BF16 = jnp.bfloat16
BLOCK = 2
PIECES = 2
AHEAD = 5
DIRECT = 3
CUTS = (0, 6, 10)
LANES = 128


def kernel(n, scale, q_hbm, k_hbm, v_hbm, out, q_buf, k_buf, v_buf, raw0, raw1, part, other, mine, mine_stat, theirs,
           theirs_stat, q_sem, k_sem, v_sem, pair_send, pair_recv, acc_send, stat_send, acc_recv, stat_recv,
           direct_acc_recv, direct_stat_recv, direct_acc_recv2, direct_stat_recv2, out_send, out_recv):
    me = lax.axis_index("sp")
    chip, core = me // 2, lax.rem(me, 2)
    chips = n // 2
    batch, heads, head = q_buf.shape
    tokens = k_buf.shape[1]
    blocks = batch // BLOCK
    staged = blocks - DIRECT
    groups = list(zip(CUTS, CUTS[1:] + (staged,)))
    raw = (raw0, raw1)

    def device(r, same):
        return lax.rem(chip + r, chips) * 2 + (core if same else 1 - core)

    class Run:
        def __init__(self, hbm, buf, sem, b):
            self.hbm, self.buf, self.first, self.sem = hbm, buf, b * BLOCK, sem.at[lax.rem(b, AHEAD)]

        def start(self):
            rows = tokens // PIECES
            for j in range(BLOCK):
                for p in range(PIECES):
                    at = (self.first + j, pl.ds(p * rows, rows))
                    pltpu.make_async_copy(self.hbm.at[at], self.buf.at[at], self.sem).start()

        def wait(self):
            run = self.buf.at[pl.ds(self.first, BLOCK)]
            pltpu.make_async_copy(run, run, self.sem).wait()

    k_copy = functools.partial(Run, k_hbm, k_buf, k_sem)
    v_copy = functools.partial(Run, v_hbm, v_buf, v_sem)

    def wait(ref, sem):
        pltpu.make_async_copy(ref, ref, sem).wait()

    def remote(src, dst, send_sem, recv_sem, to):
        pltpu.make_async_remote_copy(src_ref=src, dst_ref=dst, send_sem=send_sem, recv_sem=recv_sem,
                                     device_id={"sp": to}, device_id_type=MESH).start()

    q_copy = pltpu.make_async_copy(q_hbm, q_buf, q_sem)
    k_copy(0).start()
    q_copy.start()
    for b in range(AHEAD):
        if b > 0:
            k_copy(b).start()
        v_copy(b).start()

    barrier = pltpu.get_barrier_semaphore()
    for r in range(1, n):
        pl.semaphore_signal(barrier, inc=1, device_id={"sp": lax.rem(me + r, n)}, device_id_type=MESH)

    lane = lax.broadcasted_iota(jnp.int32, (heads, LANES), 1)

    def scores_of(s, to):
        to[...] = lax.dot_general(q_buf[s], k_buf[s], (((1,), (1,)), ((), ())), preferred_element_type=F32)

    def finish(s, raw):
        scores = raw[...]
        high = jnp.max(scores, -1, keepdims=True)
        weights = jnp.exp((scores - high) * scale)
        total = jnp.sum(weights, -1, keepdims=True)
        part[s, :, :head] = jnp.dot(weights.astype(BF16), v_buf[s], preferred_element_type=F32)
        part[s, :, head:head + LANES] = jnp.broadcast_to(high * scale, (heads, LANES))
        part[s, :, head + LANES:] = jnp.broadcast_to(total, (heads, LANES))

    def to_pair(t):
        remote(part.at[BLOCK * t + 1 - core], other.at[t], pair_send, pair_recv.at[lax.rem(t, 8)], device(0, False))

    def add_pair(t):
        a, b = part.at[BLOCK * t + core], other.at[t]
        high_a, high_b = a[:, head:head + LANES], b[:, head:head + LANES]
        high = jnp.maximum(high_a, high_b)
        scale_a, scale_b = jnp.exp(high_a - high), jnp.exp(high_b - high)
        total = scale_a * a[:, head + LANES:] + scale_b * b[:, head + LANES:]
        for at in range(0, head, LANES):
            run = slice(at, at + LANES)
            mine[t, chip, :, run] = (scale_a * a[:, run] + scale_b * b[:, run]).astype(BF16)
        both = jnp.where(lane == 0, high, total)
        return jnp.transpose(jnp.concatenate([both] * chips, 0))[:2]

    def keep_stat(t, rows):
        mine_stat[t, chip, :, :chips * heads] = rows

    def group_of(t):
        return sum((t >= cut).astype(jnp.int32) if not isinstance(t, int) else int(t >= cut) for cut in CUTS[1:])

    def to_chips(t):
        group = group_of(t)
        for r in range(1, chips):
            remote(mine.at[t, chip], mine.at[t, chip], acc_send, acc_recv.at[group], device(r, True))
            remote(mine_stat.at[t, chip], mine_stat.at[t, chip], stat_send, stat_recv.at[group], device(r, True))

    def acc_to_all(t):
        d = t - staged
        for r in reversed(range(chips)):
            remote(mine.at[t, chip], theirs.at[d, chip], acc_send, direct_acc_recv2.at[d], device(r, False))
            if r > 0:
                remote(mine.at[t, chip], mine.at[t, chip], acc_send, direct_acc_recv.at[d], device(r, True))

    def stat_to_all(t):
        d = t - staged
        for r in reversed(range(chips)):
            remote(mine_stat.at[t, chip], theirs_stat.at[d, chip], stat_send, direct_stat_recv2.at[d], device(r, False))
            if r > 0:
                remote(mine_stat.at[t, chip], mine_stat.at[t, chip], stat_send, direct_stat_recv.at[d], device(r, True))

    wide = chips * heads
    owner = lax.broadcasted_iota(jnp.int32, (1, wide), 1) // heads
    diagonal = lax.rem(lax.broadcasted_iota(jnp.int32, (heads, wide), 1), heads) == lax.broadcasted_iota(
        jnp.int32, (heads, wide), 0)

    def add_chips(work):
        for acc, stat, t, j in work:
            highs = [stat[c, 0:1, :wide] for c in range(chips)]
            totals = [stat[c, 1:2, :wide] for c in range(chips)]
            high = functools.reduce(jnp.maximum, highs)
            scales = [jnp.exp(x - high) for x in highs]
            total = functools.reduce(jnp.add, [w * x for w, x in zip(scales, totals)])
            row = scales[0]
            for c in range(1, chips):
                row = jnp.where(owner == c, scales[c], row)
            rest = jnp.where(diagonal, jnp.broadcast_to(row / total, (heads, wide)), 0.0)
            terms = []
            for _ in range(3):
                terms.append(rest.astype(BF16))
                rest = rest - terms[-1].astype(F32)
            sums = jnp.dot(jnp.concatenate(terms, 0), acc[...].reshape(wide, head), preferred_element_type=F32)
            out[t, j] = (sums[:heads] + (sums[heads:2 * heads] + sums[2 * heads:])).astype(BF16)

    def wait_group(g):
        first, last = groups[g]
        wait(mine.at[pl.ds(0, last - first), pl.ds(0, chips - 1)], acc_recv.at[g])
        wait(mine_stat.at[pl.ds(0, last - first), pl.ds(0, chips - 1)], stat_recv.at[g])

    def add_group(g):
        add_chips([(mine.at[t], mine_stat.at[t], t, core) for t in range(*groups[g])])

    def send_group(g):
        first, last = groups[g]
        run = pl.ds(first, last - first)
        remote(out.at[run, core], out.at[run, core], out_send, out_recv, device(0, False))

    def block(b):
        b, parity, first, last = b if isinstance(b, tuple) else (b, b % 2, b, b)
        if first < blocks:
            k_copy(b).wait()
        v_copy(b - 1).wait()
        if first >= 4:
            wait(other.at[0], pair_recv.at[lax.rem(b - 4, 8)])
        if first < blocks:
            later = b + AHEAD - 1
            if last + AHEAD - 1 < blocks:
                k_copy(later).start()
                v_copy(later).start()
            elif first + AHEAD - 1 < blocks:
                @pl.when(later < blocks)
                def _():
                    k_copy(later).start()
                    v_copy(later).start()
        if first == 2:
            pl.semaphore_wait(barrier, n - 1)
        if first >= 2:
            to_pair(b - 2)
        if first >= 5:
            to_chips(b - 5)
        if first < blocks:
            for j in range(BLOCK):
                scores_of(b * BLOCK + j, raw[parity].at[j])
        for j in range(BLOCK):
            finish((b - 1) * BLOCK + j, raw[1 - parity].at[j])
        if first >= 4:
            keep_stat(b - 4, add_pair(b - 4))

    q_copy.wait()
    k_copy(0).wait()
    for j in range(BLOCK):
        scores_of(j, raw[0].at[j])
    for b in range(1, 5):
        block(b)

    def two(i, _):
        block((2 * i + 5, 1, 5, blocks - 2))
        block((2 * i + 6, 0, 5, blocks - 2))
        return 0

    lax.fori_loop(0, (blocks - 6) // 2, two, 0)
    block(blocks - 1)
    block(blocks)
    to_pair(blocks - 1)
    to_chips(blocks - 4)
    for t in range(blocks - 3, blocks - 1):
        wait(other.at[0], pair_recv.at[t % 8])
    wait_group(0)
    for t in range(blocks - 3, blocks - 1):
        keep_stat(t, add_pair(t))
    add_group(0)
    for t in range(blocks - 3, blocks - 1):
        acc_to_all(t)
        stat_to_all(t)
    send_group(0)
    t = blocks - 1
    wait(other.at[0], pair_recv.at[t % 8])
    rows = add_pair(t)
    acc_to_all(t)
    keep_stat(t, rows)
    stat_to_all(t)
    for g in range(1, len(groups)):
        wait_group(g)
        add_group(g)
        send_group(g)
    for d in range(DIRECT):
        wait(mine.at[0, pl.ds(0, chips - 1)], direct_acc_recv.at[d])
        wait(mine_stat.at[0, pl.ds(0, chips - 1)], direct_stat_recv.at[d])
        wait(mine.at[0], direct_acc_recv2.at[d])
        wait(mine_stat.at[0], direct_stat_recv2.at[d])
        t = staged + d
        add_chips([(mine.at[t], mine_stat.at[t], t, core), (theirs.at[d], theirs_stat.at[d], t, 1 - core)])
    wait(out.at[pl.ds(0, staged), 0], out_recv)
    wait(out.at[pl.ds(0, staged), 0], out_send)
    wait(part.at[pl.ds(0, blocks)], pair_send)
    sends = (staged * (chips - 1) + DIRECT * (n - 1)) // chips
    wait(mine.at[pl.ds(0, sends)], acc_send)
    wait(mine_stat.at[pl.ds(0, sends)], stat_send)


def solution(mesh):
    n = mesh.shape["sp"]

    def step(q, k, v):
        batch, heads, head = q.shape
        tokens = k.shape[1]
        k = k.reshape(batch, tokens, head)
        v = v.reshape(batch, tokens, head)
        blocks, chips = batch // BLOCK, n // 2
        dma = pltpu.SemaphoreType.DMA
        return pl.pallas_call(
            functools.partial(kernel, n, head ** -0.5),
            out_shape=jax.ShapeDtypeStruct((blocks, BLOCK, heads, head), BF16),
            in_specs=[pl.BlockSpec(memory_space=pltpu.HBM)] * 3,
            out_specs=pl.BlockSpec(memory_space=pltpu.VMEM),
            scratch_shapes=[
                pltpu.VMEM((batch, heads, head), BF16),
                pltpu.VMEM((batch, tokens, head), BF16),
                pltpu.VMEM((batch, tokens, head), BF16),
                pltpu.VMEM((BLOCK, heads, tokens), F32),
                pltpu.VMEM((BLOCK, heads, tokens), F32),
                pltpu.VMEM((batch, heads, head + 2 * LANES), F32),
                pltpu.VMEM((blocks, heads, head + 2 * LANES), F32),
                pltpu.VMEM((blocks, chips, heads, head), BF16),
                pltpu.VMEM((blocks, chips, 2, LANES), F32),
                pltpu.VMEM((DIRECT, chips, heads, head), BF16),
                pltpu.VMEM((DIRECT, chips, 2, LANES), F32),
                dma, dma((AHEAD,)), dma((AHEAD,)),
                dma, dma((8,)),
                dma, dma, dma((len(CUTS),)), dma((len(CUTS),)),
                dma((DIRECT,)), dma((DIRECT,)), dma((DIRECT,)), dma((DIRECT,)),
                dma, dma,
            ],
            compiler_params=pltpu.CompilerParams(
                collective_id=0, has_side_effects=True, vmem_limit_bytes=48 * 1024 * 1024),
            name="decode",
        )(pltpu.with_memory_space_constraint(q, pltpu.HBM), k, v).reshape(q.shape)

    return jax.shard_map(
        step,
        mesh=mesh,
        in_specs=(P("dp", None, None), P("dp", "sp", None, None), P("dp", "sp", None, None)),
        out_specs=P("dp", None, None),
        check_vma=False,
    )
```

```python
import functools

import jax
import jax.numpy as jnp
from jax import lax
from jax.experimental import pallas as pl
from jax.experimental.pallas import tpu as pltpu
from jax.sharding import PartitionSpec as P

MESH = pl.DeviceIdType.MESH
F32 = jnp.float32
BF16 = jnp.bfloat16
BLOCK = 2
PIECES = 1
AHEAD = 6
DIRECT = 1
CUTS = (0, 6, 10)
LANES = 128


def kernel(n, scale, q_hbm, k_hbm, v_hbm, o_ref, q_buf, k_buf, v_buf, raw0, raw1, part, other, mine, mine_stat, theirs,
           theirs_stat, out, q_sem, k_sem, v_sem, pair_send, pair_recv, acc_send, stat_send, acc_recv, stat_recv,
           direct_acc_recv, direct_stat_recv, direct_acc_recv2, direct_stat_recv2, out_send, out_recv):
    me = lax.axis_index("sp")
    chip, core = me // 2, lax.rem(me, 2)
    chips = n // 2
    batch, heads, head = q_buf.shape
    tokens = k_buf.shape[1]
    blocks = batch // BLOCK
    staged = blocks - DIRECT
    groups = list(zip(CUTS, CUTS[1:] + (staged,)))
    raw = (raw0, raw1)

    def device(r, same):
        return lax.rem(chip + r, chips) * 2 + (core if same else 1 - core)

    class Run:
        def __init__(self, hbm, buf, sem, b):
            self.hbm, self.buf, self.first, self.sem = hbm, buf, b * BLOCK, sem.at[lax.rem(b, 2 * AHEAD)]

        def start(self):
            rows = tokens // PIECES
            for j in range(BLOCK):
                for p in range(PIECES):
                    at = (self.first + j, pl.ds(p * rows, rows))
                    pltpu.make_async_copy(self.hbm.at[at], self.buf.at[at], self.sem).start()

        def wait(self):
            run = self.buf.at[pl.ds(self.first, BLOCK)]
            pltpu.make_async_copy(run, run, self.sem).wait()

    k_copy = functools.partial(Run, k_hbm, k_buf, k_sem)
    v_copy = functools.partial(Run, v_hbm, v_buf, v_sem)

    def wait(ref, sem):
        pltpu.make_async_copy(ref, ref, sem).wait()

    def remote(src, dst, send_sem, recv_sem, to):
        pltpu.make_async_remote_copy(src_ref=src, dst_ref=dst, send_sem=send_sem, recv_sem=recv_sem,
                                     device_id={"sp": to}, device_id_type=MESH).start()

    q_copy = pltpu.make_async_copy(q_hbm, q_buf, q_sem)
    k_copy(0).start()
    q_copy.start()
    for b in range(AHEAD):
        if b > 0:
            k_copy(b).start()
        v_copy(b).start()

    barrier = pltpu.get_barrier_semaphore()
    for r in range(1, n):
        pl.semaphore_signal(barrier, inc=1, device_id={"sp": lax.rem(me + r, n)}, device_id_type=MESH)

    lane = lax.broadcasted_iota(jnp.int32, (heads, LANES), 1)

    def scores_of(s, to):
        to[...] = lax.dot_general(q_buf[s], k_buf[s], (((1,), (1,)), ((), ())), preferred_element_type=F32)

    def finish(s, raw):
        scores = raw[...]
        high = jnp.max(scores, -1, keepdims=True)
        weights = jnp.exp((scores - high) * scale)
        total = jnp.sum(weights, -1, keepdims=True)
        part[s, :, :head] = jnp.dot(weights.astype(BF16), v_buf[s], preferred_element_type=F32)
        part[s, :, head:head + LANES] = jnp.broadcast_to(high * scale, (heads, LANES))
        part[s, :, head + LANES:] = jnp.broadcast_to(total, (heads, LANES))

    def to_pair(t):
        remote(part.at[BLOCK * t + 1 - core], other.at[t], pair_send, pair_recv.at[lax.rem(t, 8)], device(0, False))

    def add_pair(t):
        a, b = part.at[BLOCK * t + core], other.at[t]
        high_a, high_b = a[:, head:head + LANES], b[:, head:head + LANES]
        high = jnp.maximum(high_a, high_b)
        scale_a, scale_b = jnp.exp(high_a - high), jnp.exp(high_b - high)
        total = scale_a * a[:, head + LANES:] + scale_b * b[:, head + LANES:]
        for at in range(0, head, LANES):
            run = slice(at, at + LANES)
            mine[t, chip, :, run] = (scale_a * a[:, run] + scale_b * b[:, run]).astype(BF16)
        both = jnp.where(lane == 0, high, total)
        mine_stat[t, chip, :, :chips * heads] = jnp.transpose(jnp.concatenate([both] * chips, 0))[:2]

    def group_of(t):
        return sum((t >= cut).astype(jnp.int32) if not isinstance(t, int) else int(t >= cut) for cut in CUTS[1:])

    def to_chips(t):
        group = group_of(t)
        for r in range(1, chips):
            remote(mine.at[t, chip], mine.at[t, chip], acc_send, acc_recv.at[group], device(r, True))
            remote(mine_stat.at[t, chip], mine_stat.at[t, chip], stat_send, stat_recv.at[group], device(r, True))

    def to_all(t):
        d = t - staged
        for r in range(chips):
            if r > 0:
                remote(mine.at[t, chip], mine.at[t, chip], acc_send, direct_acc_recv.at[d], device(r, True))
                remote(mine_stat.at[t, chip], mine_stat.at[t, chip], stat_send, direct_stat_recv.at[d], device(r, True))
            remote(mine.at[t, chip], theirs.at[d, chip], acc_send, direct_acc_recv2.at[d], device(r, False))
            remote(mine_stat.at[t, chip], theirs_stat.at[d, chip], stat_send, direct_stat_recv2.at[d], device(r, False))

    wide = chips * heads
    owner = lax.broadcasted_iota(jnp.int32, (1, wide), 1) // heads
    diagonal = lax.rem(lax.broadcasted_iota(jnp.int32, (heads, wide), 1), heads) == lax.broadcasted_iota(
        jnp.int32, (heads, wide), 0)

    def add_chips(work):
        for acc, stat, t, j in work:
            highs = [stat[c, 0:1, :wide] for c in range(chips)]
            totals = [stat[c, 1:2, :wide] for c in range(chips)]
            high = functools.reduce(jnp.maximum, highs)
            scales = [jnp.exp(x - high) for x in highs]
            total = functools.reduce(jnp.add, [w * x for w, x in zip(scales, totals)])
            row = scales[0]
            for c in range(1, chips):
                row = jnp.where(owner == c, scales[c], row)
            rest = jnp.where(diagonal, jnp.broadcast_to(row / total, (heads, wide)), 0.0)
            terms = []
            for _ in range(3):
                terms.append(rest.astype(BF16))
                rest = rest - terms[-1].astype(F32)
            sums = jnp.dot(jnp.concatenate(terms, 0), acc[...].reshape(wide, head), preferred_element_type=F32)
            out[t, j] = (sums[:heads] + (sums[heads:2 * heads] + sums[2 * heads:])).astype(BF16)

    def add_group(g):
        first, last = groups[g]
        count = (last - first) * (chips - 1)
        flat = mine.at[pl.ds(0, count // (chips - 1)), pl.ds(0, chips - 1)]
        flat_stat = mine_stat.at[pl.ds(0, count // (chips - 1)), pl.ds(0, chips - 1)]
        wait(flat, acc_recv.at[g])
        wait(flat_stat, stat_recv.at[g])
        add_chips([(mine.at[t], mine_stat.at[t], t, core) for t in range(first, last)])
        run = pl.ds(first, last - first)
        remote(out.at[run, core], out.at[run, core], out_send, out_recv, device(0, False))

    def block(b):
        b, parity, first, last = b if isinstance(b, tuple) else (b, b % 2, b, b)
        if first < blocks:
            k_copy(b).wait()
        v_copy(b - 1).wait()
        if first >= 4:
            wait(other.at[0], pair_recv.at[lax.rem(b - 4, 8)])
        if first < blocks:
            later = b + AHEAD - 1
            if last + AHEAD - 1 < blocks:
                k_copy(later).start()
                v_copy(later).start()
            elif first + AHEAD - 1 < blocks:
                @pl.when(later < blocks)
                def _():
                    k_copy(later).start()
                    v_copy(later).start()
        if first == 2:
            pl.semaphore_wait(barrier, n - 1)
        if first >= 2:
            to_pair(b - 2)
        if first >= 5:
            to_chips(b - 5)
        if first < blocks:
            for j in range(BLOCK):
                scores_of(b * BLOCK + j, raw[parity].at[j])
        for j in range(BLOCK):
            finish((b - 1) * BLOCK + j, raw[1 - parity].at[j])
        if first >= 4:
            add_pair(b - 4)

    q_copy.wait()
    k_copy(0).wait()
    for j in range(BLOCK):
        scores_of(j, raw[0].at[j])
    for b in range(1, 5):
        block(b)

    def two(i, _):
        block((2 * i + 5, 1, 5, blocks - 2))
        block((2 * i + 6, 0, 5, blocks - 2))
        return 0

    lax.fori_loop(0, (blocks - 6) // 2, two, 0)
    block(blocks - 1)
    block(blocks)
    to_pair(blocks - 1)
    to_chips(blocks - 4)
    for t in range(blocks - 3, blocks):
        if t == blocks - 1:
            add_group(0)
        wait(other.at[0], pair_recv.at[t % 8])
        add_pair(t)
        (to_all if t >= staged else to_chips)(t)
    for g in range(1, len(groups)):
        add_group(g)
    for d in range(DIRECT):
        wait(mine.at[0, pl.ds(0, chips - 1)], direct_acc_recv.at[d])
        wait(mine_stat.at[0, pl.ds(0, chips - 1)], direct_stat_recv.at[d])
        wait(mine.at[0], direct_acc_recv2.at[d])
        wait(mine_stat.at[0], direct_stat_recv2.at[d])
        t = staged + d
        add_chips([(mine.at[t], mine_stat.at[t], t, core), (theirs.at[d], theirs_stat.at[d], t, 1 - core)])
    wait(out.at[pl.ds(0, staged), 0], out_recv)
    for t in range(blocks):
        for j in range(BLOCK):
            o_ref[t * BLOCK + j] = out[t, j]
    wait(out.at[pl.ds(0, staged), 0], out_send)
    wait(part.at[pl.ds(0, blocks)], pair_send)
    sends = (staged * (chips - 1) + DIRECT * (n - 1)) // chips
    wait(mine.at[pl.ds(0, sends)], acc_send)
    wait(mine_stat.at[pl.ds(0, sends)], stat_send)


def solution(mesh):
    n = mesh.shape["sp"]

    def step(q, k, v):
        batch, heads, head = q.shape
        tokens = k.shape[1]
        k = k.reshape(batch, tokens, head)
        v = v.reshape(batch, tokens, head)
        blocks, chips = batch // BLOCK, n // 2
        dma = pltpu.SemaphoreType.DMA
        return pl.pallas_call(
            functools.partial(kernel, n, head ** -0.5),
            out_shape=jax.ShapeDtypeStruct(q.shape, BF16),
            in_specs=[pl.BlockSpec(memory_space=pltpu.HBM)] * 3,
            out_specs=pl.BlockSpec(memory_space=pltpu.VMEM),
            scratch_shapes=[
                pltpu.VMEM((batch, heads, head), BF16),
                pltpu.VMEM((batch, tokens, head), BF16),
                pltpu.VMEM((batch, tokens, head), BF16),
                pltpu.VMEM((BLOCK, heads, tokens), F32),
                pltpu.VMEM((BLOCK, heads, tokens), F32),
                pltpu.VMEM((batch, heads, head + 2 * LANES), F32),
                pltpu.VMEM((blocks, heads, head + 2 * LANES), F32),
                pltpu.VMEM((blocks, chips, heads, head), BF16),
                pltpu.VMEM((blocks, chips, 2, LANES), F32),
                pltpu.VMEM((DIRECT, chips, heads, head), BF16),
                pltpu.VMEM((DIRECT, chips, 2, LANES), F32),
                pltpu.VMEM((blocks, BLOCK, heads, head), BF16),
                dma, dma((2 * AHEAD,)), dma((2 * AHEAD,)),
                dma, dma((8,)),
                dma, dma, dma((len(CUTS),)), dma((len(CUTS),)),
                dma((DIRECT,)), dma((DIRECT,)), dma((DIRECT,)), dma((DIRECT,)),
                dma, dma,
            ],
            compiler_params=pltpu.CompilerParams(
                collective_id=0, has_side_effects=True, vmem_limit_bytes=48 * 1024 * 1024),
            name="decode",
        )(pltpu.with_memory_space_constraint(q, pltpu.HBM), k, v)

    return jax.shard_map(
        step,
        mesh=mesh,
        in_specs=(P("dp", None, None), P("dp", "sp", None, None), P("dp", "sp", None, None)),
        out_specs=P("dp", None, None),
        check_vma=False,
    )
```

```python
import functools

import jax
import jax.numpy as jnp
from jax import lax
from jax.experimental import pallas as pl
from jax.experimental.pallas import tpu as pltpu
from jax.sharding import PartitionSpec as P

MESH = pl.DeviceIdType.MESH
F32 = jnp.float32
BF16 = jnp.bfloat16
BLOCK = 2
PIECES = 2
AHEAD = 5
DIRECT = 1
CUTS = (0, 6, 10)
LANES = 128


def kernel(n, scale, q_hbm, k_hbm, v_hbm, out, q_buf, k_buf, v_buf, raw0, raw1, part, other, mine, mine_stat, theirs,
           theirs_stat, q_sem, k_sem, v_sem, pair_send, pair_recv, acc_send, stat_send, acc_recv, stat_recv,
           direct_acc_recv, direct_stat_recv, direct_acc_recv2, direct_stat_recv2, out_send, out_recv):
    me = lax.axis_index("sp")
    chip, core = me // 2, lax.rem(me, 2)
    chips = n // 2
    batch, heads, head = q_buf.shape
    tokens = k_buf.shape[1]
    blocks = batch // BLOCK
    staged = blocks - DIRECT
    groups = list(zip(CUTS, CUTS[1:] + (staged,)))
    raw = (raw0, raw1)

    def device(r, same):
        return lax.rem(chip + r, chips) * 2 + (core if same else 1 - core)

    class Run:
        def __init__(self, hbm, buf, sem, b):
            self.hbm, self.buf, self.first, self.sem = hbm, buf, b * BLOCK, sem.at[lax.rem(b, AHEAD)]

        def start(self):
            rows = tokens // PIECES
            for j in range(BLOCK):
                for p in range(PIECES):
                    at = (self.first + j, pl.ds(p * rows, rows))
                    pltpu.make_async_copy(self.hbm.at[at], self.buf.at[at], self.sem).start()

        def wait(self):
            run = self.buf.at[pl.ds(self.first, BLOCK)]
            pltpu.make_async_copy(run, run, self.sem).wait()

    k_copy = functools.partial(Run, k_hbm, k_buf, k_sem)
    v_copy = functools.partial(Run, v_hbm, v_buf, v_sem)

    def wait(ref, sem):
        pltpu.make_async_copy(ref, ref, sem).wait()

    def remote(src, dst, send_sem, recv_sem, to):
        pltpu.make_async_remote_copy(src_ref=src, dst_ref=dst, send_sem=send_sem, recv_sem=recv_sem,
                                     device_id={"sp": to}, device_id_type=MESH).start()

    q_copy = pltpu.make_async_copy(q_hbm, q_buf, q_sem)
    k_copy(0).start()
    q_copy.start()
    for b in range(AHEAD):
        if b > 0:
            k_copy(b).start()
        v_copy(b).start()

    barrier = pltpu.get_barrier_semaphore()
    for r in range(1, n):
        pl.semaphore_signal(barrier, inc=1, device_id={"sp": lax.rem(me + r, n)}, device_id_type=MESH)

    lane = lax.broadcasted_iota(jnp.int32, (heads, LANES), 1)

    def scores_of(s, to):
        to[...] = lax.dot_general(q_buf[s], k_buf[s], (((1,), (1,)), ((), ())), preferred_element_type=F32)

    def finish(s, raw):
        scores = raw[...]
        high = jnp.max(scores, -1, keepdims=True)
        weights = jnp.exp((scores - high) * scale)
        total = jnp.sum(weights, -1, keepdims=True)
        part[s, :, :head] = jnp.dot(weights.astype(BF16), v_buf[s], preferred_element_type=F32)
        part[s, :, head:head + LANES] = jnp.broadcast_to(high * scale, (heads, LANES))
        part[s, :, head + LANES:] = jnp.broadcast_to(total, (heads, LANES))

    def to_pair(t):
        remote(part.at[BLOCK * t + 1 - core], other.at[t], pair_send, pair_recv.at[lax.rem(t, 8)], device(0, False))

    def add_pair(t):
        a, b = part.at[BLOCK * t + core], other.at[t]
        high_a, high_b = a[:, head:head + LANES], b[:, head:head + LANES]
        high = jnp.maximum(high_a, high_b)
        scale_a, scale_b = jnp.exp(high_a - high), jnp.exp(high_b - high)
        total = scale_a * a[:, head + LANES:] + scale_b * b[:, head + LANES:]
        for at in range(0, head, LANES):
            run = slice(at, at + LANES)
            mine[t, chip, :, run] = (scale_a * a[:, run] + scale_b * b[:, run]).astype(BF16)
        both = jnp.where(lane == 0, high, total)
        return jnp.transpose(jnp.concatenate([both] * chips, 0))[:2]

    def keep_stat(t, rows):
        mine_stat[t, chip, :, :chips * heads] = rows

    def group_of(t):
        return sum((t >= cut).astype(jnp.int32) if not isinstance(t, int) else int(t >= cut) for cut in CUTS[1:])

    def to_chips(t):
        group = group_of(t)
        for r in range(1, chips):
            remote(mine.at[t, chip], mine.at[t, chip], acc_send, acc_recv.at[group], device(r, True))
            remote(mine_stat.at[t, chip], mine_stat.at[t, chip], stat_send, stat_recv.at[group], device(r, True))

    def acc_to_all(t):
        d = t - staged
        for r in reversed(range(chips)):
            remote(mine.at[t, chip], theirs.at[d, chip], acc_send, direct_acc_recv2.at[d], device(r, False))
            if r > 0:
                remote(mine.at[t, chip], mine.at[t, chip], acc_send, direct_acc_recv.at[d], device(r, True))

    def stat_to_all(t):
        d = t - staged
        for r in reversed(range(chips)):
            remote(mine_stat.at[t, chip], theirs_stat.at[d, chip], stat_send, direct_stat_recv2.at[d], device(r, False))
            if r > 0:
                remote(mine_stat.at[t, chip], mine_stat.at[t, chip], stat_send, direct_stat_recv.at[d], device(r, True))

    wide = chips * heads
    owner = lax.broadcasted_iota(jnp.int32, (1, wide), 1) // heads
    diagonal = lax.rem(lax.broadcasted_iota(jnp.int32, (heads, wide), 1), heads) == lax.broadcasted_iota(
        jnp.int32, (heads, wide), 0)

    def add_chips(work):
        for acc, stat, t, j in work:
            highs = [stat[c, 0:1, :wide] for c in range(chips)]
            totals = [stat[c, 1:2, :wide] for c in range(chips)]
            high = functools.reduce(jnp.maximum, highs)
            scales = [jnp.exp(x - high) for x in highs]
            total = functools.reduce(jnp.add, [w * x for w, x in zip(scales, totals)])
            row = scales[0]
            for c in range(1, chips):
                row = jnp.where(owner == c, scales[c], row)
            rest = jnp.where(diagonal, jnp.broadcast_to(row / total, (heads, wide)), 0.0)
            terms = []
            for _ in range(3):
                terms.append(rest.astype(BF16))
                rest = rest - terms[-1].astype(F32)
            sums = jnp.dot(jnp.concatenate(terms, 0), acc[...].reshape(wide, head), preferred_element_type=F32)
            out[t, j] = (sums[:heads] + (sums[heads:2 * heads] + sums[2 * heads:])).astype(BF16)

    def wait_group(g):
        first, last = groups[g]
        wait(mine.at[pl.ds(0, last - first), pl.ds(0, chips - 1)], acc_recv.at[g])
        wait(mine_stat.at[pl.ds(0, last - first), pl.ds(0, chips - 1)], stat_recv.at[g])

    def add_group(g):
        add_chips([(mine.at[t], mine_stat.at[t], t, core) for t in range(*groups[g])])

    def send_group(g):
        first, last = groups[g]
        run = pl.ds(first, last - first)
        remote(out.at[run, core], out.at[run, core], out_send, out_recv, device(0, False))

    def block(b):
        b, parity, first, last = b if isinstance(b, tuple) else (b, b % 2, b, b)
        if first < blocks:
            k_copy(b).wait()
        v_copy(b - 1).wait()
        if first >= 4:
            wait(other.at[0], pair_recv.at[lax.rem(b - 4, 8)])
        if first < blocks:
            later = b + AHEAD - 1
            if last + AHEAD - 1 < blocks:
                k_copy(later).start()
                v_copy(later).start()
            elif first + AHEAD - 1 < blocks:
                @pl.when(later < blocks)
                def _():
                    k_copy(later).start()
                    v_copy(later).start()
        if first == 2:
            pl.semaphore_wait(barrier, n - 1)
        if first >= 2:
            to_pair(b - 2)
        if first >= 5:
            to_chips(b - 5)
        if first < blocks:
            for j in range(BLOCK):
                scores_of(b * BLOCK + j, raw[parity].at[j])
        for j in range(BLOCK):
            finish((b - 1) * BLOCK + j, raw[1 - parity].at[j])
        if first >= 4:
            keep_stat(b - 4, add_pair(b - 4))

    q_copy.wait()
    k_copy(0).wait()
    for j in range(BLOCK):
        scores_of(j, raw[0].at[j])
    for b in range(1, 5):
        block(b)

    def two(i, _):
        block((2 * i + 5, 1, 5, blocks - 2))
        block((2 * i + 6, 0, 5, blocks - 2))
        return 0

    lax.fori_loop(0, (blocks - 6) // 2, two, 0)
    block(blocks - 1)
    block(blocks)
    to_pair(blocks - 1)
    to_chips(blocks - 4)
    for t in range(blocks - 3, blocks - 1):
        wait(other.at[0], pair_recv.at[t % 8])
    wait_group(0)
    for t in range(blocks - 3, blocks - 1):
        keep_stat(t, add_pair(t))
    add_group(0)
    for t in range(blocks - 3, blocks - 1):
        to_chips(t)
    send_group(0)
    t = blocks - 1
    wait(other.at[0], pair_recv.at[t % 8])
    rows = add_pair(t)
    acc_to_all(t)
    keep_stat(t, rows)
    stat_to_all(t)
    for g in range(1, len(groups)):
        wait_group(g)
        add_group(g)
        send_group(g)
    for d in range(DIRECT):
        wait(mine.at[0, pl.ds(0, chips - 1)], direct_acc_recv.at[d])
        wait(mine_stat.at[0, pl.ds(0, chips - 1)], direct_stat_recv.at[d])
        wait(mine.at[0], direct_acc_recv2.at[d])
        wait(mine_stat.at[0], direct_stat_recv2.at[d])
        t = staged + d
        add_chips([(mine.at[t], mine_stat.at[t], t, core), (theirs.at[d], theirs_stat.at[d], t, 1 - core)])
    wait(out.at[pl.ds(0, staged), 0], out_recv)
    wait(out.at[pl.ds(0, staged), 0], out_send)
    wait(part.at[pl.ds(0, blocks)], pair_send)
    sends = (staged * (chips - 1) + DIRECT * (n - 1)) // chips
    wait(mine.at[pl.ds(0, sends)], acc_send)
    wait(mine_stat.at[pl.ds(0, sends)], stat_send)


def solution(mesh):
    n = mesh.shape["sp"]

    def step(q, k, v):
        batch, heads, head = q.shape
        tokens = k.shape[1]
        k = k.reshape(batch, tokens, head)
        v = v.reshape(batch, tokens, head)
        blocks, chips = batch // BLOCK, n // 2
        dma = pltpu.SemaphoreType.DMA
        return pl.pallas_call(
            functools.partial(kernel, n, head ** -0.5),
            out_shape=jax.ShapeDtypeStruct((blocks, BLOCK, heads, head), BF16),
            in_specs=[pl.BlockSpec(memory_space=pltpu.HBM)] * 3,
            out_specs=pl.BlockSpec(memory_space=pltpu.VMEM),
            scratch_shapes=[
                pltpu.VMEM((batch, heads, head), BF16),
                pltpu.VMEM((batch, tokens, head), BF16),
                pltpu.VMEM((batch, tokens, head), BF16),
                pltpu.VMEM((BLOCK, heads, tokens), F32),
                pltpu.VMEM((BLOCK, heads, tokens), F32),
                pltpu.VMEM((batch, heads, head + 2 * LANES), F32),
                pltpu.VMEM((blocks, heads, head + 2 * LANES), F32),
                pltpu.VMEM((blocks, chips, heads, head), BF16),
                pltpu.VMEM((blocks, chips, 2, LANES), F32),
                pltpu.VMEM((DIRECT, chips, heads, head), BF16),
                pltpu.VMEM((DIRECT, chips, 2, LANES), F32),
                dma, dma((AHEAD,)), dma((AHEAD,)),
                dma, dma((8,)),
                dma, dma, dma((len(CUTS),)), dma((len(CUTS),)),
                dma((DIRECT,)), dma((DIRECT,)), dma((DIRECT,)), dma((DIRECT,)),
                dma, dma,
            ],
            compiler_params=pltpu.CompilerParams(
                collective_id=0, has_side_effects=True, vmem_limit_bytes=48 * 1024 * 1024),
            name="decode",
        )(pltpu.with_memory_space_constraint(q, pltpu.HBM), k, v).reshape(q.shape)

    return jax.shard_map(
        step,
        mesh=mesh,
        in_specs=(P("dp", None, None), P("dp", "sp", None, None), P("dp", "sp", None, None)),
        out_specs=P("dp", None, None),
        check_vma=False,
    )
```

```python
import functools

import jax
import jax.numpy as jnp
from jax import lax
from jax.experimental import pallas as pl
from jax.experimental.pallas import tpu as pltpu
from jax.sharding import PartitionSpec as P

MESH = pl.DeviceIdType.MESH
F32 = jnp.float32
BF16 = jnp.bfloat16
BLOCK = 2
PIECES = 2
AHEAD = 5
DIRECT = 1
CUTS = (0, 6, 10)
LANES = 128


def kernel(n, scale, q_hbm, k_hbm, v_hbm, out, q_buf, k_buf, v_buf, raw0, raw1, part, other, mine, mine_stat, theirs,
           theirs_stat, q_sem, k_sem, v_sem, pair_send, pair_recv, acc_send, stat_send, acc_recv, stat_recv,
           direct_acc_recv, direct_stat_recv, direct_acc_recv2, direct_stat_recv2, out_send, out_recv):
    me = lax.axis_index("sp")
    chip, core = me // 2, lax.rem(me, 2)
    chips = n // 2
    batch, heads, head = q_buf.shape
    tokens = k_buf.shape[1]
    blocks = batch // BLOCK
    staged = blocks - DIRECT
    groups = list(zip(CUTS, CUTS[1:] + (staged,)))
    raw = (raw0, raw1)

    def device(r, same):
        return lax.rem(chip + r, chips) * 2 + (core if same else 1 - core)

    class Run:
        def __init__(self, hbm, buf, sem, b):
            self.hbm, self.buf, self.first, self.sem = hbm, buf, b * BLOCK, sem.at[lax.rem(b, AHEAD)]

        def start(self):
            rows = tokens // PIECES
            for j in range(BLOCK):
                for p in range(PIECES):
                    at = (self.first + j, pl.ds(p * rows, rows))
                    pltpu.make_async_copy(self.hbm.at[at], self.buf.at[at], self.sem).start()

        def wait(self):
            run = self.buf.at[pl.ds(self.first, BLOCK)]
            pltpu.make_async_copy(run, run, self.sem).wait()

    k_copy = functools.partial(Run, k_hbm, k_buf, k_sem)
    v_copy = functools.partial(Run, v_hbm, v_buf, v_sem)

    def wait(ref, sem):
        pltpu.make_async_copy(ref, ref, sem).wait()

    def remote(src, dst, send_sem, recv_sem, to):
        pltpu.make_async_remote_copy(src_ref=src, dst_ref=dst, send_sem=send_sem, recv_sem=recv_sem,
                                     device_id={"sp": to}, device_id_type=MESH).start()

    q_copy = pltpu.make_async_copy(q_hbm, q_buf, q_sem)
    k_copy(0).start()
    q_copy.start()
    for b in range(AHEAD):
        if b > 0:
            k_copy(b).start()
        v_copy(b).start()

    barrier = pltpu.get_barrier_semaphore()
    for r in range(1, n):
        pl.semaphore_signal(barrier, inc=1, device_id={"sp": lax.rem(me + r, n)}, device_id_type=MESH)

    lane = lax.broadcasted_iota(jnp.int32, (heads, LANES), 1)

    def scores_of(s, to):
        to[...] = lax.dot_general(q_buf[s], k_buf[s], (((1,), (1,)), ((), ())), preferred_element_type=F32)

    def finish(s, raw):
        scores = raw[...]
        high = jnp.max(scores, -1, keepdims=True)
        weights = jnp.exp((scores - high) * scale)
        total = jnp.sum(weights, -1, keepdims=True)
        part[s, :, :head] = jnp.dot(weights.astype(BF16), v_buf[s], preferred_element_type=F32)
        part[s, :, head:head + LANES] = jnp.broadcast_to(high * scale, (heads, LANES))
        part[s, :, head + LANES:] = jnp.broadcast_to(total, (heads, LANES))

    def to_pair(t):
        remote(part.at[BLOCK * t + 1 - core], other.at[t], pair_send, pair_recv.at[lax.rem(t, 8)], device(0, False))

    def add_pair(t):
        a, b = part.at[BLOCK * t + core], other.at[t]
        high_a, high_b = a[:, head:head + LANES], b[:, head:head + LANES]
        high = jnp.maximum(high_a, high_b)
        scale_a, scale_b = jnp.exp(high_a - high), jnp.exp(high_b - high)
        total = scale_a * a[:, head + LANES:] + scale_b * b[:, head + LANES:]
        for at in range(0, head, LANES):
            run = slice(at, at + LANES)
            mine[t, chip, :, run] = (scale_a * a[:, run] + scale_b * b[:, run]).astype(BF16)
        both = jnp.where(lane == 0, high, total)
        mine_stat[t, chip, :, :chips * heads] = jnp.transpose(jnp.concatenate([both] * chips, 0))[:2]

    def group_of(t):
        return sum((t >= cut).astype(jnp.int32) if not isinstance(t, int) else int(t >= cut) for cut in CUTS[1:])

    def to_chips(t):
        group = group_of(t)
        for r in range(1, chips):
            remote(mine.at[t, chip], mine.at[t, chip], acc_send, acc_recv.at[group], device(r, True))
            remote(mine_stat.at[t, chip], mine_stat.at[t, chip], stat_send, stat_recv.at[group], device(r, True))

    def to_all(t):
        d = t - staged
        for r in range(chips):
            if r > 0:
                remote(mine.at[t, chip], mine.at[t, chip], acc_send, direct_acc_recv.at[d], device(r, True))
                remote(mine_stat.at[t, chip], mine_stat.at[t, chip], stat_send, direct_stat_recv.at[d], device(r, True))
            remote(mine.at[t, chip], theirs.at[d, chip], acc_send, direct_acc_recv2.at[d], device(r, False))
            remote(mine_stat.at[t, chip], theirs_stat.at[d, chip], stat_send, direct_stat_recv2.at[d], device(r, False))

    wide = chips * heads
    owner = lax.broadcasted_iota(jnp.int32, (1, wide), 1) // heads
    diagonal = lax.rem(lax.broadcasted_iota(jnp.int32, (heads, wide), 1), heads) == lax.broadcasted_iota(
        jnp.int32, (heads, wide), 0)

    def add_chips(work):
        for acc, stat, t, j in work:
            highs = [stat[c, 0:1, :wide] for c in range(chips)]
            totals = [stat[c, 1:2, :wide] for c in range(chips)]
            high = functools.reduce(jnp.maximum, highs)
            scales = [jnp.exp(x - high) for x in highs]
            total = functools.reduce(jnp.add, [w * x for w, x in zip(scales, totals)])
            row = scales[0]
            for c in range(1, chips):
                row = jnp.where(owner == c, scales[c], row)
            rest = jnp.where(diagonal, jnp.broadcast_to(row / total, (heads, wide)), 0.0)
            terms = []
            for _ in range(3):
                terms.append(rest.astype(BF16))
                rest = rest - terms[-1].astype(F32)
            sums = jnp.dot(jnp.concatenate(terms, 0), acc[...].reshape(wide, head), preferred_element_type=F32)
            out[t, j] = (sums[:heads] + (sums[heads:2 * heads] + sums[2 * heads:])).astype(BF16)

    def add_group(g):
        first, last = groups[g]
        count = (last - first) * (chips - 1)
        flat = mine.at[pl.ds(0, count // (chips - 1)), pl.ds(0, chips - 1)]
        flat_stat = mine_stat.at[pl.ds(0, count // (chips - 1)), pl.ds(0, chips - 1)]
        wait(flat, acc_recv.at[g])
        wait(flat_stat, stat_recv.at[g])
        add_chips([(mine.at[t], mine_stat.at[t], t, core) for t in range(first, last)])
        run = pl.ds(first, last - first)
        remote(out.at[run, core], out.at[run, core], out_send, out_recv, device(0, False))

    def block(b):
        b, parity, first, last = b if isinstance(b, tuple) else (b, b % 2, b, b)
        if first < blocks:
            k_copy(b).wait()
        v_copy(b - 1).wait()
        if first >= 4:
            wait(other.at[0], pair_recv.at[lax.rem(b - 4, 8)])
        if first < blocks:
            later = b + AHEAD - 1
            if last + AHEAD - 1 < blocks:
                k_copy(later).start()
                v_copy(later).start()
            elif first + AHEAD - 1 < blocks:
                @pl.when(later < blocks)
                def _():
                    k_copy(later).start()
                    v_copy(later).start()
        if first == 1:
            pl.semaphore_wait(barrier, n - 1)
        if first < blocks:
            for j in range(BLOCK):
                scores_of(b * BLOCK + j, raw[parity].at[j])
        for j in range(BLOCK):
            finish((b - 1) * BLOCK + j, raw[1 - parity].at[j])
        if first >= 4:
            add_pair(b - 4)
        to_pair(b - 1)
        if first >= 4:
            to_chips(b - 4)

    q_copy.wait()
    k_copy(0).wait()
    for j in range(BLOCK):
        scores_of(j, raw[0].at[j])
    for b in range(1, 5):
        block(b)

    def two(i, _):
        block((2 * i + 5, 1, 5, blocks - 2))
        block((2 * i + 6, 0, 5, blocks - 2))
        return 0

    lax.fori_loop(0, (blocks - 6) // 2, two, 0)
    block(blocks - 1)
    block(blocks)
    for t in range(blocks - 3, blocks):
        if t == blocks - 1:
            add_group(0)
        wait(other.at[0], pair_recv.at[t % 8])
        add_pair(t)
        (to_all if t >= staged else to_chips)(t)
    for g in range(1, len(groups)):
        add_group(g)
    for d in range(DIRECT):
        wait(mine.at[0, pl.ds(0, chips - 1)], direct_acc_recv.at[d])
        wait(mine_stat.at[0, pl.ds(0, chips - 1)], direct_stat_recv.at[d])
        wait(mine.at[0], direct_acc_recv2.at[d])
        wait(mine_stat.at[0], direct_stat_recv2.at[d])
        t = staged + d
        add_chips([(mine.at[t], mine_stat.at[t], t, core), (theirs.at[d], theirs_stat.at[d], t, 1 - core)])
    wait(out.at[pl.ds(0, staged), 0], out_recv)
    wait(out.at[pl.ds(0, staged), 0], out_send)
    wait(part.at[pl.ds(0, blocks)], pair_send)
    sends = (staged * (chips - 1) + DIRECT * (n - 1)) // chips
    wait(mine.at[pl.ds(0, sends)], acc_send)
    wait(mine_stat.at[pl.ds(0, sends)], stat_send)


def solution(mesh):
    n = mesh.shape["sp"]

    def step(q, k, v):
        batch, heads, head = q.shape
        tokens = k.shape[1]
        k = k.reshape(batch, tokens, head)
        v = v.reshape(batch, tokens, head)
        blocks, chips = batch // BLOCK, n // 2
        dma = pltpu.SemaphoreType.DMA
        return pl.pallas_call(
            functools.partial(kernel, n, head ** -0.5),
            out_shape=jax.ShapeDtypeStruct((blocks, BLOCK, heads, head), BF16),
            in_specs=[pl.BlockSpec(memory_space=pltpu.HBM)] * 3,
            out_specs=pl.BlockSpec(memory_space=pltpu.VMEM),
            scratch_shapes=[
                pltpu.VMEM((batch, heads, head), BF16),
                pltpu.VMEM((batch, tokens, head), BF16),
                pltpu.VMEM((batch, tokens, head), BF16),
                pltpu.VMEM((BLOCK, heads, tokens), F32),
                pltpu.VMEM((BLOCK, heads, tokens), F32),
                pltpu.VMEM((batch, heads, head + 2 * LANES), F32),
                pltpu.VMEM((blocks, heads, head + 2 * LANES), F32),
                pltpu.VMEM((blocks, chips, heads, head), BF16),
                pltpu.VMEM((blocks, chips, 2, LANES), F32),
                pltpu.VMEM((DIRECT, chips, heads, head), BF16),
                pltpu.VMEM((DIRECT, chips, 2, LANES), F32),
                dma, dma((AHEAD,)), dma((AHEAD,)),
                dma, dma((8,)),
                dma, dma, dma((len(CUTS),)), dma((len(CUTS),)),
                dma((DIRECT,)), dma((DIRECT,)), dma((DIRECT,)), dma((DIRECT,)),
                dma, dma,
            ],
            compiler_params=pltpu.CompilerParams(
                collective_id=0, has_side_effects=True, vmem_limit_bytes=48 * 1024 * 1024),
            name="decode",
        )(pltpu.with_memory_space_constraint(q, pltpu.HBM), k, v).reshape(q.shape)

    return jax.shard_map(
        step,
        mesh=mesh,
        in_specs=(P("dp", None, None), P("dp", "sp", None, None), P("dp", "sp", None, None)),
        out_specs=P("dp", None, None),
        check_vma=False,
    )
```

```python
import functools

import jax
import jax.numpy as jnp
from jax import lax
from jax.experimental import pallas as pl
from jax.experimental.pallas import tpu as pltpu
from jax.sharding import PartitionSpec as P

MESH = pl.DeviceIdType.MESH
F32 = jnp.float32
BF16 = jnp.bfloat16
BLOCK = 2
PIECES = 2
AHEAD = 5
DIRECT = 1
CUTS = (0, 6, 11, 13)
LANES = 128


def kernel(n, scale, q_hbm, k_hbm, v_hbm, out, q_buf, k_buf, v_buf, raw0, raw1, part, other, mine, mine_stat, theirs,
           theirs_stat, q_sem, k_sem, v_sem, pair_send, pair_recv, acc_send, stat_send, acc_recv, stat_recv,
           direct_acc_recv, direct_stat_recv, direct_acc_recv2, direct_stat_recv2, out_send, out_recv):
    me = lax.axis_index("sp")
    chip, core = me // 2, lax.rem(me, 2)
    chips = n // 2
    batch, heads, head = q_buf.shape
    tokens = k_buf.shape[1]
    blocks = batch // BLOCK
    staged = blocks - DIRECT
    groups = list(zip(CUTS, CUTS[1:] + (staged,)))
    raw = (raw0, raw1)

    def device(r, same):
        return lax.rem(chip + r, chips) * 2 + (core if same else 1 - core)

    class Run:
        def __init__(self, hbm, buf, sem, b):
            self.hbm, self.buf, self.first, self.sem = hbm, buf, b * BLOCK, sem.at[lax.rem(b, AHEAD)]

        def start(self):
            rows = tokens // PIECES
            for j in range(BLOCK):
                for p in range(PIECES):
                    at = (self.first + j, pl.ds(p * rows, rows))
                    pltpu.make_async_copy(self.hbm.at[at], self.buf.at[at], self.sem).start()

        def wait(self):
            run = self.buf.at[pl.ds(self.first, BLOCK)]
            pltpu.make_async_copy(run, run, self.sem).wait()

    k_copy = functools.partial(Run, k_hbm, k_buf, k_sem)
    v_copy = functools.partial(Run, v_hbm, v_buf, v_sem)

    def wait(ref, sem):
        pltpu.make_async_copy(ref, ref, sem).wait()

    def remote(src, dst, send_sem, recv_sem, to):
        pltpu.make_async_remote_copy(src_ref=src, dst_ref=dst, send_sem=send_sem, recv_sem=recv_sem,
                                     device_id={"sp": to}, device_id_type=MESH).start()

    q_copy = pltpu.make_async_copy(q_hbm, q_buf, q_sem)
    k_copy(0).start()
    q_copy.start()
    for b in range(AHEAD):
        if b > 0:
            k_copy(b).start()
        v_copy(b).start()

    barrier = pltpu.get_barrier_semaphore()
    for r in range(1, n):
        pl.semaphore_signal(barrier, inc=1, device_id={"sp": lax.rem(me + r, n)}, device_id_type=MESH)

    lane = lax.broadcasted_iota(jnp.int32, (heads, LANES), 1)

    def scores_of(s, to):
        to[...] = lax.dot_general(q_buf[s], k_buf[s], (((1,), (1,)), ((), ())), preferred_element_type=F32)

    def finish(s, raw):
        scores = raw[...]
        high = jnp.max(scores, -1, keepdims=True)
        weights = jnp.exp((scores - high) * scale)
        total = jnp.sum(weights, -1, keepdims=True)
        part[s, :, :head] = jnp.dot(weights.astype(BF16), v_buf[s], preferred_element_type=F32)
        part[s, :, head:head + LANES] = jnp.broadcast_to(high * scale, (heads, LANES))
        part[s, :, head + LANES:] = jnp.broadcast_to(total, (heads, LANES))

    def to_pair(t):
        remote(part.at[BLOCK * t + 1 - core], other.at[t], pair_send, pair_recv.at[lax.rem(t, 8)], device(0, False))

    def add_pair(t):
        a, b = part.at[BLOCK * t + core], other.at[t]
        high_a, high_b = a[:, head:head + LANES], b[:, head:head + LANES]
        high = jnp.maximum(high_a, high_b)
        scale_a, scale_b = jnp.exp(high_a - high), jnp.exp(high_b - high)
        total = scale_a * a[:, head + LANES:] + scale_b * b[:, head + LANES:]
        for at in range(0, head, LANES):
            run = slice(at, at + LANES)
            mine[t, chip, :, run] = (scale_a * a[:, run] + scale_b * b[:, run]).astype(BF16)
        both = jnp.where(lane == 0, high, total)
        mine_stat[t, chip, :, :chips * heads] = jnp.transpose(jnp.concatenate([both] * chips, 0))[:2]

    def group_of(t):
        return sum((t >= cut).astype(jnp.int32) if not isinstance(t, int) else int(t >= cut) for cut in CUTS[1:])

    def to_chips(t):
        group = group_of(t)
        for r in range(1, chips):
            remote(mine.at[t, chip], mine.at[t, chip], acc_send, acc_recv.at[group], device(r, True))
            remote(mine_stat.at[t, chip], mine_stat.at[t, chip], stat_send, stat_recv.at[group], device(r, True))

    def to_all(t):
        d = t - staged
        for r in range(chips):
            if r > 0:
                remote(mine.at[t, chip], mine.at[t, chip], acc_send, direct_acc_recv.at[d], device(r, True))
                remote(mine_stat.at[t, chip], mine_stat.at[t, chip], stat_send, direct_stat_recv.at[d], device(r, True))
            remote(mine.at[t, chip], theirs.at[d, chip], acc_send, direct_acc_recv2.at[d], device(r, False))
            remote(mine_stat.at[t, chip], theirs_stat.at[d, chip], stat_send, direct_stat_recv2.at[d], device(r, False))

    wide = chips * heads
    owner = lax.broadcasted_iota(jnp.int32, (1, wide), 1) // heads
    diagonal = lax.rem(lax.broadcasted_iota(jnp.int32, (heads, wide), 1), heads) == lax.broadcasted_iota(
        jnp.int32, (heads, wide), 0)

    def add_chips(work):
        for acc, stat, t, j in work:
            highs = [stat[c, 0:1, :wide] for c in range(chips)]
            totals = [stat[c, 1:2, :wide] for c in range(chips)]
            high = functools.reduce(jnp.maximum, highs)
            scales = [jnp.exp(x - high) for x in highs]
            total = functools.reduce(jnp.add, [w * x for w, x in zip(scales, totals)])
            row = scales[0]
            for c in range(1, chips):
                row = jnp.where(owner == c, scales[c], row)
            rest = jnp.where(diagonal, jnp.broadcast_to(row / total, (heads, wide)), 0.0)
            terms = []
            for _ in range(3):
                terms.append(rest.astype(BF16))
                rest = rest - terms[-1].astype(F32)
            sums = jnp.dot(jnp.concatenate(terms, 0), acc[...].reshape(wide, head), preferred_element_type=F32)
            out[t, j] = (sums[:heads] + (sums[heads:2 * heads] + sums[2 * heads:])).astype(BF16)

    def add_group(g):
        first, last = groups[g]
        count = (last - first) * (chips - 1)
        flat = mine.at[pl.ds(0, count // (chips - 1)), pl.ds(0, chips - 1)]
        flat_stat = mine_stat.at[pl.ds(0, count // (chips - 1)), pl.ds(0, chips - 1)]
        wait(flat, acc_recv.at[g])
        wait(flat_stat, stat_recv.at[g])
        add_chips([(mine.at[t], mine_stat.at[t], t, core) for t in range(first, last)])
        run = pl.ds(first, last - first)
        remote(out.at[run, core], out.at[run, core], out_send, out_recv, device(0, False))

    def block(b):
        b, parity, first, last = b if isinstance(b, tuple) else (b, b % 2, b, b)
        if first < blocks:
            k_copy(b).wait()
        v_copy(b - 1).wait()
        if first >= 4:
            wait(other.at[0], pair_recv.at[lax.rem(b - 4, 8)])
        if first < blocks:
            later = b + AHEAD - 1
            if last + AHEAD - 1 < blocks:
                k_copy(later).start()
                v_copy(later).start()
            elif first + AHEAD - 1 < blocks:
                @pl.when(later < blocks)
                def _():
                    k_copy(later).start()
                    v_copy(later).start()
        if first == 1:
            pl.semaphore_wait(barrier, n - 1)
        if first < blocks:
            for j in range(BLOCK):
                scores_of(b * BLOCK + j, raw[parity].at[j])
        for j in range(BLOCK):
            finish((b - 1) * BLOCK + j, raw[1 - parity].at[j])
        if first >= 4:
            add_pair(b - 4)
        to_pair(b - 1)
        if first >= 4:
            to_chips(b - 4)

    q_copy.wait()
    k_copy(0).wait()
    for j in range(BLOCK):
        scores_of(j, raw[0].at[j])
    for b in range(1, 5):
        block(b)

    def two(i, _):
        block((2 * i + 5, 1, 5, blocks - 2))
        block((2 * i + 6, 0, 5, blocks - 2))
        return 0

    lax.fori_loop(0, (blocks - 6) // 2, two, 0)
    block(blocks - 1)
    block(blocks)
    for t in range(blocks - 3, blocks):
        if t == blocks - 2:
            add_group(0)
        wait(other.at[0], pair_recv.at[t % 8])
        add_pair(t)
        (to_all if t >= staged else to_chips)(t)
    for g in range(1, len(groups)):
        add_group(g)
    for d in range(DIRECT):
        wait(mine.at[0, pl.ds(0, chips - 1)], direct_acc_recv.at[d])
        wait(mine_stat.at[0, pl.ds(0, chips - 1)], direct_stat_recv.at[d])
        wait(mine.at[0], direct_acc_recv2.at[d])
        wait(mine_stat.at[0], direct_stat_recv2.at[d])
        t = staged + d
        add_chips([(mine.at[t], mine_stat.at[t], t, core), (theirs.at[d], theirs_stat.at[d], t, 1 - core)])
    wait(out.at[pl.ds(0, staged), 0], out_recv)
    wait(out.at[pl.ds(0, staged), 0], out_send)
    wait(part.at[pl.ds(0, blocks)], pair_send)
    sends = (staged * (chips - 1) + DIRECT * (n - 1)) // chips
    wait(mine.at[pl.ds(0, sends)], acc_send)
    wait(mine_stat.at[pl.ds(0, sends)], stat_send)


def solution(mesh):
    n = mesh.shape["sp"]

    def step(q, k, v):
        batch, heads, head = q.shape
        tokens = k.shape[1]
        k = k.reshape(batch, tokens, head)
        v = v.reshape(batch, tokens, head)
        blocks, chips = batch // BLOCK, n // 2
        dma = pltpu.SemaphoreType.DMA
        return pl.pallas_call(
            functools.partial(kernel, n, head ** -0.5),
            out_shape=jax.ShapeDtypeStruct((blocks, BLOCK, heads, head), BF16),
            in_specs=[pl.BlockSpec(memory_space=pltpu.HBM)] * 3,
            out_specs=pl.BlockSpec(memory_space=pltpu.VMEM),
            scratch_shapes=[
                pltpu.VMEM((batch, heads, head), BF16),
                pltpu.VMEM((batch, tokens, head), BF16),
                pltpu.VMEM((batch, tokens, head), BF16),
                pltpu.VMEM((BLOCK, heads, tokens), F32),
                pltpu.VMEM((BLOCK, heads, tokens), F32),
                pltpu.VMEM((batch, heads, head + 2 * LANES), F32),
                pltpu.VMEM((blocks, heads, head + 2 * LANES), F32),
                pltpu.VMEM((blocks, chips, heads, head), BF16),
                pltpu.VMEM((blocks, chips, 2, LANES), F32),
                pltpu.VMEM((DIRECT, chips, heads, head), BF16),
                pltpu.VMEM((DIRECT, chips, 2, LANES), F32),
                dma, dma((AHEAD,)), dma((AHEAD,)),
                dma, dma((8,)),
                dma, dma, dma((len(CUTS),)), dma((len(CUTS),)),
                dma((DIRECT,)), dma((DIRECT,)), dma((DIRECT,)), dma((DIRECT,)),
                dma, dma,
            ],
            compiler_params=pltpu.CompilerParams(
                collective_id=0, has_side_effects=True, vmem_limit_bytes=48 * 1024 * 1024),
            name="decode",
        )(pltpu.with_memory_space_constraint(q, pltpu.HBM), k, v).reshape(q.shape)

    return jax.shard_map(
        step,
        mesh=mesh,
        in_specs=(P("dp", None, None), P("dp", "sp", None, None), P("dp", "sp", None, None)),
        out_specs=P("dp", None, None),
        check_vma=False,
    )
```

```python
import functools

import jax
import jax.numpy as jnp
from jax import lax
from jax.experimental import pallas as pl
from jax.experimental.pallas import tpu as pltpu
from jax.sharding import PartitionSpec as P

MESH = pl.DeviceIdType.MESH
F32 = jnp.float32
BF16 = jnp.bfloat16
BLOCK = 2
PIECES = 2
AHEAD = 5
DIRECT = 2
CUTS = (0, 6, 10, 13)
LANES = 128


def kernel(n, scale, q_hbm, k_hbm, v_hbm, out, q_buf, k_buf, v_buf, raw0, raw1, part, other, mine, mine_stat, theirs,
           theirs_stat, q_sem, k_sem, v_sem, pair_send, pair_recv, acc_send, stat_send, acc_recv, stat_recv,
           direct_acc_recv, direct_stat_recv, direct_acc_recv2, direct_stat_recv2, out_send, out_recv):
    me = lax.axis_index("sp")
    chip, core = me // 2, lax.rem(me, 2)
    chips = n // 2
    batch, heads, head = q_buf.shape
    tokens = k_buf.shape[1]
    blocks = batch // BLOCK
    staged = blocks - DIRECT
    groups = list(zip(CUTS, CUTS[1:] + (staged,)))
    raw = (raw0, raw1)

    def device(r, same):
        return lax.rem(chip + r, chips) * 2 + (core if same else 1 - core)

    class Run:
        def __init__(self, hbm, buf, sem, b):
            self.hbm, self.buf, self.first, self.sem = hbm, buf, b * BLOCK, sem.at[lax.rem(b, AHEAD)]

        def start(self):
            rows = tokens // PIECES
            for j in range(BLOCK):
                for p in range(PIECES):
                    at = (self.first + j, pl.ds(p * rows, rows))
                    pltpu.make_async_copy(self.hbm.at[at], self.buf.at[at], self.sem).start()

        def wait(self):
            run = self.buf.at[pl.ds(self.first, BLOCK)]
            pltpu.make_async_copy(run, run, self.sem).wait()

    k_copy = functools.partial(Run, k_hbm, k_buf, k_sem)
    v_copy = functools.partial(Run, v_hbm, v_buf, v_sem)

    def wait(ref, sem):
        pltpu.make_async_copy(ref, ref, sem).wait()

    def remote(src, dst, send_sem, recv_sem, to):
        pltpu.make_async_remote_copy(src_ref=src, dst_ref=dst, send_sem=send_sem, recv_sem=recv_sem,
                                     device_id={"sp": to}, device_id_type=MESH).start()

    q_copy = pltpu.make_async_copy(q_hbm, q_buf, q_sem)
    k_copy(0).start()
    q_copy.start()
    for b in range(AHEAD):
        if b > 0:
            k_copy(b).start()
        v_copy(b).start()

    barrier = pltpu.get_barrier_semaphore()
    for r in range(1, n):
        pl.semaphore_signal(barrier, inc=1, device_id={"sp": lax.rem(me + r, n)}, device_id_type=MESH)

    lane = lax.broadcasted_iota(jnp.int32, (heads, LANES), 1)

    def scores_of(s, to):
        to[...] = lax.dot_general(q_buf[s], k_buf[s], (((1,), (1,)), ((), ())), preferred_element_type=F32)

    def finish(s, raw):
        scores = raw[...]
        high = jnp.max(scores, -1, keepdims=True)
        weights = jnp.exp((scores - high) * scale)
        total = jnp.sum(weights, -1, keepdims=True)
        part[s, :, :head] = jnp.dot(weights.astype(BF16), v_buf[s], preferred_element_type=F32)
        part[s, :, head:head + LANES] = jnp.broadcast_to(high * scale, (heads, LANES))
        part[s, :, head + LANES:] = jnp.broadcast_to(total, (heads, LANES))

    def to_pair(t):
        remote(part.at[BLOCK * t + 1 - core], other.at[t], pair_send, pair_recv.at[lax.rem(t, 8)], device(0, False))

    def add_pair(t):
        a, b = part.at[BLOCK * t + core], other.at[t]
        high_a, high_b = a[:, head:head + LANES], b[:, head:head + LANES]
        high = jnp.maximum(high_a, high_b)
        scale_a, scale_b = jnp.exp(high_a - high), jnp.exp(high_b - high)
        total = scale_a * a[:, head + LANES:] + scale_b * b[:, head + LANES:]
        for at in range(0, head, LANES):
            run = slice(at, at + LANES)
            mine[t, chip, :, run] = (scale_a * a[:, run] + scale_b * b[:, run]).astype(BF16)
        both = jnp.where(lane == 0, high, total)
        mine_stat[t, chip, :, :chips * heads] = jnp.transpose(jnp.concatenate([both] * chips, 0))[:2]

    def group_of(t):
        return sum((t >= cut).astype(jnp.int32) if not isinstance(t, int) else int(t >= cut) for cut in CUTS[1:])

    def to_chips(t):
        group = group_of(t)
        for r in range(1, chips):
            remote(mine.at[t, chip], mine.at[t, chip], acc_send, acc_recv.at[group], device(r, True))
            remote(mine_stat.at[t, chip], mine_stat.at[t, chip], stat_send, stat_recv.at[group], device(r, True))

    def to_all(t):
        d = t - staged
        for r in range(chips):
            if r > 0:
                remote(mine.at[t, chip], mine.at[t, chip], acc_send, direct_acc_recv.at[d], device(r, True))
                remote(mine_stat.at[t, chip], mine_stat.at[t, chip], stat_send, direct_stat_recv.at[d], device(r, True))
            remote(mine.at[t, chip], theirs.at[d, chip], acc_send, direct_acc_recv2.at[d], device(r, False))
            remote(mine_stat.at[t, chip], theirs_stat.at[d, chip], stat_send, direct_stat_recv2.at[d], device(r, False))

    wide = chips * heads
    owner = lax.broadcasted_iota(jnp.int32, (1, wide), 1) // heads
    diagonal = lax.rem(lax.broadcasted_iota(jnp.int32, (heads, wide), 1), heads) == lax.broadcasted_iota(
        jnp.int32, (heads, wide), 0)

    def add_chips(work):
        for acc, stat, t, j in work:
            highs = [stat[c, 0:1, :wide] for c in range(chips)]
            totals = [stat[c, 1:2, :wide] for c in range(chips)]
            high = functools.reduce(jnp.maximum, highs)
            scales = [jnp.exp(x - high) for x in highs]
            total = functools.reduce(jnp.add, [w * x for w, x in zip(scales, totals)])
            row = scales[0]
            for c in range(1, chips):
                row = jnp.where(owner == c, scales[c], row)
            rest = jnp.where(diagonal, jnp.broadcast_to(row / total, (heads, wide)), 0.0)
            terms = []
            for _ in range(3):
                terms.append(rest.astype(BF16))
                rest = rest - terms[-1].astype(F32)
            sums = jnp.dot(jnp.concatenate(terms, 0), acc[...].reshape(wide, head), preferred_element_type=F32)
            out[t, j] = (sums[:heads] + (sums[heads:2 * heads] + sums[2 * heads:])).astype(BF16)

    def add_group(g):
        first, last = groups[g]
        count = (last - first) * (chips - 1)
        flat = mine.at[pl.ds(0, count // (chips - 1)), pl.ds(0, chips - 1)]
        flat_stat = mine_stat.at[pl.ds(0, count // (chips - 1)), pl.ds(0, chips - 1)]
        wait(flat, acc_recv.at[g])
        wait(flat_stat, stat_recv.at[g])
        add_chips([(mine.at[t], mine_stat.at[t], t, core) for t in range(first, last)])
        run = pl.ds(first, last - first)
        remote(out.at[run, core], out.at[run, core], out_send, out_recv, device(0, False))

    def block(b):
        b, parity, first, last = b if isinstance(b, tuple) else (b, b % 2, b, b)
        if first < blocks:
            k_copy(b).wait()
        v_copy(b - 1).wait()
        if first >= 4:
            wait(other.at[0], pair_recv.at[lax.rem(b - 4, 8)])
        if first < blocks:
            later = b + AHEAD - 1
            if last + AHEAD - 1 < blocks:
                k_copy(later).start()
                v_copy(later).start()
            elif first + AHEAD - 1 < blocks:
                @pl.when(later < blocks)
                def _():
                    k_copy(later).start()
                    v_copy(later).start()
        if first == 1:
            pl.semaphore_wait(barrier, n - 1)
        if first < blocks:
            for j in range(BLOCK):
                scores_of(b * BLOCK + j, raw[parity].at[j])
        for j in range(BLOCK):
            finish((b - 1) * BLOCK + j, raw[1 - parity].at[j])
        if first >= 4:
            add_pair(b - 4)
        to_pair(b - 1)
        if first >= 4:
            to_chips(b - 4)

    q_copy.wait()
    k_copy(0).wait()
    for j in range(BLOCK):
        scores_of(j, raw[0].at[j])
    for b in range(1, 5):
        block(b)

    def two(i, _):
        block((2 * i + 5, 1, 5, blocks - 2))
        block((2 * i + 6, 0, 5, blocks - 2))
        return 0

    lax.fori_loop(0, (blocks - 6) // 2, two, 0)
    block(blocks - 1)
    block(blocks)
    for t in range(blocks - 3, blocks):
        if t == blocks - 2:
            add_group(0)
        wait(other.at[0], pair_recv.at[t % 8])
        add_pair(t)
        (to_all if t >= staged else to_chips)(t)
    for g in range(1, len(groups)):
        add_group(g)
    for d in range(DIRECT):
        wait(mine.at[0, pl.ds(0, chips - 1)], direct_acc_recv.at[d])
        wait(mine_stat.at[0, pl.ds(0, chips - 1)], direct_stat_recv.at[d])
        wait(mine.at[0], direct_acc_recv2.at[d])
        wait(mine_stat.at[0], direct_stat_recv2.at[d])
        t = staged + d
        add_chips([(mine.at[t], mine_stat.at[t], t, core), (theirs.at[d], theirs_stat.at[d], t, 1 - core)])
    wait(out.at[pl.ds(0, staged), 0], out_recv)
    wait(out.at[pl.ds(0, staged), 0], out_send)
    wait(part.at[pl.ds(0, blocks)], pair_send)
    sends = (staged * (chips - 1) + DIRECT * (n - 1)) // chips
    wait(mine.at[pl.ds(0, sends)], acc_send)
    wait(mine_stat.at[pl.ds(0, sends)], stat_send)


def solution(mesh):
    n = mesh.shape["sp"]

    def step(q, k, v):
        batch, heads, head = q.shape
        tokens = k.shape[1]
        k = k.reshape(batch, tokens, head)
        v = v.reshape(batch, tokens, head)
        blocks, chips = batch // BLOCK, n // 2
        dma = pltpu.SemaphoreType.DMA
        return pl.pallas_call(
            functools.partial(kernel, n, head ** -0.5),
            out_shape=jax.ShapeDtypeStruct((blocks, BLOCK, heads, head), BF16),
            in_specs=[pl.BlockSpec(memory_space=pltpu.HBM)] * 3,
            out_specs=pl.BlockSpec(memory_space=pltpu.VMEM),
            scratch_shapes=[
                pltpu.VMEM((batch, heads, head), BF16),
                pltpu.VMEM((batch, tokens, head), BF16),
                pltpu.VMEM((batch, tokens, head), BF16),
                pltpu.VMEM((BLOCK, heads, tokens), F32),
                pltpu.VMEM((BLOCK, heads, tokens), F32),
                pltpu.VMEM((batch, heads, head + 2 * LANES), F32),
                pltpu.VMEM((blocks, heads, head + 2 * LANES), F32),
                pltpu.VMEM((blocks, chips, heads, head), BF16),
                pltpu.VMEM((blocks, chips, 2, LANES), F32),
                pltpu.VMEM((DIRECT, chips, heads, head), BF16),
                pltpu.VMEM((DIRECT, chips, 2, LANES), F32),
                dma, dma((AHEAD,)), dma((AHEAD,)),
                dma, dma((8,)),
                dma, dma, dma((len(CUTS),)), dma((len(CUTS),)),
                dma((DIRECT,)), dma((DIRECT,)), dma((DIRECT,)), dma((DIRECT,)),
                dma, dma,
            ],
            compiler_params=pltpu.CompilerParams(
                collective_id=0, has_side_effects=True, vmem_limit_bytes=48 * 1024 * 1024),
            name="decode",
        )(pltpu.with_memory_space_constraint(q, pltpu.HBM), k, v).reshape(q.shape)

    return jax.shard_map(
        step,
        mesh=mesh,
        in_specs=(P("dp", None, None), P("dp", "sp", None, None), P("dp", "sp", None, None)),
        out_specs=P("dp", None, None),
        check_vma=False,
    )
```

```python
import functools

import jax
import jax.numpy as jnp
from jax import lax
from jax.experimental import pallas as pl
from jax.experimental.pallas import tpu as pltpu
from jax.sharding import PartitionSpec as P

MESH = pl.DeviceIdType.MESH
F32 = jnp.float32
BF16 = jnp.bfloat16
BLOCK = 2
PIECES = 2
AHEAD = 5
DIRECT = 1
CUTS = (0, 6, 11, 13)
LANES = 128


def kernel(n, scale, q_hbm, k_hbm, v_hbm, out, q_buf, k_buf, v_buf, raw0, raw1, part, other, mine, mine_stat, theirs,
           theirs_stat, q_sem, k_sem, v_sem, pair_send, pair_recv, acc_send, stat_send, acc_recv, stat_recv,
           direct_acc_recv, direct_stat_recv, direct_acc_recv2, direct_stat_recv2, out_send, out_recv):
    me = lax.axis_index("sp")
    chip, core = me // 2, lax.rem(me, 2)
    chips = n // 2
    batch, heads, head = q_buf.shape
    tokens = k_buf.shape[1]
    blocks = batch // BLOCK
    staged = blocks - DIRECT
    groups = list(zip(CUTS, CUTS[1:] + (staged,)))
    raw = (raw0, raw1)

    def device(r, same):
        return lax.rem(chip + r, chips) * 2 + (core if same else 1 - core)

    class Run:
        def __init__(self, hbm, buf, sem, b):
            self.hbm, self.buf, self.first, self.sem = hbm, buf, b * BLOCK, sem.at[lax.rem(b, AHEAD)]

        def start(self):
            rows = tokens // PIECES
            for j in range(BLOCK):
                for p in range(PIECES):
                    at = (self.first + j, pl.ds(p * rows, rows))
                    pltpu.make_async_copy(self.hbm.at[at], self.buf.at[at], self.sem).start()

        def wait(self):
            run = self.buf.at[pl.ds(self.first, BLOCK)]
            pltpu.make_async_copy(run, run, self.sem).wait()

    k_copy = functools.partial(Run, k_hbm, k_buf, k_sem)
    v_copy = functools.partial(Run, v_hbm, v_buf, v_sem)

    def wait(ref, sem):
        pltpu.make_async_copy(ref, ref, sem).wait()

    def remote(src, dst, send_sem, recv_sem, to):
        pltpu.make_async_remote_copy(src_ref=src, dst_ref=dst, send_sem=send_sem, recv_sem=recv_sem,
                                     device_id={"sp": to}, device_id_type=MESH).start()

    q_copy = pltpu.make_async_copy(q_hbm, q_buf, q_sem)
    k_copy(0).start()
    q_copy.start()
    for b in range(AHEAD):
        if b > 0:
            k_copy(b).start()
        v_copy(b).start()

    barrier = pltpu.get_barrier_semaphore()
    for r in range(1, n):
        pl.semaphore_signal(barrier, inc=1, device_id={"sp": lax.rem(me + r, n)}, device_id_type=MESH)

    lane = lax.broadcasted_iota(jnp.int32, (heads, LANES), 1)

    def scores_of(s, to):
        to[...] = lax.dot_general(q_buf[s], k_buf[s], (((1,), (1,)), ((), ())), preferred_element_type=F32)

    def finish(s, raw):
        scores = raw[...]
        high = jnp.max(scores, -1, keepdims=True)
        weights = jnp.exp((scores - high) * scale)
        total = jnp.sum(weights, -1, keepdims=True)
        part[s, :, :head] = jnp.dot(weights.astype(BF16), v_buf[s], preferred_element_type=F32)
        part[s, :, head:head + LANES] = jnp.broadcast_to(high * scale, (heads, LANES))
        part[s, :, head + LANES:] = jnp.broadcast_to(total, (heads, LANES))

    def to_pair(t):
        remote(part.at[BLOCK * t + 1 - core], other.at[t], pair_send, pair_recv.at[lax.rem(t, 8)], device(0, False))

    def add_pair(t):
        a, b = part.at[BLOCK * t + core], other.at[t]
        high_a, high_b = a[:, head:head + LANES], b[:, head:head + LANES]
        high = jnp.maximum(high_a, high_b)
        scale_a, scale_b = jnp.exp(high_a - high), jnp.exp(high_b - high)
        total = scale_a * a[:, head + LANES:] + scale_b * b[:, head + LANES:]
        for at in range(0, head, LANES):
            run = slice(at, at + LANES)
            mine[t, chip, :, run] = (scale_a * a[:, run] + scale_b * b[:, run]).astype(BF16)
        both = jnp.where(lane == 0, high, total)
        mine_stat[t, chip, :, :chips * heads] = jnp.transpose(jnp.concatenate([both] * chips, 0))[:2]

    def group_of(t):
        return sum((t >= cut).astype(jnp.int32) if not isinstance(t, int) else int(t >= cut) for cut in CUTS[1:])

    def to_chips(t):
        group = group_of(t)
        for r in range(1, chips):
            remote(mine.at[t, chip], mine.at[t, chip], acc_send, acc_recv.at[group], device(r, True))
            remote(mine_stat.at[t, chip], mine_stat.at[t, chip], stat_send, stat_recv.at[group], device(r, True))

    def to_all(t):
        d = t - staged
        for r in range(chips):
            if r > 0:
                remote(mine.at[t, chip], mine.at[t, chip], acc_send, direct_acc_recv.at[d], device(r, True))
                remote(mine_stat.at[t, chip], mine_stat.at[t, chip], stat_send, direct_stat_recv.at[d], device(r, True))
            remote(mine.at[t, chip], theirs.at[d, chip], acc_send, direct_acc_recv2.at[d], device(r, False))
            remote(mine_stat.at[t, chip], theirs_stat.at[d, chip], stat_send, direct_stat_recv2.at[d], device(r, False))

    wide = chips * heads
    owner = lax.broadcasted_iota(jnp.int32, (1, wide), 1) // heads
    diagonal = lax.rem(lax.broadcasted_iota(jnp.int32, (heads, wide), 1), heads) == lax.broadcasted_iota(
        jnp.int32, (heads, wide), 0)

    def add_chips(work):
        for acc, stat, t, j in work:
            highs = [stat[c, 0:1, :wide] for c in range(chips)]
            totals = [stat[c, 1:2, :wide] for c in range(chips)]
            high = functools.reduce(jnp.maximum, highs)
            scales = [jnp.exp(x - high) for x in highs]
            total = functools.reduce(jnp.add, [w * x for w, x in zip(scales, totals)])
            row = scales[0]
            for c in range(1, chips):
                row = jnp.where(owner == c, scales[c], row)
            rest = jnp.where(diagonal, jnp.broadcast_to(row / total, (heads, wide)), 0.0)
            terms = []
            for _ in range(3):
                terms.append(rest.astype(BF16))
                rest = rest - terms[-1].astype(F32)
            sums = jnp.dot(jnp.concatenate(terms, 0), acc[...].reshape(wide, head), preferred_element_type=F32)
            out[t, j] = (sums[:heads] + (sums[heads:2 * heads] + sums[2 * heads:])).astype(BF16)

    def add_group(g):
        first, last = groups[g]
        count = (last - first) * (chips - 1)
        flat = mine.at[pl.ds(0, count // (chips - 1)), pl.ds(0, chips - 1)]
        flat_stat = mine_stat.at[pl.ds(0, count // (chips - 1)), pl.ds(0, chips - 1)]
        wait(flat, acc_recv.at[g])
        wait(flat_stat, stat_recv.at[g])
        add_chips([(mine.at[t], mine_stat.at[t], t, core) for t in range(first, last)])
        run = pl.ds(first, last - first)
        remote(out.at[run, core], out.at[run, core], out_send, out_recv, device(0, False))

    def block(b):
        b, parity, first, last = b if isinstance(b, tuple) else (b, b % 2, b, b)
        if first < blocks:
            k_copy(b).wait()
        v_copy(b - 1).wait()
        if first >= 4:
            wait(other.at[0], pair_recv.at[lax.rem(b - 4, 8)])
        if first < blocks:
            later = b + AHEAD - 1
            if last + AHEAD - 1 < blocks:
                k_copy(later).start()
                v_copy(later).start()
            elif first + AHEAD - 1 < blocks:
                @pl.when(later < blocks)
                def _():
                    k_copy(later).start()
                    v_copy(later).start()
        if first == 1:
            pl.semaphore_wait(barrier, n - 1)
        if first < blocks:
            for j in range(BLOCK):
                scores_of(b * BLOCK + j, raw[parity].at[j])
        for j in range(BLOCK):
            finish((b - 1) * BLOCK + j, raw[1 - parity].at[j])
        if first >= 4:
            add_pair(b - 4)
        to_pair(b - 1)
        if first >= 4:
            to_chips(b - 4)

    q_copy.wait()
    k_copy(0).wait()
    for j in range(BLOCK):
        scores_of(j, raw[0].at[j])
    for b in range(1, 5):
        block(b)

    for b in range(5, blocks - 1):
        block(b)
    block(blocks - 1)
    block(blocks)
    for t in range(blocks - 3, blocks):
        if t == blocks - 2:
            add_group(0)
        wait(other.at[0], pair_recv.at[t % 8])
        add_pair(t)
        (to_all if t >= staged else to_chips)(t)
    for g in range(1, len(groups)):
        add_group(g)
    for d in range(DIRECT):
        wait(mine.at[0, pl.ds(0, chips - 1)], direct_acc_recv.at[d])
        wait(mine_stat.at[0, pl.ds(0, chips - 1)], direct_stat_recv.at[d])
        wait(mine.at[0], direct_acc_recv2.at[d])
        wait(mine_stat.at[0], direct_stat_recv2.at[d])
        t = staged + d
        add_chips([(mine.at[t], mine_stat.at[t], t, core), (theirs.at[d], theirs_stat.at[d], t, 1 - core)])
    wait(out.at[pl.ds(0, staged), 0], out_recv)
    wait(out.at[pl.ds(0, staged), 0], out_send)
    wait(part.at[pl.ds(0, blocks)], pair_send)
    sends = (staged * (chips - 1) + DIRECT * (n - 1)) // chips
    wait(mine.at[pl.ds(0, sends)], acc_send)
    wait(mine_stat.at[pl.ds(0, sends)], stat_send)


def solution(mesh):
    n = mesh.shape["sp"]

    def step(q, k, v):
        batch, heads, head = q.shape
        tokens = k.shape[1]
        k = k.reshape(batch, tokens, head)
        v = v.reshape(batch, tokens, head)
        blocks, chips = batch // BLOCK, n // 2
        dma = pltpu.SemaphoreType.DMA
        return pl.pallas_call(
            functools.partial(kernel, n, head ** -0.5),
            out_shape=jax.ShapeDtypeStruct((blocks, BLOCK, heads, head), BF16),
            in_specs=[pl.BlockSpec(memory_space=pltpu.HBM)] * 3,
            out_specs=pl.BlockSpec(memory_space=pltpu.VMEM),
            scratch_shapes=[
                pltpu.VMEM((batch, heads, head), BF16),
                pltpu.VMEM((batch, tokens, head), BF16),
                pltpu.VMEM((batch, tokens, head), BF16),
                pltpu.VMEM((BLOCK, heads, tokens), F32),
                pltpu.VMEM((BLOCK, heads, tokens), F32),
                pltpu.VMEM((batch, heads, head + 2 * LANES), F32),
                pltpu.VMEM((blocks, heads, head + 2 * LANES), F32),
                pltpu.VMEM((blocks, chips, heads, head), BF16),
                pltpu.VMEM((blocks, chips, 2, LANES), F32),
                pltpu.VMEM((DIRECT, chips, heads, head), BF16),
                pltpu.VMEM((DIRECT, chips, 2, LANES), F32),
                dma, dma((AHEAD,)), dma((AHEAD,)),
                dma, dma((8,)),
                dma, dma, dma((len(CUTS),)), dma((len(CUTS),)),
                dma((DIRECT,)), dma((DIRECT,)), dma((DIRECT,)), dma((DIRECT,)),
                dma, dma,
            ],
            compiler_params=pltpu.CompilerParams(
                collective_id=0, has_side_effects=True, vmem_limit_bytes=48 * 1024 * 1024),
            name="decode",
        )(pltpu.with_memory_space_constraint(q, pltpu.HBM), k, v).reshape(q.shape)

    return jax.shard_map(
        step,
        mesh=mesh,
        in_specs=(P("dp", None, None), P("dp", "sp", None, None), P("dp", "sp", None, None)),
        out_specs=P("dp", None, None),
        check_vma=False,
    )
```

```python
import functools

import jax
import jax.numpy as jnp
from jax import lax
from jax.experimental import pallas as pl
from jax.experimental.pallas import tpu as pltpu
from jax.sharding import PartitionSpec as P

MESH = pl.DeviceIdType.MESH
F32 = jnp.float32
BF16 = jnp.bfloat16
BLOCK = 2
PIECES = 2
AHEAD = 8
DIRECT = 1
CUTS = (0, 6, 11, 13)
LANES = 128


def kernel(n, scale, q_hbm, k_hbm, v_hbm, out, q_buf, k_buf, v_buf, raw0, raw1, part, other, mine, mine_stat, theirs,
           theirs_stat, q_sem, k_sem, v_sem, pair_send, pair_recv, acc_send, stat_send, acc_recv, stat_recv,
           direct_acc_recv, direct_stat_recv, direct_acc_recv2, direct_stat_recv2, out_send, out_recv):
    me = lax.axis_index("sp")
    chip, core = me // 2, lax.rem(me, 2)
    chips = n // 2
    batch, heads, head = q_buf.shape
    tokens = k_buf.shape[1]
    blocks = batch // BLOCK
    staged = blocks - DIRECT
    groups = list(zip(CUTS, CUTS[1:] + (staged,)))
    raw = (raw0, raw1)

    def device(r, same):
        return lax.rem(chip + r, chips) * 2 + (core if same else 1 - core)

    class Run:
        def __init__(self, hbm, buf, sem, b):
            self.hbm, self.buf, self.first, self.sem = hbm, buf, b * BLOCK, sem.at[lax.rem(b, AHEAD)]

        def start(self):
            rows = tokens // PIECES
            for j in range(BLOCK):
                for p in range(PIECES):
                    at = (self.first + j, pl.ds(p * rows, rows))
                    pltpu.make_async_copy(self.hbm.at[at], self.buf.at[at], self.sem).start()

        def wait(self):
            run = self.buf.at[pl.ds(self.first, BLOCK)]
            pltpu.make_async_copy(run, run, self.sem).wait()

    k_copy = functools.partial(Run, k_hbm, k_buf, k_sem)
    v_copy = functools.partial(Run, v_hbm, v_buf, v_sem)

    def wait(ref, sem):
        pltpu.make_async_copy(ref, ref, sem).wait()

    def remote(src, dst, send_sem, recv_sem, to):
        pltpu.make_async_remote_copy(src_ref=src, dst_ref=dst, send_sem=send_sem, recv_sem=recv_sem,
                                     device_id={"sp": to}, device_id_type=MESH).start()

    q_copy = pltpu.make_async_copy(q_hbm, q_buf, q_sem)
    k_copy(0).start()
    q_copy.start()
    for b in range(AHEAD):
        if b > 0:
            k_copy(b).start()
        v_copy(b).start()

    barrier = pltpu.get_barrier_semaphore()
    for r in range(1, n):
        pl.semaphore_signal(barrier, inc=1, device_id={"sp": lax.rem(me + r, n)}, device_id_type=MESH)

    lane = lax.broadcasted_iota(jnp.int32, (heads, LANES), 1)

    def scores_of(s, to):
        to[...] = lax.dot_general(q_buf[s], k_buf[s], (((1,), (1,)), ((), ())), preferred_element_type=F32)

    def finish(s, raw):
        scores = raw[...]
        high = jnp.max(scores, -1, keepdims=True)
        weights = jnp.exp((scores - high) * scale)
        total = jnp.sum(weights, -1, keepdims=True)
        part[s, :, :head] = jnp.dot(weights.astype(BF16), v_buf[s], preferred_element_type=F32)
        part[s, :, head:head + LANES] = jnp.broadcast_to(high * scale, (heads, LANES))
        part[s, :, head + LANES:] = jnp.broadcast_to(total, (heads, LANES))

    def to_pair(t):
        remote(part.at[BLOCK * t + 1 - core], other.at[t], pair_send, pair_recv.at[lax.rem(t, 8)], device(0, False))

    def add_pair(t):
        a, b = part.at[BLOCK * t + core], other.at[t]
        high_a, high_b = a[:, head:head + LANES], b[:, head:head + LANES]
        high = jnp.maximum(high_a, high_b)
        scale_a, scale_b = jnp.exp(high_a - high), jnp.exp(high_b - high)
        total = scale_a * a[:, head + LANES:] + scale_b * b[:, head + LANES:]
        for at in range(0, head, LANES):
            run = slice(at, at + LANES)
            mine[t, chip, :, run] = (scale_a * a[:, run] + scale_b * b[:, run]).astype(BF16)
        both = jnp.where(lane == 0, high, total)
        mine_stat[t, chip, :, :chips * heads] = jnp.transpose(jnp.concatenate([both] * chips, 0))[:2]

    def group_of(t):
        return sum((t >= cut).astype(jnp.int32) if not isinstance(t, int) else int(t >= cut) for cut in CUTS[1:])

    def to_chips(t):
        group = group_of(t)
        for r in range(1, chips):
            remote(mine.at[t, chip], mine.at[t, chip], acc_send, acc_recv.at[group], device(r, True))
            remote(mine_stat.at[t, chip], mine_stat.at[t, chip], stat_send, stat_recv.at[group], device(r, True))

    def to_all(t):
        d = t - staged
        for r in range(chips):
            if r > 0:
                remote(mine.at[t, chip], mine.at[t, chip], acc_send, direct_acc_recv.at[d], device(r, True))
                remote(mine_stat.at[t, chip], mine_stat.at[t, chip], stat_send, direct_stat_recv.at[d], device(r, True))
            remote(mine.at[t, chip], theirs.at[d, chip], acc_send, direct_acc_recv2.at[d], device(r, False))
            remote(mine_stat.at[t, chip], theirs_stat.at[d, chip], stat_send, direct_stat_recv2.at[d], device(r, False))

    wide = chips * heads
    owner = lax.broadcasted_iota(jnp.int32, (1, wide), 1) // heads
    diagonal = lax.rem(lax.broadcasted_iota(jnp.int32, (heads, wide), 1), heads) == lax.broadcasted_iota(
        jnp.int32, (heads, wide), 0)

    def add_chips(work):
        for acc, stat, t, j in work:
            highs = [stat[c, 0:1, :wide] for c in range(chips)]
            totals = [stat[c, 1:2, :wide] for c in range(chips)]
            high = functools.reduce(jnp.maximum, highs)
            scales = [jnp.exp(x - high) for x in highs]
            total = functools.reduce(jnp.add, [w * x for w, x in zip(scales, totals)])
            row = scales[0]
            for c in range(1, chips):
                row = jnp.where(owner == c, scales[c], row)
            rest = jnp.where(diagonal, jnp.broadcast_to(row / total, (heads, wide)), 0.0)
            terms = []
            for _ in range(3):
                terms.append(rest.astype(BF16))
                rest = rest - terms[-1].astype(F32)
            sums = jnp.dot(jnp.concatenate(terms, 0), acc[...].reshape(wide, head), preferred_element_type=F32)
            out[t, j] = (sums[:heads] + (sums[heads:2 * heads] + sums[2 * heads:])).astype(BF16)

    def add_group(g):
        first, last = groups[g]
        count = (last - first) * (chips - 1)
        flat = mine.at[pl.ds(0, count // (chips - 1)), pl.ds(0, chips - 1)]
        flat_stat = mine_stat.at[pl.ds(0, count // (chips - 1)), pl.ds(0, chips - 1)]
        wait(flat, acc_recv.at[g])
        wait(flat_stat, stat_recv.at[g])
        add_chips([(mine.at[t], mine_stat.at[t], t, core) for t in range(first, last)])
        run = pl.ds(first, last - first)
        remote(out.at[run, core], out.at[run, core], out_send, out_recv, device(0, False))

    def block(b):
        b, parity, first, last = b if isinstance(b, tuple) else (b, b % 2, b, b)
        if first < blocks:
            k_copy(b).wait()
        v_copy(b - 1).wait()
        if first >= 4:
            wait(other.at[0], pair_recv.at[lax.rem(b - 4, 8)])
        if first < blocks:
            later = b + AHEAD - 1
            if last + AHEAD - 1 < blocks:
                k_copy(later).start()
                v_copy(later).start()
            elif first + AHEAD - 1 < blocks:
                @pl.when(later < blocks)
                def _():
                    k_copy(later).start()
                    v_copy(later).start()
        if first == 1:
            pl.semaphore_wait(barrier, n - 1)
        if first < blocks:
            for j in range(BLOCK):
                scores_of(b * BLOCK + j, raw[parity].at[j])
        for j in range(BLOCK):
            finish((b - 1) * BLOCK + j, raw[1 - parity].at[j])
        if first >= 4:
            add_pair(b - 4)
        to_pair(b - 1)
        if first >= 4:
            to_chips(b - 4)

    q_copy.wait()
    k_copy(0).wait()
    for j in range(BLOCK):
        scores_of(j, raw[0].at[j])
    for b in range(1, 5):
        block(b)

    for b in range(5, blocks - 1):
        block(b)
    block(blocks - 1)
    block(blocks)
    for t in range(blocks - 3, blocks):
        if t == blocks - 2:
            add_group(0)
        wait(other.at[0], pair_recv.at[t % 8])
        add_pair(t)
        (to_all if t >= staged else to_chips)(t)
    for g in range(1, len(groups)):
        add_group(g)
    for d in range(DIRECT):
        wait(mine.at[0, pl.ds(0, chips - 1)], direct_acc_recv.at[d])
        wait(mine_stat.at[0, pl.ds(0, chips - 1)], direct_stat_recv.at[d])
        wait(mine.at[0], direct_acc_recv2.at[d])
        wait(mine_stat.at[0], direct_stat_recv2.at[d])
        t = staged + d
        add_chips([(mine.at[t], mine_stat.at[t], t, core), (theirs.at[d], theirs_stat.at[d], t, 1 - core)])
    wait(out.at[pl.ds(0, staged), 0], out_recv)
    wait(out.at[pl.ds(0, staged), 0], out_send)
    wait(part.at[pl.ds(0, blocks)], pair_send)
    sends = (staged * (chips - 1) + DIRECT * (n - 1)) // chips
    wait(mine.at[pl.ds(0, sends)], acc_send)
    wait(mine_stat.at[pl.ds(0, sends)], stat_send)


def solution(mesh):
    n = mesh.shape["sp"]

    def step(q, k, v):
        batch, heads, head = q.shape
        tokens = k.shape[1]
        k = k.reshape(batch, tokens, head)
        v = v.reshape(batch, tokens, head)
        blocks, chips = batch // BLOCK, n // 2
        dma = pltpu.SemaphoreType.DMA
        return pl.pallas_call(
            functools.partial(kernel, n, head ** -0.5),
            out_shape=jax.ShapeDtypeStruct((blocks, BLOCK, heads, head), BF16),
            in_specs=[pl.BlockSpec(memory_space=pltpu.HBM)] * 3,
            out_specs=pl.BlockSpec(memory_space=pltpu.VMEM),
            scratch_shapes=[
                pltpu.VMEM((batch, heads, head), BF16),
                pltpu.VMEM((batch, tokens, head), BF16),
                pltpu.VMEM((batch, tokens, head), BF16),
                pltpu.VMEM((BLOCK, heads, tokens), F32),
                pltpu.VMEM((BLOCK, heads, tokens), F32),
                pltpu.VMEM((batch, heads, head + 2 * LANES), F32),
                pltpu.VMEM((blocks, heads, head + 2 * LANES), F32),
                pltpu.VMEM((blocks, chips, heads, head), BF16),
                pltpu.VMEM((blocks, chips, 2, LANES), F32),
                pltpu.VMEM((DIRECT, chips, heads, head), BF16),
                pltpu.VMEM((DIRECT, chips, 2, LANES), F32),
                dma, dma((AHEAD,)), dma((AHEAD,)),
                dma, dma((8,)),
                dma, dma, dma((len(CUTS),)), dma((len(CUTS),)),
                dma((DIRECT,)), dma((DIRECT,)), dma((DIRECT,)), dma((DIRECT,)),
                dma, dma,
            ],
            compiler_params=pltpu.CompilerParams(
                collective_id=0, has_side_effects=True, vmem_limit_bytes=48 * 1024 * 1024),
            name="decode",
        )(pltpu.with_memory_space_constraint(q, pltpu.HBM), k, v).reshape(q.shape)

    return jax.shard_map(
        step,
        mesh=mesh,
        in_specs=(P("dp", None, None), P("dp", "sp", None, None), P("dp", "sp", None, None)),
        out_specs=P("dp", None, None),
        check_vma=False,
    )
```

```python
import functools

import jax
import jax.numpy as jnp
from jax import lax
from jax.experimental import pallas as pl
from jax.experimental.pallas import tpu as pltpu
from jax.sharding import PartitionSpec as P

MESH = pl.DeviceIdType.MESH
F32 = jnp.float32
BF16 = jnp.bfloat16
BLOCK = 2
PIECES = 2
AHEAD = 4
DIRECT = 1
CUTS = (0, 6, 11, 13)
LANES = 128


def kernel(n, scale, q_hbm, k_hbm, v_hbm, out, q_buf, k_buf, v_buf, raw0, raw1, part, other, mine, mine_stat, theirs,
           theirs_stat, q_sem, k_sem, v_sem, pair_send, pair_recv, acc_send, stat_send, acc_recv, stat_recv,
           direct_acc_recv, direct_stat_recv, direct_acc_recv2, direct_stat_recv2, out_send, out_recv):
    me = lax.axis_index("sp")
    chip, core = me // 2, lax.rem(me, 2)
    chips = n // 2
    batch, heads, head = q_buf.shape
    tokens = k_buf.shape[1]
    blocks = batch // BLOCK
    staged = blocks - DIRECT
    groups = list(zip(CUTS, CUTS[1:] + (staged,)))
    raw = (raw0, raw1)

    def device(r, same):
        return lax.rem(chip + r, chips) * 2 + (core if same else 1 - core)

    class Run:
        def __init__(self, hbm, buf, sem, b):
            self.hbm, self.buf, self.first, self.sem = hbm, buf, b * BLOCK, sem.at[lax.rem(b, AHEAD)]

        def start(self):
            rows = tokens // PIECES
            for j in range(BLOCK):
                for p in range(PIECES):
                    at = (self.first + j, pl.ds(p * rows, rows))
                    pltpu.make_async_copy(self.hbm.at[at], self.buf.at[at], self.sem).start()

        def wait(self):
            run = self.buf.at[pl.ds(self.first, BLOCK)]
            pltpu.make_async_copy(run, run, self.sem).wait()

    k_copy = functools.partial(Run, k_hbm, k_buf, k_sem)
    v_copy = functools.partial(Run, v_hbm, v_buf, v_sem)

    def wait(ref, sem):
        pltpu.make_async_copy(ref, ref, sem).wait()

    def remote(src, dst, send_sem, recv_sem, to):
        pltpu.make_async_remote_copy(src_ref=src, dst_ref=dst, send_sem=send_sem, recv_sem=recv_sem,
                                     device_id={"sp": to}, device_id_type=MESH).start()

    q_copy = pltpu.make_async_copy(q_hbm, q_buf, q_sem)
    k_copy(0).start()
    q_copy.start()
    for b in range(AHEAD):
        if b > 0:
            k_copy(b).start()
        v_copy(b).start()

    barrier = pltpu.get_barrier_semaphore()
    for r in range(1, n):
        pl.semaphore_signal(barrier, inc=1, device_id={"sp": lax.rem(me + r, n)}, device_id_type=MESH)

    lane = lax.broadcasted_iota(jnp.int32, (heads, LANES), 1)

    def scores_of(s, to):
        to[...] = lax.dot_general(q_buf[s], k_buf[s], (((1,), (1,)), ((), ())), preferred_element_type=F32)

    def finish(s, raw):
        scores = raw[...]
        high = jnp.max(scores, -1, keepdims=True)
        weights = jnp.exp((scores - high) * scale)
        total = jnp.sum(weights, -1, keepdims=True)
        part[s, :, :head] = jnp.dot(weights.astype(BF16), v_buf[s], preferred_element_type=F32)
        part[s, :, head:head + LANES] = jnp.broadcast_to(high * scale, (heads, LANES))
        part[s, :, head + LANES:] = jnp.broadcast_to(total, (heads, LANES))

    def to_pair(t):
        remote(part.at[BLOCK * t + 1 - core], other.at[t], pair_send, pair_recv.at[lax.rem(t, 8)], device(0, False))

    def add_pair(t):
        a, b = part.at[BLOCK * t + core], other.at[t]
        high_a, high_b = a[:, head:head + LANES], b[:, head:head + LANES]
        high = jnp.maximum(high_a, high_b)
        scale_a, scale_b = jnp.exp(high_a - high), jnp.exp(high_b - high)
        total = scale_a * a[:, head + LANES:] + scale_b * b[:, head + LANES:]
        for at in range(0, head, LANES):
            run = slice(at, at + LANES)
            mine[t, chip, :, run] = (scale_a * a[:, run] + scale_b * b[:, run]).astype(BF16)
        both = jnp.where(lane == 0, high, total)
        mine_stat[t, chip, :, :chips * heads] = jnp.transpose(jnp.concatenate([both] * chips, 0))[:2]

    def group_of(t):
        return sum((t >= cut).astype(jnp.int32) if not isinstance(t, int) else int(t >= cut) for cut in CUTS[1:])

    def to_chips(t):
        group = group_of(t)
        for r in range(1, chips):
            remote(mine.at[t, chip], mine.at[t, chip], acc_send, acc_recv.at[group], device(r, True))
            remote(mine_stat.at[t, chip], mine_stat.at[t, chip], stat_send, stat_recv.at[group], device(r, True))

    def to_all(t):
        d = t - staged
        for r in range(chips):
            if r > 0:
                remote(mine.at[t, chip], mine.at[t, chip], acc_send, direct_acc_recv.at[d], device(r, True))
                remote(mine_stat.at[t, chip], mine_stat.at[t, chip], stat_send, direct_stat_recv.at[d], device(r, True))
            remote(mine.at[t, chip], theirs.at[d, chip], acc_send, direct_acc_recv2.at[d], device(r, False))
            remote(mine_stat.at[t, chip], theirs_stat.at[d, chip], stat_send, direct_stat_recv2.at[d], device(r, False))

    wide = chips * heads
    owner = lax.broadcasted_iota(jnp.int32, (1, wide), 1) // heads
    diagonal = lax.rem(lax.broadcasted_iota(jnp.int32, (heads, wide), 1), heads) == lax.broadcasted_iota(
        jnp.int32, (heads, wide), 0)

    def add_chips(work):
        for acc, stat, t, j in work:
            highs = [stat[c, 0:1, :wide] for c in range(chips)]
            totals = [stat[c, 1:2, :wide] for c in range(chips)]
            high = functools.reduce(jnp.maximum, highs)
            scales = [jnp.exp(x - high) for x in highs]
            total = functools.reduce(jnp.add, [w * x for w, x in zip(scales, totals)])
            row = scales[0]
            for c in range(1, chips):
                row = jnp.where(owner == c, scales[c], row)
            rest = jnp.where(diagonal, jnp.broadcast_to(row / total, (heads, wide)), 0.0)
            terms = []
            for _ in range(3):
                terms.append(rest.astype(BF16))
                rest = rest - terms[-1].astype(F32)
            sums = jnp.dot(jnp.concatenate(terms, 0), acc[...].reshape(wide, head), preferred_element_type=F32)
            out[t, j] = (sums[:heads] + (sums[heads:2 * heads] + sums[2 * heads:])).astype(BF16)

    def add_group(g):
        first, last = groups[g]
        count = (last - first) * (chips - 1)
        flat = mine.at[pl.ds(0, count // (chips - 1)), pl.ds(0, chips - 1)]
        flat_stat = mine_stat.at[pl.ds(0, count // (chips - 1)), pl.ds(0, chips - 1)]
        wait(flat, acc_recv.at[g])
        wait(flat_stat, stat_recv.at[g])
        add_chips([(mine.at[t], mine_stat.at[t], t, core) for t in range(first, last)])
        run = pl.ds(first, last - first)
        remote(out.at[run, core], out.at[run, core], out_send, out_recv, device(0, False))

    def block(b):
        b, parity, first, last = b if isinstance(b, tuple) else (b, b % 2, b, b)
        if first < blocks:
            k_copy(b).wait()
        v_copy(b - 1).wait()
        if first >= 4:
            wait(other.at[0], pair_recv.at[lax.rem(b - 4, 8)])
        if first < blocks:
            later = b + AHEAD - 1
            if last + AHEAD - 1 < blocks:
                k_copy(later).start()
                v_copy(later).start()
            elif first + AHEAD - 1 < blocks:
                @pl.when(later < blocks)
                def _():
                    k_copy(later).start()
                    v_copy(later).start()
        if first == 1:
            pl.semaphore_wait(barrier, n - 1)
        if first < blocks:
            for j in range(BLOCK):
                scores_of(b * BLOCK + j, raw[parity].at[j])
        for j in range(BLOCK):
            finish((b - 1) * BLOCK + j, raw[1 - parity].at[j])
        if first >= 4:
            add_pair(b - 4)
        to_pair(b - 1)
        if first >= 4:
            to_chips(b - 4)

    q_copy.wait()
    k_copy(0).wait()
    for j in range(BLOCK):
        scores_of(j, raw[0].at[j])
    for b in range(1, 5):
        block(b)

    for b in range(5, blocks - 1):
        block(b)
    block(blocks - 1)
    block(blocks)
    for t in range(blocks - 3, blocks):
        if t == blocks - 2:
            add_group(0)
        wait(other.at[0], pair_recv.at[t % 8])
        add_pair(t)
        (to_all if t >= staged else to_chips)(t)
    for g in range(1, len(groups)):
        add_group(g)
    for d in range(DIRECT):
        wait(mine.at[0, pl.ds(0, chips - 1)], direct_acc_recv.at[d])
        wait(mine_stat.at[0, pl.ds(0, chips - 1)], direct_stat_recv.at[d])
        wait(mine.at[0], direct_acc_recv2.at[d])
        wait(mine_stat.at[0], direct_stat_recv2.at[d])
        t = staged + d
        add_chips([(mine.at[t], mine_stat.at[t], t, core), (theirs.at[d], theirs_stat.at[d], t, 1 - core)])
    wait(out.at[pl.ds(0, staged), 0], out_recv)
    wait(out.at[pl.ds(0, staged), 0], out_send)
    wait(part.at[pl.ds(0, blocks)], pair_send)
    sends = (staged * (chips - 1) + DIRECT * (n - 1)) // chips
    wait(mine.at[pl.ds(0, sends)], acc_send)
    wait(mine_stat.at[pl.ds(0, sends)], stat_send)


def solution(mesh):
    n = mesh.shape["sp"]

    def step(q, k, v):
        batch, heads, head = q.shape
        tokens = k.shape[1]
        k = k.reshape(batch, tokens, head)
        v = v.reshape(batch, tokens, head)
        blocks, chips = batch // BLOCK, n // 2
        dma = pltpu.SemaphoreType.DMA
        return pl.pallas_call(
            functools.partial(kernel, n, head ** -0.5),
            out_shape=jax.ShapeDtypeStruct((blocks, BLOCK, heads, head), BF16),
            in_specs=[pl.BlockSpec(memory_space=pltpu.HBM)] * 3,
            out_specs=pl.BlockSpec(memory_space=pltpu.VMEM),
            scratch_shapes=[
                pltpu.VMEM((batch, heads, head), BF16),
                pltpu.VMEM((batch, tokens, head), BF16),
                pltpu.VMEM((batch, tokens, head), BF16),
                pltpu.VMEM((BLOCK, heads, tokens), F32),
                pltpu.VMEM((BLOCK, heads, tokens), F32),
                pltpu.VMEM((batch, heads, head + 2 * LANES), F32),
                pltpu.VMEM((blocks, heads, head + 2 * LANES), F32),
                pltpu.VMEM((blocks, chips, heads, head), BF16),
                pltpu.VMEM((blocks, chips, 2, LANES), F32),
                pltpu.VMEM((DIRECT, chips, heads, head), BF16),
                pltpu.VMEM((DIRECT, chips, 2, LANES), F32),
                dma, dma((AHEAD,)), dma((AHEAD,)),
                dma, dma((8,)),
                dma, dma, dma((len(CUTS),)), dma((len(CUTS),)),
                dma((DIRECT,)), dma((DIRECT,)), dma((DIRECT,)), dma((DIRECT,)),
                dma, dma,
            ],
            compiler_params=pltpu.CompilerParams(
                collective_id=0, has_side_effects=True, vmem_limit_bytes=48 * 1024 * 1024),
            name="decode",
        )(pltpu.with_memory_space_constraint(q, pltpu.HBM), k, v).reshape(q.shape)

    return jax.shard_map(
        step,
        mesh=mesh,
        in_specs=(P("dp", None, None), P("dp", "sp", None, None), P("dp", "sp", None, None)),
        out_specs=P("dp", None, None),
        check_vma=False,
    )
```

```python
import functools

import jax
import jax.numpy as jnp
from jax import lax
from jax.experimental import pallas as pl
from jax.experimental.pallas import tpu as pltpu
from jax.sharding import PartitionSpec as P

MESH = pl.DeviceIdType.MESH
F32 = jnp.float32
BF16 = jnp.bfloat16
BLOCK = 2
PIECES = 2
AHEAD = 3
DIRECT = 1
CUTS = (0, 6, 11, 13)
LANES = 128


def kernel(n, scale, q_hbm, k_hbm, v_hbm, out, q_buf, k_buf, v_buf, raw0, raw1, part, other, mine, mine_stat, theirs,
           theirs_stat, q_sem, k_sem, v_sem, pair_send, pair_recv, acc_send, stat_send, acc_recv, stat_recv,
           direct_acc_recv, direct_stat_recv, direct_acc_recv2, direct_stat_recv2, out_send, out_recv):
    me = lax.axis_index("sp")
    chip, core = me // 2, lax.rem(me, 2)
    chips = n // 2
    batch, heads, head = q_buf.shape
    tokens = k_buf.shape[1]
    blocks = batch // BLOCK
    staged = blocks - DIRECT
    groups = list(zip(CUTS, CUTS[1:] + (staged,)))
    raw = (raw0, raw1)

    def device(r, same):
        return lax.rem(chip + r, chips) * 2 + (core if same else 1 - core)

    class Run:
        def __init__(self, hbm, buf, sem, b):
            self.hbm, self.buf, self.first, self.sem = hbm, buf, b * BLOCK, sem.at[lax.rem(b, AHEAD)]

        def start(self):
            rows = tokens // PIECES
            for j in range(BLOCK):
                for p in range(PIECES):
                    at = (self.first + j, pl.ds(p * rows, rows))
                    pltpu.make_async_copy(self.hbm.at[at], self.buf.at[at], self.sem).start()

        def wait(self):
            run = self.buf.at[pl.ds(self.first, BLOCK)]
            pltpu.make_async_copy(run, run, self.sem).wait()

    k_copy = functools.partial(Run, k_hbm, k_buf, k_sem)
    v_copy = functools.partial(Run, v_hbm, v_buf, v_sem)

    def wait(ref, sem):
        pltpu.make_async_copy(ref, ref, sem).wait()

    def remote(src, dst, send_sem, recv_sem, to):
        pltpu.make_async_remote_copy(src_ref=src, dst_ref=dst, send_sem=send_sem, recv_sem=recv_sem,
                                     device_id={"sp": to}, device_id_type=MESH).start()

    q_copy = pltpu.make_async_copy(q_hbm, q_buf, q_sem)
    k_copy(0).start()
    q_copy.start()
    for b in range(AHEAD):
        if b > 0:
            k_copy(b).start()
        v_copy(b).start()

    barrier = pltpu.get_barrier_semaphore()
    for r in range(1, n):
        pl.semaphore_signal(barrier, inc=1, device_id={"sp": lax.rem(me + r, n)}, device_id_type=MESH)

    lane = lax.broadcasted_iota(jnp.int32, (heads, LANES), 1)

    def scores_of(s, to):
        to[...] = lax.dot_general(q_buf[s], k_buf[s], (((1,), (1,)), ((), ())), preferred_element_type=F32)

    def finish(s, raw):
        scores = raw[...]
        high = jnp.max(scores, -1, keepdims=True)
        weights = jnp.exp((scores - high) * scale)
        total = jnp.sum(weights, -1, keepdims=True)
        part[s, :, :head] = jnp.dot(weights.astype(BF16), v_buf[s], preferred_element_type=F32)
        part[s, :, head:head + LANES] = jnp.broadcast_to(high * scale, (heads, LANES))
        part[s, :, head + LANES:] = jnp.broadcast_to(total, (heads, LANES))

    def to_pair(t):
        remote(part.at[BLOCK * t + 1 - core], other.at[t], pair_send, pair_recv.at[lax.rem(t, 8)], device(0, False))

    def add_pair(t):
        a, b = part.at[BLOCK * t + core], other.at[t]
        high_a, high_b = a[:, head:head + LANES], b[:, head:head + LANES]
        high = jnp.maximum(high_a, high_b)
        scale_a, scale_b = jnp.exp(high_a - high), jnp.exp(high_b - high)
        total = scale_a * a[:, head + LANES:] + scale_b * b[:, head + LANES:]
        for at in range(0, head, LANES):
            run = slice(at, at + LANES)
            mine[t, chip, :, run] = (scale_a * a[:, run] + scale_b * b[:, run]).astype(BF16)
        both = jnp.where(lane == 0, high, total)
        mine_stat[t, chip, :, :chips * heads] = jnp.transpose(jnp.concatenate([both] * chips, 0))[:2]

    def group_of(t):
        return sum((t >= cut).astype(jnp.int32) if not isinstance(t, int) else int(t >= cut) for cut in CUTS[1:])

    def to_chips(t):
        group = group_of(t)
        for r in range(1, chips):
            remote(mine.at[t, chip], mine.at[t, chip], acc_send, acc_recv.at[group], device(r, True))
            remote(mine_stat.at[t, chip], mine_stat.at[t, chip], stat_send, stat_recv.at[group], device(r, True))

    def to_all(t):
        d = t - staged
        for r in range(chips):
            if r > 0:
                remote(mine.at[t, chip], mine.at[t, chip], acc_send, direct_acc_recv.at[d], device(r, True))
                remote(mine_stat.at[t, chip], mine_stat.at[t, chip], stat_send, direct_stat_recv.at[d], device(r, True))
            remote(mine.at[t, chip], theirs.at[d, chip], acc_send, direct_acc_recv2.at[d], device(r, False))
            remote(mine_stat.at[t, chip], theirs_stat.at[d, chip], stat_send, direct_stat_recv2.at[d], device(r, False))

    wide = chips * heads
    owner = lax.broadcasted_iota(jnp.int32, (1, wide), 1) // heads
    diagonal = lax.rem(lax.broadcasted_iota(jnp.int32, (heads, wide), 1), heads) == lax.broadcasted_iota(
        jnp.int32, (heads, wide), 0)

    def add_chips(work):
        for acc, stat, t, j in work:
            highs = [stat[c, 0:1, :wide] for c in range(chips)]
            totals = [stat[c, 1:2, :wide] for c in range(chips)]
            high = functools.reduce(jnp.maximum, highs)
            scales = [jnp.exp(x - high) for x in highs]
            total = functools.reduce(jnp.add, [w * x for w, x in zip(scales, totals)])
            row = scales[0]
            for c in range(1, chips):
                row = jnp.where(owner == c, scales[c], row)
            rest = jnp.where(diagonal, jnp.broadcast_to(row / total, (heads, wide)), 0.0)
            terms = []
            for _ in range(3):
                terms.append(rest.astype(BF16))
                rest = rest - terms[-1].astype(F32)
            sums = jnp.dot(jnp.concatenate(terms, 0), acc[...].reshape(wide, head), preferred_element_type=F32)
            out[t, j] = (sums[:heads] + (sums[heads:2 * heads] + sums[2 * heads:])).astype(BF16)

    def add_group(g):
        first, last = groups[g]
        count = (last - first) * (chips - 1)
        flat = mine.at[pl.ds(0, count // (chips - 1)), pl.ds(0, chips - 1)]
        flat_stat = mine_stat.at[pl.ds(0, count // (chips - 1)), pl.ds(0, chips - 1)]
        wait(flat, acc_recv.at[g])
        wait(flat_stat, stat_recv.at[g])
        add_chips([(mine.at[t], mine_stat.at[t], t, core) for t in range(first, last)])
        run = pl.ds(first, last - first)
        remote(out.at[run, core], out.at[run, core], out_send, out_recv, device(0, False))

    def block(b):
        b, parity, first, last = b if isinstance(b, tuple) else (b, b % 2, b, b)
        if first < blocks:
            k_copy(b).wait()
        v_copy(b - 1).wait()
        if first >= 4:
            wait(other.at[0], pair_recv.at[lax.rem(b - 4, 8)])
        if first < blocks:
            later = b + AHEAD - 1
            if last + AHEAD - 1 < blocks:
                k_copy(later).start()
                v_copy(later).start()
            elif first + AHEAD - 1 < blocks:
                @pl.when(later < blocks)
                def _():
                    k_copy(later).start()
                    v_copy(later).start()
        if first == 1:
            pl.semaphore_wait(barrier, n - 1)
        if first < blocks:
            for j in range(BLOCK):
                scores_of(b * BLOCK + j, raw[parity].at[j])
        for j in range(BLOCK):
            finish((b - 1) * BLOCK + j, raw[1 - parity].at[j])
        if first >= 4:
            add_pair(b - 4)
        to_pair(b - 1)
        if first >= 4:
            to_chips(b - 4)

    q_copy.wait()
    k_copy(0).wait()
    for j in range(BLOCK):
        scores_of(j, raw[0].at[j])
    for b in range(1, 5):
        block(b)

    for b in range(5, blocks - 1):
        block(b)
    block(blocks - 1)
    block(blocks)
    for t in range(blocks - 3, blocks):
        if t == blocks - 2:
            add_group(0)
        wait(other.at[0], pair_recv.at[t % 8])
        add_pair(t)
        (to_all if t >= staged else to_chips)(t)
    for g in range(1, len(groups)):
        add_group(g)
    for d in range(DIRECT):
        wait(mine.at[0, pl.ds(0, chips - 1)], direct_acc_recv.at[d])
        wait(mine_stat.at[0, pl.ds(0, chips - 1)], direct_stat_recv.at[d])
        wait(mine.at[0], direct_acc_recv2.at[d])
        wait(mine_stat.at[0], direct_stat_recv2.at[d])
        t = staged + d
        add_chips([(mine.at[t], mine_stat.at[t], t, core), (theirs.at[d], theirs_stat.at[d], t, 1 - core)])
    wait(out.at[pl.ds(0, staged), 0], out_recv)
    wait(out.at[pl.ds(0, staged), 0], out_send)
    wait(part.at[pl.ds(0, blocks)], pair_send)
    sends = (staged * (chips - 1) + DIRECT * (n - 1)) // chips
    wait(mine.at[pl.ds(0, sends)], acc_send)
    wait(mine_stat.at[pl.ds(0, sends)], stat_send)


def solution(mesh):
    n = mesh.shape["sp"]

    def step(q, k, v):
        batch, heads, head = q.shape
        tokens = k.shape[1]
        k = k.reshape(batch, tokens, head)
        v = v.reshape(batch, tokens, head)
        blocks, chips = batch // BLOCK, n // 2
        dma = pltpu.SemaphoreType.DMA
        return pl.pallas_call(
            functools.partial(kernel, n, head ** -0.5),
            out_shape=jax.ShapeDtypeStruct((blocks, BLOCK, heads, head), BF16),
            in_specs=[pl.BlockSpec(memory_space=pltpu.HBM)] * 3,
            out_specs=pl.BlockSpec(memory_space=pltpu.VMEM),
            scratch_shapes=[
                pltpu.VMEM((batch, heads, head), BF16),
                pltpu.VMEM((batch, tokens, head), BF16),
                pltpu.VMEM((batch, tokens, head), BF16),
                pltpu.VMEM((BLOCK, heads, tokens), F32),
                pltpu.VMEM((BLOCK, heads, tokens), F32),
                pltpu.VMEM((batch, heads, head + 2 * LANES), F32),
                pltpu.VMEM((blocks, heads, head + 2 * LANES), F32),
                pltpu.VMEM((blocks, chips, heads, head), BF16),
                pltpu.VMEM((blocks, chips, 2, LANES), F32),
                pltpu.VMEM((DIRECT, chips, heads, head), BF16),
                pltpu.VMEM((DIRECT, chips, 2, LANES), F32),
                dma, dma((AHEAD,)), dma((AHEAD,)),
                dma, dma((8,)),
                dma, dma, dma((len(CUTS),)), dma((len(CUTS),)),
                dma((DIRECT,)), dma((DIRECT,)), dma((DIRECT,)), dma((DIRECT,)),
                dma, dma,
            ],
            compiler_params=pltpu.CompilerParams(
                collective_id=0, has_side_effects=True, vmem_limit_bytes=48 * 1024 * 1024),
            name="decode",
        )(pltpu.with_memory_space_constraint(q, pltpu.HBM), k, v).reshape(q.shape)

    return jax.shard_map(
        step,
        mesh=mesh,
        in_specs=(P("dp", None, None), P("dp", "sp", None, None), P("dp", "sp", None, None)),
        out_specs=P("dp", None, None),
        check_vma=False,
    )
```

```python
import functools

import jax
import jax.numpy as jnp
from jax import lax
from jax.experimental import pallas as pl
from jax.experimental.pallas import tpu as pltpu
from jax.sharding import PartitionSpec as P

MESH = pl.DeviceIdType.MESH
F32 = jnp.float32
BF16 = jnp.bfloat16
BLOCK = 2
PIECES = 2
FIRST = 2
AHEAD = 4
DIRECT = 1
CUTS = (0, 6, 11, 13)
LANES = 128


def kernel(n, scale, q_hbm, k_hbm, v_hbm, out, q_buf, k_buf, v_buf, raw0, raw1, part, other, mine, mine_stat, theirs,
           theirs_stat, q_sem, k_sem, v_sem, pair_send, pair_recv, acc_send, stat_send, acc_recv, stat_recv,
           direct_acc_recv, direct_stat_recv, direct_acc_recv2, direct_stat_recv2, out_send, out_recv):
    me = lax.axis_index("sp")
    chip, core = me // 2, lax.rem(me, 2)
    chips = n // 2
    batch, heads, head = q_buf.shape
    tokens = k_buf.shape[1]
    blocks = batch // BLOCK
    staged = blocks - DIRECT
    groups = list(zip(CUTS, CUTS[1:] + (staged,)))
    raw = (raw0, raw1)

    def device(r, same):
        return lax.rem(chip + r, chips) * 2 + (core if same else 1 - core)

    class Run:
        def __init__(self, hbm, buf, sem, b):
            self.hbm, self.buf, self.first, self.sem = hbm, buf, b * BLOCK, sem.at[lax.rem(b, AHEAD)]

        def start(self):
            rows = tokens // PIECES
            for j in range(BLOCK):
                for p in range(PIECES):
                    at = (self.first + j, pl.ds(p * rows, rows))
                    pltpu.make_async_copy(self.hbm.at[at], self.buf.at[at], self.sem).start()

        def wait(self):
            run = self.buf.at[pl.ds(self.first, BLOCK)]
            pltpu.make_async_copy(run, run, self.sem).wait()

    k_copy = functools.partial(Run, k_hbm, k_buf, k_sem)
    v_copy = functools.partial(Run, v_hbm, v_buf, v_sem)

    def wait(ref, sem):
        pltpu.make_async_copy(ref, ref, sem).wait()

    def remote(src, dst, send_sem, recv_sem, to):
        pltpu.make_async_remote_copy(src_ref=src, dst_ref=dst, send_sem=send_sem, recv_sem=recv_sem,
                                     device_id={"sp": to}, device_id_type=MESH).start()

    q_copy = pltpu.make_async_copy(q_hbm, q_buf, q_sem)
    k_copy(0).start()
    q_copy.start()
    for b in range(FIRST):
        if b > 0:
            k_copy(b).start()
        v_copy(b).start()

    barrier = pltpu.get_barrier_semaphore()
    for r in range(1, n):
        pl.semaphore_signal(barrier, inc=1, device_id={"sp": lax.rem(me + r, n)}, device_id_type=MESH)

    lane = lax.broadcasted_iota(jnp.int32, (heads, LANES), 1)

    def scores_of(s, to):
        to[...] = lax.dot_general(q_buf[s], k_buf[s], (((1,), (1,)), ((), ())), preferred_element_type=F32)

    def finish(s, raw):
        scores = raw[...]
        high = jnp.max(scores, -1, keepdims=True)
        weights = jnp.exp((scores - high) * scale)
        total = jnp.sum(weights, -1, keepdims=True)
        part[s, :, :head] = jnp.dot(weights.astype(BF16), v_buf[s], preferred_element_type=F32)
        part[s, :, head:head + LANES] = jnp.broadcast_to(high * scale, (heads, LANES))
        part[s, :, head + LANES:] = jnp.broadcast_to(total, (heads, LANES))

    def to_pair(t):
        remote(part.at[BLOCK * t + 1 - core], other.at[t], pair_send, pair_recv.at[lax.rem(t, 8)], device(0, False))

    def add_pair(t):
        a, b = part.at[BLOCK * t + core], other.at[t]
        high_a, high_b = a[:, head:head + LANES], b[:, head:head + LANES]
        high = jnp.maximum(high_a, high_b)
        scale_a, scale_b = jnp.exp(high_a - high), jnp.exp(high_b - high)
        total = scale_a * a[:, head + LANES:] + scale_b * b[:, head + LANES:]
        for at in range(0, head, LANES):
            run = slice(at, at + LANES)
            mine[t, chip, :, run] = (scale_a * a[:, run] + scale_b * b[:, run]).astype(BF16)
        both = jnp.where(lane == 0, high, total)
        mine_stat[t, chip, :, :chips * heads] = jnp.transpose(jnp.concatenate([both] * chips, 0))[:2]

    def group_of(t):
        return sum((t >= cut).astype(jnp.int32) if not isinstance(t, int) else int(t >= cut) for cut in CUTS[1:])

    def to_chips(t):
        group = group_of(t)
        for r in range(1, chips):
            remote(mine.at[t, chip], mine.at[t, chip], acc_send, acc_recv.at[group], device(r, True))
            remote(mine_stat.at[t, chip], mine_stat.at[t, chip], stat_send, stat_recv.at[group], device(r, True))

    def to_all(t):
        d = t - staged
        for r in range(chips):
            if r > 0:
                remote(mine.at[t, chip], mine.at[t, chip], acc_send, direct_acc_recv.at[d], device(r, True))
                remote(mine_stat.at[t, chip], mine_stat.at[t, chip], stat_send, direct_stat_recv.at[d], device(r, True))
            remote(mine.at[t, chip], theirs.at[d, chip], acc_send, direct_acc_recv2.at[d], device(r, False))
            remote(mine_stat.at[t, chip], theirs_stat.at[d, chip], stat_send, direct_stat_recv2.at[d], device(r, False))

    wide = chips * heads
    owner = lax.broadcasted_iota(jnp.int32, (1, wide), 1) // heads
    diagonal = lax.rem(lax.broadcasted_iota(jnp.int32, (heads, wide), 1), heads) == lax.broadcasted_iota(
        jnp.int32, (heads, wide), 0)

    def add_chips(work):
        for acc, stat, t, j in work:
            highs = [stat[c, 0:1, :wide] for c in range(chips)]
            totals = [stat[c, 1:2, :wide] for c in range(chips)]
            high = functools.reduce(jnp.maximum, highs)
            scales = [jnp.exp(x - high) for x in highs]
            total = functools.reduce(jnp.add, [w * x for w, x in zip(scales, totals)])
            row = scales[0]
            for c in range(1, chips):
                row = jnp.where(owner == c, scales[c], row)
            rest = jnp.where(diagonal, jnp.broadcast_to(row / total, (heads, wide)), 0.0)
            terms = []
            for _ in range(3):
                terms.append(rest.astype(BF16))
                rest = rest - terms[-1].astype(F32)
            sums = jnp.dot(jnp.concatenate(terms, 0), acc[...].reshape(wide, head), preferred_element_type=F32)
            out[t, j] = (sums[:heads] + (sums[heads:2 * heads] + sums[2 * heads:])).astype(BF16)

    def add_group(g):
        first, last = groups[g]
        count = (last - first) * (chips - 1)
        flat = mine.at[pl.ds(0, count // (chips - 1)), pl.ds(0, chips - 1)]
        flat_stat = mine_stat.at[pl.ds(0, count // (chips - 1)), pl.ds(0, chips - 1)]
        wait(flat, acc_recv.at[g])
        wait(flat_stat, stat_recv.at[g])
        add_chips([(mine.at[t], mine_stat.at[t], t, core) for t in range(first, last)])
        run = pl.ds(first, last - first)
        remote(out.at[run, core], out.at[run, core], out_send, out_recv, device(0, False))

    def block(b):
        b, parity, first, last = b if isinstance(b, tuple) else (b, b % 2, b, b)
        if first < blocks:
            k_copy(b).wait()
        v_copy(b - 1).wait()
        if first >= 4:
            wait(other.at[0], pair_recv.at[lax.rem(b - 4, 8)])
        if b == 1:
            k_copy(AHEAD - 1).start()
            v_copy(AHEAD - 1).start()
        if first < blocks:
            later = b + AHEAD - 1
            if last + AHEAD - 1 < blocks:
                k_copy(later).start()
                v_copy(later).start()
            elif first + AHEAD - 1 < blocks:
                @pl.when(later < blocks)
                def _():
                    k_copy(later).start()
                    v_copy(later).start()
        if first == 1:
            pl.semaphore_wait(barrier, n - 1)
        if first < blocks:
            for j in range(BLOCK):
                scores_of(b * BLOCK + j, raw[parity].at[j])
        for j in range(BLOCK):
            finish((b - 1) * BLOCK + j, raw[1 - parity].at[j])
        if first >= 4:
            add_pair(b - 4)
        to_pair(b - 1)
        if first >= 4:
            to_chips(b - 4)

    q_copy.wait()
    k_copy(0).wait()
    for b in range(FIRST, AHEAD - 1):
        k_copy(b).start()
        v_copy(b).start()
    for j in range(BLOCK):
        scores_of(j, raw[0].at[j])
    for b in range(1, 5):
        block(b)

    for b in range(5, blocks - 1):
        block(b)
    block(blocks - 1)
    block(blocks)
    for t in range(blocks - 3, blocks):
        if t == blocks - 2:
            add_group(0)
        wait(other.at[0], pair_recv.at[t % 8])
        add_pair(t)
        (to_all if t >= staged else to_chips)(t)
    for g in range(1, len(groups)):
        add_group(g)
    for d in range(DIRECT):
        wait(mine.at[0, pl.ds(0, chips - 1)], direct_acc_recv.at[d])
        wait(mine_stat.at[0, pl.ds(0, chips - 1)], direct_stat_recv.at[d])
        wait(mine.at[0], direct_acc_recv2.at[d])
        wait(mine_stat.at[0], direct_stat_recv2.at[d])
        t = staged + d
        add_chips([(mine.at[t], mine_stat.at[t], t, core), (theirs.at[d], theirs_stat.at[d], t, 1 - core)])
    wait(out.at[pl.ds(0, staged), 0], out_recv)
    wait(out.at[pl.ds(0, staged), 0], out_send)
    wait(part.at[pl.ds(0, blocks)], pair_send)
    sends = (staged * (chips - 1) + DIRECT * (n - 1)) // chips
    wait(mine.at[pl.ds(0, sends)], acc_send)
    wait(mine_stat.at[pl.ds(0, sends)], stat_send)


def solution(mesh):
    n = mesh.shape["sp"]

    def step(q, k, v):
        batch, heads, head = q.shape
        tokens = k.shape[1]
        k = k.reshape(batch, tokens, head)
        v = v.reshape(batch, tokens, head)
        blocks, chips = batch // BLOCK, n // 2
        dma = pltpu.SemaphoreType.DMA
        return pl.pallas_call(
            functools.partial(kernel, n, head ** -0.5),
            out_shape=jax.ShapeDtypeStruct((blocks, BLOCK, heads, head), BF16),
            in_specs=[pl.BlockSpec(memory_space=pltpu.HBM)] * 3,
            out_specs=pl.BlockSpec(memory_space=pltpu.VMEM),
            scratch_shapes=[
                pltpu.VMEM((batch, heads, head), BF16),
                pltpu.VMEM((batch, tokens, head), BF16),
                pltpu.VMEM((batch, tokens, head), BF16),
                pltpu.VMEM((BLOCK, heads, tokens), F32),
                pltpu.VMEM((BLOCK, heads, tokens), F32),
                pltpu.VMEM((batch, heads, head + 2 * LANES), F32),
                pltpu.VMEM((blocks, heads, head + 2 * LANES), F32),
                pltpu.VMEM((blocks, chips, heads, head), BF16),
                pltpu.VMEM((blocks, chips, 2, LANES), F32),
                pltpu.VMEM((DIRECT, chips, heads, head), BF16),
                pltpu.VMEM((DIRECT, chips, 2, LANES), F32),
                dma, dma((AHEAD,)), dma((AHEAD,)),
                dma, dma((8,)),
                dma, dma, dma((len(CUTS),)), dma((len(CUTS),)),
                dma((DIRECT,)), dma((DIRECT,)), dma((DIRECT,)), dma((DIRECT,)),
                dma, dma,
            ],
            compiler_params=pltpu.CompilerParams(
                collective_id=0, has_side_effects=True, vmem_limit_bytes=48 * 1024 * 1024),
            name="decode",
        )(pltpu.with_memory_space_constraint(q, pltpu.HBM), k, v).reshape(q.shape)

    return jax.shard_map(
        step,
        mesh=mesh,
        in_specs=(P("dp", None, None), P("dp", "sp", None, None), P("dp", "sp", None, None)),
        out_specs=P("dp", None, None),
        check_vma=False,
    )
```
